256 devices in a mesh: gx: 8 (over x, core), gy: 4 (over y), gz: 8 (over z).
Axes of the slice: x: 4, y: 4, z: 8, core: 2. Of those that a mesh axis runs over, the one named last changes fastest.
Arguments:
- velocity: float32 [3, 128, 128, 1024], P(None, 'gx', 'gy', 'gz'), may hold values from -6 to 6
- forcing: float32 [3, 128, 128, 1024], P(None, 'gx', 'gy', 'gz'), may hold values from -12 to 12
- phase_block: int32 [32, 32, 256], P('gx', 'gy', 'gz'), may hold values from 0 to 7
- prefactor: float32 [8], replicated, may hold values from 0.5 to 4
- yield_stress: float32 [8], replicated, may hold values from 1 to 16
Outputs:
- smoothed: float32 [3, 128, 128, 1024], P(None, 'gx', 'gy', 'gz')
- viscosity_field: float32 [128, 128, 1024], P('gx', 'gy', 'gz')
- coarse_one: float32 [64, 64, 512], P('gx', 'gy', 'gz')
- coarse_two: float32 [32, 32, 256], P('gx', 'gy', 'gz')
- coarse_three: float32 [16, 16, 128], P('gx', 'gy', 'gz')
- residual_field: float32 [3, 128, 128, 1024], P(None, 'gx', 'gy', 'gz')
- residual_rms: float32 [], replicated
The draws below stay inside these ranges and needn't reach their ends.
All inputs are finite; a program needn't handle non-finite values.
Results may differ from the reference program's by a relative error of at most 0.000053.
Values sent between devices are 32-bit elements; how exact they have to be, the bound alone decides.
No kernel may reach another device: no remote copies, remote signals or barrier semaphores. Data moves between devices by JAX's collectives and lax.ppermute only.
A program may use at most 64 MiB of HBM per device.

```python
import math
import jax
import jax.numpy as jnp
from jax import lax

BLOCK = 4
NPHASE = 8
SWEEPS = 2
NX = 128
NY = 128
NZ = 1024


def draw_forcing(key, part):
    first_key = jax.random.fold_in(key, 11)
    position = jnp.arange(NX, dtype=jnp.float32) / NX
    ramp = (1.0 + 2.0 * position)[None, :, None, None]
    values = jax.random.truncated_normal(first_key, -4.0, 4.0, (3, NX, NY, NZ), jnp.float32)
    return values * ramp


def set_ends(array, stream_key, smallest, high):
    place = [jax.random.randint(jax.random.fold_in(stream_key, axis), (), 0, length) for axis, length in enumerate(array.shape)]
    widest = array.shape.index(max(array.shape))
    beside = place[:widest] + [(place[widest] + 1) % array.shape[widest]] + place[widest + 1:]
    return array.at[tuple(place)].set(smallest).at[tuple(beside)].set(high)


def block_scale(own_key, shape, pieces, smallest, largest):
    def one(dim, parts):
        steps = jax.random.uniform(jax.random.fold_in(jax.random.fold_in(own_key, 6), dim), (parts,), jnp.float32, smallest / len(pieces), largest / len(pieces))
        return jnp.repeat(jnp.exp(steps), shape[dim] // parts).reshape((-1,) + (1,) * (len(shape) - dim - 1))

    loudness = one(*pieces[0])
    for cut in pieces[1:]:
        loudness = loudness * one(*cut)
    return loudness


def bell_draw(own_key, shape, spread, bound, shards=(), kind=jnp.bfloat16):
    values = spread * jax.random.normal(own_key, shape, jnp.float32)
    if shards:
        values = values * block_scale(own_key, shape, shards, -0.22, 0.18)
    return jnp.clip(values, -bound, bound).astype(kind)


def setup_inputs(seed: int = 0) -> dict:
    splits = jax.random.split(jax.random.key(seed), 6)
    velocity = bell_draw(splits[0], (3, NX, NY, NZ), 1.0, 6.0, ((1, 8), (2, 4), (3, 8)), jnp.float32)
    forcing = draw_forcing(jax.random.fold_in(splits[5], 71), 0)
    phase_block = set_ends(jax.random.randint(splits[2], (NX // BLOCK, NY // BLOCK, NZ // BLOCK), 0, NPHASE), jax.random.fold_in(splits[2], 1), 0, NPHASE - 1).astype(jnp.int32)
    prefactor = jnp.clip(jnp.exp(jax.random.uniform(splits[3], (NPHASE,), jnp.float32, math.log(0.5), math.log(4.0))), 0.5, 4.0)
    yield_stress = jnp.clip(jnp.exp(jax.random.uniform(splits[4], (NPHASE,), jnp.float32, math.log(1.0), math.log(16.0))), 1.0, 16.0)
    return dict(velocity=velocity, forcing=forcing, phase_block=phase_block, prefactor=prefactor, yield_stress=yield_stress)


RELAXATION = 0.8
NEIGHBOUR_OFFSETS = ((1, 0, 0), (-1, 0, 0), (0, 1, 0), (0, -1, 0), (0, 0, 1), (0, 0, -1))
UNIT_STEPS = ((1, 0, 0), (0, 1, 0), (0, 0, 1))

def offset_view(field, shift_x, shift_y, shift_z):
    size_x = field.shape[-3] - 2
    size_y = field.shape[-2] - 2
    size_z = field.shape[-1] - 2
    return field[..., 1 + shift_x:1 + shift_x + size_x, 1 + shift_y:1 + shift_y + size_y, 1 + shift_z:1 + shift_z + size_z]

def viscosity_of(padded_vel, prefactor_cells, yield_cells):
    gradient = []
    for comp_a in range(3):
        row_list = []
        for comp_b in range(3):
            step_up = UNIT_STEPS[comp_b]
            step_down = (-step_up[0], -step_up[1], -step_up[2])
            row_list.append(0.5 * (offset_view(padded_vel[comp_a], *step_up) - offset_view(padded_vel[comp_a], *step_down)))
        gradient.append(row_list)
    strain_sq = jnp.zeros(gradient[0][0].shape, jnp.float32)
    for comp_a in range(3):
        for comp_b in range(3):
            strain = 0.5 * (gradient[comp_a][comp_b] + gradient[comp_b][comp_a])
            strain_sq = strain_sq + strain * strain
    invariant = 0.5 * strain_sq + 1.0
    creeping = prefactor_cells * jnp.power(invariant, -1.0 / 3.0)
    plastic = yield_cells / (2.0 * jnp.sqrt(invariant))
    return jnp.minimum(creeping, plastic)

def restrict_dim(field, dim_index):
    coarse_len = (field.shape[dim_index] - 2) // 2

    def every_other(start):
        return lax.slice_in_dim(field, start, start + 2 * coarse_len - 1, 2, dim_index)
    return (every_other(0) + 3.0 * every_other(1) + 3.0 * every_other(2) + every_other(3)) * 0.125

def coarsen(padded):
    return restrict_dim(restrict_dim(restrict_dim(padded, 0), 1), 2)

def smooth_terms(padded_vel, padded_visc):
    centre = offset_view(padded_visc, 0, 0, 0)
    diagonal = jnp.zeros(centre.shape, jnp.float32)
    neighbours = jnp.zeros((3,) + centre.shape, jnp.float32)
    for offset in NEIGHBOUR_OFFSETS:
        face_visc = 0.5 * (centre + offset_view(padded_visc, *offset))
        diagonal = diagonal + face_visc
        neighbours = neighbours + face_visc[None] * offset_view(padded_vel, *offset)
    return (diagonal, neighbours)

def jacobi_sweep(padded_vel, padded_visc, forcing):
    diagonal, neighbours = smooth_terms(padded_vel, padded_visc)
    centre_vel = offset_view(padded_vel, 0, 0, 0)
    return centre_vel + RELAXATION * (forcing - (diagonal[None] * centre_vel - neighbours)) / diagonal[None]

def misfit(padded_vel, padded_visc, forcing):
    diagonal, neighbours = smooth_terms(padded_vel, padded_visc)
    centre_vel = offset_view(padded_vel, 0, 0, 0)
    return forcing - (diagonal[None] * centre_vel - neighbours)

def pad_vel(field):
    return jnp.pad(field, ((0, 0), (1, 1), (1, 1), (1, 1)))

def reference(velocity, forcing, phase_block, prefactor, yield_stress):
    cell_phase = jnp.repeat(jnp.repeat(jnp.repeat(phase_block, BLOCK, 0), BLOCK, 1), BLOCK, 2)
    prefactor_cells = prefactor[cell_phase]
    yield_cells = yield_stress[cell_phase]
    viscosity_field = viscosity_of(pad_vel(velocity), prefactor_cells, yield_cells)
    coarse_one = coarsen(jnp.pad(viscosity_field, 1))
    coarse_two = coarsen(jnp.pad(coarse_one, 1))
    coarse_three = coarsen(jnp.pad(coarse_two, 1))
    padded_visc = jnp.pad(viscosity_field, 1)
    current = velocity
    for sweep_index in range(SWEEPS):
        current = jacobi_sweep(pad_vel(current), padded_visc, forcing)
    misfit_field = misfit(pad_vel(current), padded_visc, forcing)
    residual_rms = jnp.sqrt(jnp.sum(misfit_field * misfit_field) / (3.0 * NX * NY * NZ))
    return (current, viscosity_field, coarse_one, coarse_two, coarse_three, misfit_field, residual_rms)
```

```python
import functools

import jax
import jax.numpy as jnp
from jax import lax
from jax.experimental import pallas as pl
from jax.experimental.pallas import tpu as pltpu
from jax.sharding import PartitionSpec as P

F32 = jnp.float32
BLOCK = 4
AX = ("gx", "gy", "gz")
NX, NY, NZ = 16, 32, 128
VMEM = pl.BlockSpec(memory_space=pltpu.VMEM)
SMEM = pl.BlockSpec(memory_space=pltpu.SMEM)


def sds(*shape):
    return jax.ShapeDtypeStruct(shape, F32)


def position(axis):
    index = lax.axis_index(axis)
    return lax.rem(index, 2) == 0, index > 0, index < lax.axis_size(axis) - 1


def lanes(rows=8, width=128):
    return lax.broadcasted_iota(jnp.int32, (rows, width), 1)


def subs(rows=8, width=128):
    return lax.broadcasted_iota(jnp.int32, (rows, width), 0)


def roll(value, shift, axis):
    size = value.shape[axis]
    shift = shift % size
    return pltpu.roll(value, shift, axis) if shift else value


def pair_a(value, axis):
    count = lax.axis_size(axis)
    return lax.ppermute(value, axis, [(i, i ^ 1) for i in range(count)])


def pair_b(value, axis):
    count = lax.axis_size(axis)
    return lax.ppermute(
        value, axis, [(i, (i + 1) % count if i % 2 else (i - 1) % count) for i in range(count)]
    )


def params():
    return pltpu.CompilerParams(vmem_limit_bytes=40 << 20)


def cost(flops):
    return pl.CostEstimate(flops=flops, bytes_accessed=1 << 20, transcendentals=0)


def pack_x(vel, forc, phase, send_a, send_b):
    even, _, _ = position("gx")
    for out, first in ((send_a, jnp.where(even, 1, 0)), (send_b, jnp.where(even, 0, 1))):
        for c in range(3):
            for i in range(4):
                out[4 * c + i] = vel[c, 12 * first + i]
            for i in range(2):
                out[12 + 2 * c + i] = forc[c, 14 * first + i]
        out[18, 0:8] = phase[3 * first]


def halo(pair, axis, index):
    even, has_lo, has_hi = position(axis)
    a, b = pair[0][index], pair[1][index]
    lo = jnp.where(has_lo, jnp.where(even, b, a), 0.0)
    hi = jnp.where(has_hi, jnp.where(even, a, b), 0.0)
    return lo, hi


def tile_of(own, c, plane, o, width, rx, base, ry):
    rows = slice(8 * o, 8 * o + 8)
    if o == 4:
        sub = subs()
        if width == 4:
            lo, hi = halo(ry, "gy", c * 12 + plane % 12)
            if plane < 12:
                return jnp.where(sub < 4, hi, roll(lo, 4, 0))
            return jnp.where(sub < 4, roll(hi, 4, 0), lo)
        lo, hi = halo(ry, "gy", 36 + c * 5 + plane % 5)
        k = plane // 5
        return jnp.where(sub < 4, roll(hi, -2 * k, 0), roll(lo, 6 - 2 * k, 0))
    if plane < width:
        return halo(rx, "gx", (base + width * c + plane, rows))[0]
    if plane >= NX + width:
        return halo(rx, "gx", (base + width * c + plane - NX - width, rows))[1]
    return own[c, plane - width, rows]


def phase_rows(phase, rx, b):
    if b == 0:
        return halo(rx, "gx", (18, slice(0, 8)))[0]
    if b == 5:
        return halo(rx, "gx", (18, slice(0, 8)))[1]
    return phase[b - 1]


def phase_tiles(phase, rx, ry):
    lo, hi = halo(ry, "gy", 51)
    sub = subs()
    tiles = []
    for b in range(6):
        tiles.append(phase_rows(phase, rx, b))
        outer = jnp.where(sub == 0, hi[b : b + 1], jnp.where(sub == 1, lo[b : b + 1], 0.0))
        tiles.append(outer)
    return tiles


def pack_y(vel, forc, phase, rx_a, rx_b, send_a, send_b):
    rx = (rx_a, rx_b)
    even, _, _ = position("gy")
    sub = subs()

    def put(index, lo, hi):
        send_a[index] = jnp.where(even, hi, lo)
        send_b[index] = jnp.where(even, lo, hi)

    def u(c, p, o):
        return tile_of(vel, c, p, o, 4, rx, 0, None)

    def f(c, p, o):
        return tile_of(forc, c, p, o, 2, rx, 12, None)

    for c in range(3):
        for p in range(12):
            lo = jnp.where(sub < 4, u(c, p, 0), roll(u(c, p + 12, 0), 4, 0))
            hi = jnp.where(sub < 4, roll(u(c, p, 3), 4, 0), u(c, p + 12, 3))
            put(c * 12 + p, lo, hi)
        for g in range(5):
            lo = f(c, g, 0)
            hi = roll(f(c, g, 3), 2, 0)
            for k in range(1, 4):
                here = (sub >> 1) == k
                lo = jnp.where(here, roll(f(c, g + 5 * k, 0), 2 * k, 0), lo)
                hi = jnp.where(here, roll(f(c, g + 5 * k, 3), 2 * k + 2, 0), hi)
            put(36 + c * 5 + g, lo, hi)
    lo = jnp.zeros((8, 128), F32)
    hi = lo
    for b in range(6):
        tile = phase_rows(phase, rx, b)
        lo = jnp.where(sub == b, tile[0:1], lo)
        hi = jnp.where(sub == b, tile[7:8], hi)
    put(51, lo, hi)


def pack_tiles(tiles):
    lane = lanes()
    group = lane >> 3
    packed = []
    for half in range(2):
        value = jnp.zeros((8, 128), F32)
        for j, tile in enumerate(tiles[16 * half : 16 * half + 16]):
            value = jnp.where(group == j, roll(tile(), 8 * j + 4, 1), value)
        packed.append(value)
    keep = (lane & 4) == 0
    hi = jnp.where(keep, packed[0], roll(packed[1], 4, 1))
    lo = jnp.where(keep, roll(packed[0], -4, 1), packed[1])
    return lo, hi


def unpack_tiles(from_lo, from_hi, count):
    lane = lanes()
    keep = (lane & 4) == 0
    packed = (
        jnp.where(keep, from_lo, roll(from_hi, 4, 1)),
        jnp.where(keep, roll(from_lo, -4, 1), from_hi),
    )
    wanted = (lane < 4) | (lane >= 124)
    return [
        jnp.where(wanted, roll(packed[t // 16], 124 - 8 * (t % 16), 1), 0.0) for t in range(count)
    ]


def pack_z(vel, forc, phase, rx_a, rx_b, ry_a, ry_b, send_a, send_b):
    rx, ry = (rx_a, rx_b), (ry_a, ry_b)
    even, _, _ = position("gz")

    def put(index, lo, hi):
        send_a[index] = jnp.where(even, hi, lo)
        send_b[index] = jnp.where(even, lo, hi)

    for c in range(3):
        for q in range(4):
            put(4 * c + q, *pack_tiles([
                functools.partial(tile_of, vel, c, 6 * q + p, o, 4, rx, 0, ry)
                for p in range(6) for o in range(5)
            ]))
            put(12 + 4 * c + q, *pack_tiles([
                functools.partial(tile_of, forc, c, 5 * q + p, o, 2, rx, 12, ry)
                for p in range(5) for o in range(5)
            ]))
    lane = lanes()
    lo = jnp.zeros((8, 128), F32)
    hi = lo
    for j, tile in enumerate(phase_tiles(phase, rx, ry)):
        lo = jnp.where(lane == j, roll(tile, j, 1), lo)
        hi = jnp.where(lane == j, roll(tile, j - 31, 1), hi)
    put(24, lo, hi)


def shift_up(value):
    last = lanes() == 127
    a, b = roll(value[:, :128], 127, 1), roll(value[:, 128:], 127, 1)
    return jnp.concatenate([jnp.where(last, b, a), jnp.where(last, a, b)], axis=1)


def shift_down(value):
    first = lanes() == 0
    a, b = roll(value[:, :128], 1, 1), roll(value[:, 128:], 1, 1)
    return jnp.concatenate([jnp.where(first, b, a), jnp.where(first, a, b)], axis=1)


def band(rows, row_z, col_m):
    row = row_z(lax.broadcasted_iota(jnp.int32, (rows, 128), 0))
    col = col_m(lax.broadcasted_iota(jnp.int32, (rows, 128), 1))
    at = row - 2 * col + 1
    return jnp.where((at == 0) | (at == 3), 0.125, jnp.where((at == 1) | (at == 2), 0.375, 0.0)).astype(F32)


def exact_dot(a, b):
    return jnp.dot(a, b, preferred_element_type=F32, precision=lax.Precision.HIGHEST)


def four(a, b, c, d):
    return (a + 3.0 * b + 3.0 * c + d) * 0.125


def put_rows(ref, index, o, value):
    ref[index + (slice(8 + 8 * o, 16 + 8 * o),)] = value
    if o == 0:
        ref[index + (slice(48, 56),)] = value
    if o == 4:
        ref[index + (slice(0, 8),)] = value


def local_work(
    vel, forc, phase_ref, rx_a, rx_b, ry_a, ry_b, rz_a, rz_b, pre, yld,
    smoothed, visc_out, one_out, two_out, residual, partial,
    u_ref, f_ref, cells, v_ref, u1, u2, w_m, w_s, y1, c1, t2, t3,
):
    rx, ry, rz = (rx_a, rx_b), (ry_a, ry_b), (rz_a, rz_b)
    lo_x, hi_x = (flag.astype(F32) for flag in position("gx")[1:])
    lo_y, hi_y = (flag.astype(F32) for flag in position("gy")[1:])
    lo_z, hi_z = (flag.astype(F32) for flag in position("gz")[1:])
    lane = lanes()

    for c in range(3):
        for q in range(4):
            tiles = unpack_tiles(*halo(rz, "gz", 4 * c + q), 30)
            for t, side in enumerate(tiles):
                p, o = 6 * q + t // 5, t % 5
                own = tile_of(vel, c, p, o, 4, rx, 0, ry)
                put_rows(u_ref, (c, p), o, jnp.concatenate([own, side], axis=1))
            tiles = unpack_tiles(*halo(rz, "gz", 12 + 4 * c + q), 25)
            for t, side in enumerate(tiles):
                p, o = 5 * q + t // 5, t % 5
                own = tile_of(forc, c, p, o, 2, rx, 12, ry)
                f_ref[c, p, 8 * o : 8 * o + 8] = jnp.concatenate([own, side], axis=1)

    lo, hi = halo(rz, "gz", 24)
    rows = []
    for j, tile in enumerate(phase_tiles(phase_ref, rx, ry)):
        tile = jnp.where(lane == 32, roll(hi, 32 - j, 1), tile)
        rows.append(jnp.where(lane == 33, roll(lo, 33 - j, 1), tile))
    ph = jnp.concatenate(rows, axis=0)
    zi = lax.broadcasted_iota(jnp.int32, (128, 256), 1)
    bz = lax.broadcasted_iota(jnp.int32, (128, 256), 0)
    wide = jnp.where(zi < 128, zi >> 2, jnp.where(zi < 192, 32, 33))
    ph_z = jnp.dot(ph, (wide == bz).astype(F32), preferred_element_type=F32)
    ri = lax.broadcasted_iota(jnp.int32, (40, 16), 0)
    by = lax.broadcasted_iota(jnp.int32, (40, 16), 1)
    tall = (jnp.where(ri < 32, ri >> 2, jnp.where(ri < 36, 8, 9)) == by).astype(F32)
    for b in range(6):
        cells[b] = jnp.dot(tall, ph_z[16 * b : 16 * b + 16], preferred_element_type=F32)

    wide_lane = lanes(8, 256)
    mask_z = jnp.where(
        wide_lane < 128, 1.0, jnp.where(wide_lane < 131, hi_z, jnp.where(wide_lane >= 253, lo_z, 0.0))
    )
    row4 = subs(8, 256)
    mask_zy = mask_z * jnp.where(row4 < 4, hi_y, lo_y)

    def viscosity(vx, _):
        px = vx + 1
        mask_x = jnp.where(vx < 3, lo_x, jnp.where(vx >= 19, hi_x, 1.0))
        bx = (vx + 1) >> 2
        for o in range(5):
            d = []
            for c in range(3):
                mid = u_ref[c, px, 8 + 8 * o : 16 + 8 * o]
                d.append((
                    u_ref[c, px + 1, 8 + 8 * o : 16 + 8 * o] - u_ref[c, px - 1, 8 + 8 * o : 16 + 8 * o],
                    u_ref[c, px, 9 + 8 * o : 17 + 8 * o] - u_ref[c, px, 7 + 8 * o : 15 + 8 * o],
                    shift_up(mid) - shift_down(mid),
                ))
            a01, a02, a12 = d[0][1] + d[1][0], d[0][2] + d[2][0], d[1][2] + d[2][1]
            own = d[0][0] * d[0][0] + d[1][1] * d[1][1] + d[2][2] * d[2][2]
            off = a01 * a01 + a02 * a02 + a12 * a12
            invariant = 1.0 + (own * 0.125 + off * 0.0625)
            phase = cells[bx, 8 * o : 8 * o + 8]
            creep = jnp.full((8, 256), pre[0], F32)
            limit = jnp.full((8, 256), yld[0], F32)
            for k in range(1, 8):
                here = phase == float(k)
                creep = jnp.where(here, pre[k], creep)
                limit = jnp.where(here, yld[k], limit)
            value = jnp.minimum(
                creep * jnp.exp(jnp.log(invariant) * (-1.0 / 3.0)), (0.5 * limit) * lax.rsqrt(invariant)
            )
            put_rows(v_ref, (vx,), o, value * (mask_x * (mask_zy if o == 4 else mask_z)))
        return 0

    lax.fori_loop(0, 22, viscosity, 0)

    def faces(vx, o):
        mid = v_ref[vx, 8 + 8 * o : 16 + 8 * o]
        return mid, (
            mid + v_ref[vx + 1, 8 + 8 * o : 16 + 8 * o],
            mid + v_ref[vx - 1, 8 + 8 * o : 16 + 8 * o],
            mid + v_ref[vx, 9 + 8 * o : 17 + 8 * o],
            mid + v_ref[vx, 7 + 8 * o : 15 + 8 * o],
            mid + shift_up(mid),
            mid + shift_down(mid),
        )

    def around(ref, c, p, o, f):
        mid = ref[c, p, 8 + 8 * o : 16 + 8 * o]
        total = f[0] * ref[c, p + 1, 8 + 8 * o : 16 + 8 * o]
        total = total + f[1] * ref[c, p - 1, 8 + 8 * o : 16 + 8 * o]
        total = total + f[2] * ref[c, p, 9 + 8 * o : 17 + 8 * o]
        total = total + f[3] * ref[c, p, 7 + 8 * o : 15 + 8 * o]
        total = total + f[4] * shift_up(mid)
        return mid, total + f[5] * shift_down(mid)

    def sweep(source, target, first, first_u):
        def body(x, _):
            for o in range(5):
                mid_v, f = faces(x + first, o)
                diag = (f[0] + f[1]) + (f[2] + f[3]) + (f[4] + f[5])
                rate = jnp.where(mid_v > 0.0, 0.8 / diag, 0.0)
                for c in range(3):
                    mid, total = around(source, c, x + first_u, o, f)
                    force = f_ref[c, x + first - 1, 8 * o : 8 * o + 8]
                    put_rows(target, (c, x), o, 0.2 * mid + rate * (2.0 * force + total))
            return 0

        return body

    lax.fori_loop(0, 20, sweep(u_ref, u1, 1, 2), 0)
    lax.fori_loop(0, 18, sweep(u1, u2, 2, 1), 0)

    def last(x, acc):
        for o in range(4):
            _, f = faces(x + 3, o)
            diag = (f[0] + f[1]) + (f[2] + f[3]) + (f[4] + f[5])
            for c in range(3):
                mid, total = around(u2, c, x + 1, o, f)
                force = f_ref[c, x + 2, 8 * o : 8 * o + 8]
                value = (force + 0.5 * (total - diag * mid))[:, :128]
                residual[c, x, 8 * o : 8 * o + 8] = value
                smoothed[c, x, 8 * o : 8 * o + 8] = mid[:, :128]
                acc = acc + value * value
            visc_out[x, 8 * o : 8 * o + 8] = v_ref[x + 3, 8 + 8 * o : 16 + 8 * o, 0:128]
        return acc

    acc = lax.fori_loop(0, NX, last, jnp.zeros((8, 128), F32))
    square = jnp.sum(jnp.sum(acc, axis=1, keepdims=True), axis=0, keepdims=True)

    def coarse_x(k, _):
        value = four(v_ref[2 * k], v_ref[2 * k + 1], v_ref[2 * k + 2], v_ref[2 * k + 3])
        w_m[k] = value[:, :128]
        w_s[k] = value[:, 128:]
        return 0

    lax.fori_loop(0, 10, coarse_x, 0)
    y1[...] = jnp.zeros(y1.shape, F32)
    for k in range(10):
        for ref, at in ((w_m, 0), (w_s, 128)):
            y1[k, 0:18, at : at + 128] = four(*(ref[k, pl.ds(5 + i, 18, stride=2)] for i in range(4)))
    band1 = band(256, lambda r: jnp.where(r < 192, r, r - 256), lambda m: jnp.where(m < 65, m, jnp.where(m == 65, -1, 1000)))
    coarse = exact_dot(y1[...].reshape(240, 256), band1).reshape(10, 24, 128)
    row24, lane24 = subs(24), lanes(24)
    mask_yz = jnp.where(row24 == 0, lo_y, jnp.where(row24 == 17, hi_y, 1.0)) * jnp.where(
        lane24 == 64, hi_z, jnp.where(lane24 == 65, lo_z, 1.0)
    )
    for k in range(10):
        mask = mask_yz * (lo_x if k == 0 else hi_x if k == 9 else 1.0)
        c1[k] = coarse[k] * mask
    for k in range(8):
        one_out[k] = c1[k + 1, 1:17, 0:64]
    rows = []
    for k in range(4):
        t2[...] = four(c1[2 * k], c1[2 * k + 1], c1[2 * k + 2], c1[2 * k + 3])
        rows.append(four(*(t2[pl.ds(i, 8, stride=2)] for i in range(4))))
    band2 = band(128, lambda r: jnp.where(r < 65, r, jnp.where(r == 65, -1, 100000)), lambda m: jnp.where(m < 32, m, 1000))
    coarse = exact_dot(jnp.concatenate(rows, axis=0), band2)
    planes = [coarse[8 * k : 8 * k + 8] for k in range(4)]
    for k in range(4):
        two_out[k] = planes[k][:, 0:32]
    thirds = (
        0.125 * planes[0],
        0.125 * (3.0 * planes[0] + 3.0 * planes[1] + planes[2]),
        0.125 * (planes[1] + 3.0 * planes[2] + 3.0 * planes[3]),
        0.125 * planes[3],
    )
    rows = []
    t3[...] = jnp.zeros(t3.shape, F32)
    for k in range(4):
        t3[4:12] = thirds[k]
        rows.append(four(*(t3[pl.ds(1 + i, 8, stride=2)] for i in range(4))))
    band3 = band(128, lambda r: jnp.where(r < 32, r, 100000), lambda m: jnp.where(m < 18, m - 1, 1000))
    coarse = exact_dot(jnp.concatenate(rows, axis=0), band3)
    for k in range(4):
        partial[k] = jnp.where(subs() == 7, square, coarse[8 * k : 8 * k + 8])


def with_sum(tile, total):
    row = lax.broadcasted_iota(jnp.int32, tile.shape, tile.ndim - 2)
    return jnp.where(row == 7, total, tile)


def finish(partial):
    total = partial[0, 7:8, :]
    even, has_lo, has_hi = position("gx")
    got_a = pair_a(with_sum(jnp.where(even, partial[3], partial[0]), total), "gx")
    total = total + got_a[7:8]
    got_b = pair_b(with_sum(jnp.where(even, partial[0], partial[3]), total), "gx")
    total = total + got_b[7:8]
    lo, hi = jnp.where(even, got_b, got_a), jnp.where(even, got_a, got_b)
    inner = jnp.stack(
        [partial[1] + jnp.where(has_lo, lo, 0.0), partial[2] + jnp.where(has_hi, hi, 0.0)]
    )
    total = total + far("gx", total)
    even, has_lo, has_hi = position("gy")
    got_a = pair_a(with_sum(inner, total), "gy")
    total = total + got_a[0, 7:8]
    got_b = pair_b(with_sum(inner, total), "gy")
    total = total + got_b[0, 7:8]
    lo, hi = jnp.where(even, got_b, got_a), jnp.where(even, got_a, got_b)
    row = lax.broadcasted_iota(jnp.int32, inner.shape, 1)
    inner = (
        inner
        + jnp.where((row == 1) & has_lo, jnp.roll(lo, -4, 1), 0.0)
        + jnp.where((row == 4) & has_hi, jnp.roll(hi, 4, 1), 0.0)
    )
    even, has_lo, has_hi = position("gz")
    got_a = pair_a(with_sum(inner, total), "gz")
    total = total + got_a[0, 7:8]
    got_b = pair_b(with_sum(inner, total), "gz")
    total = total + got_b[0, 7:8]
    lo, hi = jnp.where(even, got_b, got_a), jnp.where(even, got_a, got_b)
    total = total + far("gz", total)
    three = inner[:, 1:5, 1:17]
    z = lax.broadcasted_iota(jnp.int32, three.shape, 2)
    three = (
        three
        + jnp.where((z == 0) & has_lo, lo[:, 1:5, 17:18], 0.0)
        + jnp.where((z == 15) & has_hi, hi[:, 1:5, 0:1], 0.0)
    )
    return total[0, 0], three


def far(axis, total):
    count = lax.axis_size(axis)
    if count == 4:
        return jnp.zeros_like(total)
    return lax.ppermute(total, axis, [(i, (i + count // 2) % count) for i in range(count)])


def pack(kernel, shape, name, *args):
    return pl.pallas_call(
        kernel, out_shape=[sds(*shape)] * 2, in_specs=[VMEM] * len(args), out_specs=[VMEM] * 2,
        compiler_params=params(), name=name,
    )(*args)


def per_device(velocity, forcing, phase_block, prefactor, yield_stress):
    phase = jnp.pad(phase_block.astype(F32), ((0, 0), (0, 0), (0, 96)))
    own = (velocity, forcing, phase)
    send_a, send_b = pack(pack_x, (19, 32, 128), "pack_x", *own)
    rx = (pair_a(send_a, "gx"), pair_b(send_b, "gx"))
    send_a, send_b = pack(pack_y, (52, 8, 128), "pack_y", *own, *rx)
    ry = (pair_a(send_a, "gy"), pair_b(send_b, "gy"))
    send_a, send_b = pack(pack_z, (25, 8, 128), "pack_z", *own, *rx, *ry)
    rz = (pair_a(send_a, "gz"), pair_b(send_b, "gz"))
    smoothed, visc, one, two, residual, partial = pl.pallas_call(
        local_work,
        out_shape=[
            sds(3, NX, NY, NZ), sds(NX, NY, NZ), sds(8, 16, 64), sds(4, 8, 32), sds(3, NX, NY, NZ), sds(4, 8, 128),
        ],
        in_specs=[VMEM] * 9 + [SMEM] * 2,
        out_specs=[VMEM] * 6,
        scratch_shapes=[
            pltpu.VMEM((3, 24, 56, 256), F32), pltpu.VMEM((3, 20, 40, 256), F32), pltpu.VMEM((6, 40, 256), F32),
            pltpu.VMEM((22, 56, 256), F32), pltpu.VMEM((3, 20, 56, 256), F32), pltpu.VMEM((3, 18, 56, 256), F32),
            pltpu.VMEM((10, 56, 128), F32), pltpu.VMEM((10, 56, 128), F32), pltpu.VMEM((10, 24, 256), F32),
            pltpu.VMEM((10, 24, 128), F32), pltpu.VMEM((24, 128), F32), pltpu.VMEM((24, 128), F32),
        ],
        compiler_params=params(), name="local_work",
    )(*own, *rx, *ry, *rz, prefactor, yield_stress)
    total, three = finish(partial)
    cells = 3.0 * NX * NY * NZ
    for axis in AX:
        cells = cells * lax.axis_size(axis)
    return smoothed, visc, one, two, three, residual, jnp.sqrt(total / cells)


def solution(mesh):
    field, cell = P(None, *AX), P(*AX)
    return jax.shard_map(
        per_device,
        mesh=mesh,
        in_specs=(field, field, cell, P(), P()),
        out_specs=(field, cell, cell, cell, cell, field, P()),
        check_vma=False,
    )
```

```python
import functools

import jax
import jax.numpy as jnp
from jax import lax
from jax.experimental import pallas as pl
from jax.experimental.pallas import tpu as pltpu
from jax.sharding import PartitionSpec as P

F32 = jnp.float32
BLOCK = 4
AX = ("gx", "gy", "gz")
NX, NY, NZ = 16, 32, 128
VMEM = pl.BlockSpec(memory_space=pltpu.VMEM)
SMEM = pl.BlockSpec(memory_space=pltpu.SMEM)


def sds(*shape):
    return jax.ShapeDtypeStruct(shape, F32)


def position(axis):
    index = lax.axis_index(axis)
    return lax.rem(index, 2) == 0, index > 0, index < lax.axis_size(axis) - 1


def lanes(rows=8, width=128):
    return lax.broadcasted_iota(jnp.int32, (rows, width), 1)


def subs(rows=8, width=128):
    return lax.broadcasted_iota(jnp.int32, (rows, width), 0)


def roll(value, shift, axis):
    size = value.shape[axis]
    shift = shift % size
    return pltpu.roll(value, shift, axis) if shift else value


def pair_a(value, axis):
    count = lax.axis_size(axis)
    return lax.ppermute(value, axis, [(i, i ^ 1) for i in range(count)])


def pair_b(value, axis):
    count = lax.axis_size(axis)
    return lax.ppermute(
        value, axis, [(i, (i + 1) % count if i % 2 else (i - 1) % count) for i in range(count)]
    )


def params():
    return pltpu.CompilerParams(vmem_limit_bytes=40 << 20)


def cost(flops):
    return pl.CostEstimate(flops=flops, bytes_accessed=1 << 20, transcendentals=0)


def pack_x(vel, forc, phase, send_a, send_b):
    even, _, _ = position("gx")
    for out, first in ((send_a, jnp.where(even, 1, 0)), (send_b, jnp.where(even, 0, 1))):
        for c in range(3):
            for i in range(4):
                out[4 * c + i] = vel[c, 12 * first + i]
            for i in range(2):
                out[12 + 2 * c + i] = forc[c, 14 * first + i]
        out[18, 0:8] = phase[3 * first]


def halo(pair, axis, index):
    even, has_lo, has_hi = position(axis)
    a, b = pair[0][index], pair[1][index]
    lo = jnp.where(has_lo, jnp.where(even, b, a), 0.0)
    hi = jnp.where(has_hi, jnp.where(even, a, b), 0.0)
    return lo, hi


def tile_of(own, c, plane, o, width, rx, base, ry):
    rows = slice(8 * o, 8 * o + 8)
    if o == 4:
        sub = subs()
        if width == 4:
            lo, hi = halo(ry, "gy", c * 12 + plane % 12)
            if plane < 12:
                return jnp.where(sub < 4, hi, roll(lo, 4, 0))
            return jnp.where(sub < 4, roll(hi, 4, 0), lo)
        lo, hi = halo(ry, "gy", 36 + c * 5 + plane % 5)
        k = plane // 5
        return jnp.where(sub < 4, roll(hi, -2 * k, 0), roll(lo, 6 - 2 * k, 0))
    if plane < width:
        return halo(rx, "gx", (base + width * c + plane, rows))[0]
    if plane >= NX + width:
        return halo(rx, "gx", (base + width * c + plane - NX - width, rows))[1]
    return own[c, plane - width, rows]


def phase_rows(phase, rx, b):
    if b == 0:
        return halo(rx, "gx", (18, slice(0, 8)))[0]
    if b == 5:
        return halo(rx, "gx", (18, slice(0, 8)))[1]
    return phase[b - 1]


def phase_tiles(phase, rx, ry):
    lo, hi = halo(ry, "gy", 51)
    sub = subs()
    tiles = []
    for b in range(6):
        tiles.append(phase_rows(phase, rx, b))
        outer = jnp.where(sub == 0, hi[b : b + 1], jnp.where(sub == 1, lo[b : b + 1], 0.0))
        tiles.append(outer)
    return tiles


def pack_y(vel, forc, phase, rx_a, rx_b, send_a, send_b):
    rx = (rx_a, rx_b)
    even, _, _ = position("gy")
    sub = subs()

    def put(index, lo, hi):
        send_a[index] = jnp.where(even, hi, lo)
        send_b[index] = jnp.where(even, lo, hi)

    def u(c, p, o):
        return tile_of(vel, c, p, o, 4, rx, 0, None)

    def f(c, p, o):
        return tile_of(forc, c, p, o, 2, rx, 12, None)

    for c in range(3):
        for p in range(12):
            lo = jnp.where(sub < 4, u(c, p, 0), roll(u(c, p + 12, 0), 4, 0))
            hi = jnp.where(sub < 4, roll(u(c, p, 3), 4, 0), u(c, p + 12, 3))
            put(c * 12 + p, lo, hi)
        for g in range(5):
            lo = f(c, g, 0)
            hi = roll(f(c, g, 3), 2, 0)
            for k in range(1, 4):
                here = (sub >> 1) == k
                lo = jnp.where(here, roll(f(c, g + 5 * k, 0), 2 * k, 0), lo)
                hi = jnp.where(here, roll(f(c, g + 5 * k, 3), 2 * k + 2, 0), hi)
            put(36 + c * 5 + g, lo, hi)
    lo = jnp.zeros((8, 128), F32)
    hi = lo
    for b in range(6):
        tile = phase_rows(phase, rx, b)
        lo = jnp.where(sub == b, tile[0:1], lo)
        hi = jnp.where(sub == b, tile[7:8], hi)
    put(51, lo, hi)


def slots():
    lane = lanes()
    return lane >> 5, lane & 31


def edge_tile(tile, i, low_plane, planes):
    slot, pos = slots()
    value = jnp.zeros((8, 128), F32)
    for g in range(4):
        plane = 6 * g + i - low_plane
        if not 0 <= plane < planes:
            continue
        own = tile(plane)
        here = slot == g
        value = jnp.where(here & (pos < 16), roll(own, 32 * g + 4, 1), value)
        value = jnp.where(here & (pos >= 16), roll(own, 32 * g + 28, 1), value)
    return jnp.where(((pos >= 4) & (pos < 12)) | ((pos >= 20) & (pos < 28)), value, 0.0)


def edge_own(vel, forc, rx_a, rx_b, eu, ef):
    rx = (rx_a, rx_b)
    for c in range(3):
        for i in range(6):
            for o in range(4):
                rows = slice(8 * o, 8 * o + 8)
                eu[c, i, rows] = edge_tile(lambda p: tile_of(vel, c, p, o, 4, rx, 0, None), i, 0, 24)
                ef[c, i, rows] = edge_tile(lambda p: tile_of(forc, c, p, o, 2, rx, 12, None), i, 2, 20)


def pack_z(phase, rx_a, rx_b, ry_a, ry_b, eu, ef, send_a, send_b, eu4, ef4, tiles):
    rx, ry = (rx_a, rx_b), (ry_a, ry_b)
    even, _, _ = position("gz")

    def put(index, lo, hi):
        send_a[index] = jnp.where(even, hi, lo)
        send_b[index] = jnp.where(even, lo, hi)

    lane = lanes()
    place = (lane & 31) >> 2
    for c in range(3):
        for i in range(6):
            eu4[c, i] = edge_tile(lambda p: tile_of(None, c, p, 4, 4, rx, 0, ry), i, 0, 24)
            ef4[c, i] = edge_tile(lambda p: tile_of(None, c, p, 4, 2, rx, 12, ry), i, 2, 20)
    for base, own, own4 in ((0, eu, eu4), (12, ef, ef4)):
        for w in range(12):
            lo = jnp.zeros((8, 128), F32)
            hi = lo
            for k in range(min(8, 90 - 8 * w)):
                n = 8 * w + k
                c, i, o = n // 30, n // 5 % 6, n % 5
                tile = own4[c, i] if o == 4 else own[c, i, 8 * o : 8 * o + 8]
                lo = jnp.where(place == k, roll(tile, 4 * k - 4, 1), lo)
                hi = jnp.where(place == k, roll(tile, 4 * k - 24, 1), hi)
            put(base + w, lo, hi)
    lo = jnp.zeros((8, 128), F32)
    hi = lo
    for j, tile in enumerate(phase_tiles(phase, rx, ry)):
        tiles[j] = tile
        lo = jnp.where(lane == j, roll(tile, j, 1), lo)
        hi = jnp.where(lane == j, roll(tile, j - 31, 1), hi)
    put(24, lo, hi)


def exact_dot(a, b):
    return jnp.dot(a, b, preferred_element_type=F32, precision=lax.Precision.HIGHEST)


def four(a, b, c, d):
    return (a + 3.0 * b + 3.0 * c + d) * 0.125


def put_rows(ref, index, o, value):
    ref[index + (slice(8 + 8 * o, 16 + 8 * o),)] = value
    if o == 0:
        ref[index + (slice(48, 56),)] = value
    if o == 4:
        ref[index + (slice(0, 8),)] = value


def tables(tiles, wide, pre, yld, creep, limit):
    block = lax.broadcasted_iota(jnp.int32, (128, 128), 0)
    spread = jnp.dot(
        jnp.concatenate(tiles, axis=0), (wide == block).astype(F32), preferred_element_type=F32
    )
    row = lax.broadcasted_iota(jnp.int32, (40, 16), 0)
    by = lax.broadcasted_iota(jnp.int32, (40, 16), 1)
    tall = (jnp.where(row < 32, row >> 2, jnp.where(row < 36, 8, 9)) == by).astype(F32)
    for b in range(6):
        phase = jnp.dot(tall, spread[16 * b : 16 * b + 16], preferred_element_type=F32)
        first = jnp.full(phase.shape, pre[0], F32)
        second = jnp.full(phase.shape, yld[0], F32)
        for k in range(1, 8):
            here = phase == float(k)
            first = jnp.where(here, pre[k], first)
            second = jnp.where(here, yld[k], second)
        creep[b] = first
        limit[b] = 0.5 * second


def viscosity_tile(u, creep, limit):
    d = []
    for c in range(3):
        mid = u(c, 0, 0)
        d.append((u(c, 1, 0) - u(c, -1, 0), u(c, 0, 1) - u(c, 0, -1), roll(mid, 127, 1) - roll(mid, 1, 1)))
    a01, a02, a12 = d[0][1] + d[1][0], d[0][2] + d[2][0], d[1][2] + d[2][1]
    own = d[0][0] * d[0][0] + d[1][1] * d[1][1] + d[2][2] * d[2][2]
    off = a01 * a01 + a02 * a02 + a12 * a12
    invariant = 1.0 + (own * 0.125 + off * 0.0625)
    return jnp.minimum(creep * jnp.exp(jnp.log(invariant) * (-1.0 / 3.0)), limit * lax.rsqrt(invariant))


def around(ref, index, o):
    head, p = index[:-1], index[-1]
    mid = ref[head + (p, slice(8 + 8 * o, 16 + 8 * o))]
    return mid, (
        ref[head + (p + 1, slice(8 + 8 * o, 16 + 8 * o))],
        ref[head + (p - 1, slice(8 + 8 * o, 16 + 8 * o))],
        ref[head + (p, slice(9 + 8 * o, 17 + 8 * o))],
        ref[head + (p, slice(7 + 8 * o, 15 + 8 * o))],
        roll(mid, 127, 1),
        roll(mid, 1, 1),
    )


def faces(v_ref, vx, o):
    mid, near = around(v_ref, (vx,), o)
    f = [mid + value for value in near]
    return mid, f, (f[0] + f[1]) + (f[2] + f[3]) + (f[4] + f[5])


def weighted(ref, index, o, f):
    mid, near = around(ref, index, o)
    total = f[0] * near[0]
    for k in range(1, 6):
        total = total + f[k] * near[k]
    return mid, total


def relax(mid_v, diag):
    return jnp.where(mid_v > 0.0, 0.8 / diag, 0.0)


def flags(axis):
    return tuple(flag.astype(F32) for flag in position(axis)[1:])


def main_work(
    vel, forc, phase_ref, rx_a, rx_b, ry_a, ry_b, pre, yld,
    v_ref, u2, residual, square,
    u_ref, f_ref, creep, limit, u1,
):
    rx, ry = (rx_a, rx_b), (ry_a, ry_b)
    lo_x, hi_x = flags("gx")
    lo_y, hi_y = flags("gy")
    for c in range(3):
        for p in range(24):
            for o in range(5):
                put_rows(u_ref, (c, p), o, tile_of(vel, c, p, o, 4, rx, 0, ry))
        for p in range(20):
            for o in range(5):
                f_ref[c, p, 8 * o : 8 * o + 8] = tile_of(forc, c, p, o, 2, rx, 12, ry)
    wide = lax.broadcasted_iota(jnp.int32, (128, 128), 1) >> 2
    tables(phase_tiles(phase_ref, rx, ry), wide, pre, yld, creep, limit)
    mask_y = jnp.where(subs() < 4, hi_y, lo_y)

    def viscosity(vx, _):
        mask_x = jnp.where(vx < 3, lo_x, jnp.where(vx >= 19, hi_x, 1.0))
        bx = (vx + 1) >> 2
        for o in range(5):
            value = viscosity_tile(
                lambda c, dx, dy: u_ref[c, vx + 1 + dx, 8 + 8 * o + dy : 16 + 8 * o + dy],
                creep[bx, 8 * o : 8 * o + 8], limit[bx, 8 * o : 8 * o + 8],
            )
            put_rows(v_ref, (vx,), o, value * (mask_y * mask_x if o == 4 else mask_x))
        return 0

    lax.fori_loop(0, 22, viscosity, 0)

    def sweep(source, target, first, first_u):
        def body(x, _):
            for o in range(5):
                mid_v, f, diag = faces(v_ref, x + first, o)
                rate = relax(mid_v, diag)
                for c in range(3):
                    mid, total = weighted(source, (c, x + first_u), o, f)
                    force = f_ref[c, x + first - 1, 8 * o : 8 * o + 8]
                    put_rows(target, (c, x), o, 0.2 * mid + rate * (2.0 * force + total))
            return 0

        return body

    lax.fori_loop(0, 20, sweep(u_ref, u1, 1, 2), 0)
    lax.fori_loop(0, 18, sweep(u1, u2, 2, 1), 0)

    def last(x, acc):
        for o in range(4):
            _, f, diag = faces(v_ref, x + 3, o)
            for c in range(3):
                mid, total = weighted(u2, (c, x + 1), o, f)
                value = f_ref[c, x + 2, 8 * o : 8 * o + 8] + 0.5 * (total - diag * mid)
                residual[c, x, 8 * o : 8 * o + 8] = value
                acc = acc + value * value
        return acc

    acc = lax.fori_loop(0, NX, last, jnp.zeros((8, 128), F32))
    lane = lanes()
    square[...] = jnp.where((lane >= 4) & (lane < 124), acc, 0.0)


def put_edge(ref, index, i, o, value):
    put_rows(ref, index + (i + 1,), o, value)


def wrap_planes(ref, lead):
    for index in lead:
        for r in range(7):
            rows = slice(8 * r, 8 * r + 8)
            ref[index + (0, rows)] = roll(ref[index + (6, rows)], 32, 1)
            ref[index + (7, rows)] = roll(ref[index + (1, rows)], -32, 1)


def edge_work(
    rz_a, rz_b, eu, ef, eu4, ef4, phases, square, pre, yld,
    v_out, u_out, r_out, total_out,
    u_ref, f_ref, creep, limit, creep_e, limit_e, v_ref, u1, u2,
):
    rz = (rz_a, rz_b)
    lo_x, hi_x = flags("gx")
    lo_y, hi_y = flags("gy")
    lo_z, hi_z = flags("gz")
    lane = lanes()
    slot, pos = slots()
    lead = ((0,), (1,), (2,))
    for base, own, own4 in ((0, eu, eu4), (12, ef, ef4)):
        for w in range(12):
            lo, hi = halo(rz, "gz", base + w)
            for k in range(min(8, 90 - 8 * w)):
                n = 8 * w + k
                c, i, o = n // 30, n // 5 % 6, n % 5
                tile = own4[c, i] if o == 4 else own[c, i, 8 * o : 8 * o + 8]
                tile = jnp.where(pos < 4, roll(lo, -4 * k, 1), tile)
                tile = jnp.where(pos >= 28, roll(hi, 28 - 4 * k, 1), tile)
                if base == 0:
                    put_edge(u_ref, (c,), i, o, tile)
                else:
                    f_ref[c, i, 8 * o : 8 * o + 8] = tile
    wrap_planes(u_ref, lead)

    lo, hi = halo(rz, "gz", 24)
    tiles = []
    for j in range(12):
        tile = jnp.where(lane == 32, roll(hi, 32 - j, 1), phases[j])
        tiles.append(jnp.where(lane == 33, roll(lo, 33 - j, 1), tile))
    at = lax.broadcasted_iota(jnp.int32, (128, 128), 1) & 31
    wide = jnp.where(at < 4, 33, jnp.where(at < 12, (at - 4) >> 2, jnp.where(at < 20, 127, 25 + (at >> 2))))
    tables(tiles, wide, pre, yld, creep, limit)
    for i in range(6):
        first, second = creep[i // 4], limit[i // 4]
        slot40 = lanes(40) >> 5
        for g in range(1, 4):
            b = (6 * g + i) // 4
            first = jnp.where(slot40 == g, creep[b], first)
            second = jnp.where(slot40 == g, limit[b], second)
        creep_e[i] = first
        limit_e[i] = second

    mask_z = jnp.where(pos < 4, lo_z, jnp.where(pos >= 28, hi_z, jnp.where((pos < 12) | (pos >= 20), 1.0, 0.0)))
    mask_y = jnp.where(subs() < 4, hi_y, lo_y)

    def viscosity(i, _):
        px = 6 * slot + i
        mask = mask_z * jnp.where(px < 4, lo_x, jnp.where(px >= 20, hi_x, 1.0))
        for o in range(5):
            value = viscosity_tile(
                lambda c, dx, dy: u_ref[c, i + 1 + dx, 8 + 8 * o + dy : 16 + 8 * o + dy],
                creep_e[i, 8 * o : 8 * o + 8], limit_e[i, 8 * o : 8 * o + 8],
            )
            value = value * (mask * mask_y if o == 4 else mask)
            put_edge(v_ref, (), i, o, value)
            v_out[i, 8 * o : 8 * o + 8] = value
        return 0

    lax.fori_loop(0, 6, viscosity, 0)
    wrap_planes(v_ref, ((),))

    def sweep(source, target):
        def body(i, _):
            for o in range(5):
                mid_v, f, diag = faces(v_ref, i + 1, o)
                rate = relax(mid_v, diag)
                for c in range(3):
                    mid, total = weighted(source, (c, i + 1), o, f)
                    force = f_ref[c, i, 8 * o : 8 * o + 8]
                    put_edge(target, (c,), i, o, 0.2 * mid + rate * (2.0 * force + total))
            return 0

        lax.fori_loop(0, 6, body, 0)
        wrap_planes(target, lead)

    sweep(u_ref, u1)
    sweep(u1, u2)

    def last(i, acc):
        px = 6 * slot + i
        count = (px >= 4) & (px < 20) & (((pos >= 4) & (pos < 8)) | ((pos >= 24) & (pos < 28)))
        for o in range(4):
            _, f, diag = faces(v_ref, i + 1, o)
            for c in range(3):
                mid, total = weighted(u2, (c, i + 1), o, f)
                value = f_ref[c, i, 8 * o : 8 * o + 8] + 0.5 * (total - diag * mid)
                r_out[c, i, 8 * o : 8 * o + 8] = value
                u_out[c, i, 8 * o : 8 * o + 8] = mid
                acc = acc + jnp.where(count, value * value, 0.0)
        return acc

    acc = lax.fori_loop(0, 6, last, square[...])
    total = jnp.sum(jnp.sum(acc, axis=1, keepdims=True), axis=0, keepdims=True)
    total_out[...] = jnp.broadcast_to(total, (1, 128))


def band(rows, row_z, col_m):
    row = row_z(lax.broadcasted_iota(jnp.int32, (rows, 128), 0))
    col = col_m(lax.broadcasted_iota(jnp.int32, (rows, 128), 1))
    at = row - 2 * col + 1
    return jnp.where((at == 0) | (at == 3), 0.125, jnp.where((at == 1) | (at == 2), 0.375, 0.0)).astype(F32)


def merge(own, edge, g):
    lane = lanes()
    value = jnp.where(lane < 4, roll(edge, -32 * g - 4, 1), own)
    return jnp.where(lane >= 124, roll(edge, 100 - 32 * g, 1), value)


def collect(
    v_ref, u2, residual_in, ve, ue, re,
    smoothed, visc_out, one_out, two_out, residual, partial,
    v_m, v_s, w_m, w_s, y1, c1, t2, t3,
):
    lo_x, hi_x = flags("gx")
    lo_y, hi_y = flags("gy")
    lo_z, hi_z = flags("gz")
    lane = lanes()
    for vx in range(22):
        g, i = (vx + 1) // 6, (vx + 1) % 6
        for o in range(5):
            edge = ve[i, 8 * o : 8 * o + 8]
            value = merge(v_ref[vx, 8 + 8 * o : 16 + 8 * o], edge, g)
            put_rows(v_m, (vx,), o, value)
            side = jnp.where(lane < 4, roll(edge, -28 - 32 * g, 1), 0.0)
            put_rows(v_s, (vx,), o, jnp.where(lane >= 124, roll(edge, 124 - 32 * g, 1), side))
            if 3 <= vx < 19 and o < 4:
                visc_out[vx - 3, 8 * o : 8 * o + 8] = value
    for x in range(NX):
        g, i = (x + 4) // 6, (x + 4) % 6
        for c in range(3):
            for o in range(4):
                rows = slice(8 * o, 8 * o + 8)
                smoothed[c, x, rows] = merge(u2[c, x + 1, 8 + 8 * o : 16 + 8 * o], ue[c, i, rows], g)
                residual[c, x, rows] = merge(residual_in[c, x, rows], re[c, i, rows], g)

    def coarse_x(k, _):
        w_m[k] = four(v_m[2 * k], v_m[2 * k + 1], v_m[2 * k + 2], v_m[2 * k + 3])
        w_s[k] = four(v_s[2 * k], v_s[2 * k + 1], v_s[2 * k + 2], v_s[2 * k + 3])
        return 0

    lax.fori_loop(0, 10, coarse_x, 0)
    y1[...] = jnp.zeros(y1.shape, F32)
    for k in range(10):
        for ref, at in ((w_m, 0), (w_s, 128)):
            y1[k, 0:18, at : at + 128] = four(*(ref[k, pl.ds(5 + i, 18, stride=2)] for i in range(4)))
    band1 = band(256, lambda r: jnp.where(r < 192, r, r - 256), lambda m: jnp.where(m < 65, m, jnp.where(m == 65, -1, 1000)))
    coarse = exact_dot(y1[...].reshape(240, 256), band1).reshape(10, 24, 128)
    row24, lane24 = subs(24), lanes(24)
    mask_yz = jnp.where(row24 == 0, lo_y, jnp.where(row24 == 17, hi_y, 1.0)) * jnp.where(
        lane24 == 64, hi_z, jnp.where(lane24 == 65, lo_z, 1.0)
    )
    for k in range(10):
        mask = mask_yz * (lo_x if k == 0 else hi_x if k == 9 else 1.0)
        c1[k] = coarse[k] * mask
    for k in range(8):
        one_out[k] = c1[k + 1, 1:17, 0:64]
    rows = []
    for k in range(4):
        t2[...] = four(c1[2 * k], c1[2 * k + 1], c1[2 * k + 2], c1[2 * k + 3])
        rows.append(four(*(t2[pl.ds(i, 8, stride=2)] for i in range(4))))
    band2 = band(128, lambda r: jnp.where(r < 65, r, jnp.where(r == 65, -1, 100000)), lambda m: jnp.where(m < 32, m, 1000))
    coarse = exact_dot(jnp.concatenate(rows, axis=0), band2)
    planes = [coarse[8 * k : 8 * k + 8] for k in range(4)]
    for k in range(4):
        two_out[k] = planes[k][:, 0:32]
    thirds = (
        0.125 * planes[0],
        0.125 * (3.0 * planes[0] + 3.0 * planes[1] + planes[2]),
        0.125 * (planes[1] + 3.0 * planes[2] + 3.0 * planes[3]),
        0.125 * planes[3],
    )
    rows = []
    t3[...] = jnp.zeros(t3.shape, F32)
    for k in range(4):
        t3[4:12] = thirds[k]
        rows.append(four(*(t3[pl.ds(1 + i, 8, stride=2)] for i in range(4))))
    band3 = band(128, lambda r: jnp.where(r < 32, r, 100000), lambda m: jnp.where(m < 18, m - 1, 1000))
    coarse = exact_dot(jnp.concatenate(rows, axis=0), band3)
    for k in range(4):
        partial[k] = coarse[8 * k : 8 * k + 8]


def with_sum(tile, total):
    row = lax.broadcasted_iota(jnp.int32, tile.shape, tile.ndim - 2)
    return jnp.where(row == 7, total, tile)


def finish(partial, total):
    even, has_lo, has_hi = position("gx")
    got_a = pair_a(with_sum(jnp.where(even, partial[3], partial[0]), total), "gx")
    total = total + got_a[7:8]
    got_b = pair_b(with_sum(jnp.where(even, partial[0], partial[3]), total), "gx")
    total = total + got_b[7:8]
    lo, hi = jnp.where(even, got_b, got_a), jnp.where(even, got_a, got_b)
    inner = jnp.stack(
        [partial[1] + jnp.where(has_lo, lo, 0.0), partial[2] + jnp.where(has_hi, hi, 0.0)]
    )
    even, has_lo, has_hi = position("gy")
    got_a = pair_a(with_sum(inner, total), "gy")
    total = total + got_a[0, 7:8]
    got_b = pair_b(with_sum(inner, total), "gy")
    total = total + got_b[0, 7:8]
    lo, hi = jnp.where(even, got_b, got_a), jnp.where(even, got_a, got_b)
    row = lax.broadcasted_iota(jnp.int32, inner.shape, 1)
    inner = (
        inner
        + jnp.where((row == 1) & has_lo, jnp.roll(lo, -4, 1), 0.0)
        + jnp.where((row == 4) & has_hi, jnp.roll(hi, 4, 1), 0.0)
    )
    even, has_lo, has_hi = position("gz")
    got_a = pair_a(with_sum(inner, total), "gz")
    total = total + got_a[0, 7:8]
    got_b = pair_b(with_sum(inner, total), "gz")
    total = total + got_b[0, 7:8]
    lo, hi = jnp.where(even, got_b, got_a), jnp.where(even, got_a, got_b)
    three = inner[:, 1:5, 1:17]
    z = lax.broadcasted_iota(jnp.int32, three.shape, 2)
    three = (
        three
        + jnp.where((z == 0) & has_lo, lo[:, 1:5, 17:18], 0.0)
        + jnp.where((z == 15) & has_hi, hi[:, 1:5, 0:1], 0.0)
    )
    return total[0, 0], three


def far(axis, total):
    count = lax.axis_size(axis)
    if count == 4:
        return jnp.zeros_like(total)
    return lax.ppermute(total, axis, [(i, (i + count // 2) % count) for i in range(count)])


def pack(kernel, shape, name, *args):
    return pl.pallas_call(
        kernel, out_shape=[sds(*shape)] * 2, in_specs=[VMEM] * len(args), out_specs=[VMEM] * 2,
        compiler_params=params(), name=name,
    )(*args)


def per_device(velocity, forcing, phase_block, prefactor, yield_stress):
    phase = jnp.pad(phase_block.astype(F32), ((0, 0), (0, 0), (0, 96)))
    own = (velocity, forcing, phase)
    send_a, send_b = pack(pack_x, (19, 32, 128), "pack_x", *own)
    rx = (pair_a(send_a, "gx"), pair_b(send_b, "gx"))
    send_a, send_b = pack(pack_y, (52, 8, 128), "pack_y", *own, *rx)
    ry = (pair_a(send_a, "gy"), pair_b(send_b, "gy"))
    eu, ef = pl.pallas_call(
        edge_own, out_shape=[sds(3, 6, 32, 128)] * 2, in_specs=[VMEM] * 4, out_specs=[VMEM] * 2,
        compiler_params=params(), cost_estimate=cost(3 << 23), name="edge_own",
    )(velocity, forcing, *rx)
    send_a, send_b, eu4, ef4, tiles = pl.pallas_call(
        pack_z, out_shape=[sds(25, 8, 128)] * 2 + [sds(3, 6, 8, 128)] * 2 + [sds(12, 8, 128)],
        in_specs=[VMEM] * 7, out_specs=[VMEM] * 5, compiler_params=params(), name="pack_z",
    )(phase, *rx, *ry, eu, ef)
    rz = (pair_a(send_a, "gz"), pair_b(send_b, "gz"))
    v, u2, res, square = pl.pallas_call(
        main_work,
        out_shape=[sds(22, 56, 128), sds(3, 18, 56, 128), sds(3, NX, NY, NZ), sds(8, 128)],
        in_specs=[VMEM] * 7 + [SMEM] * 2, out_specs=[VMEM] * 4,
        scratch_shapes=[
            pltpu.VMEM((3, 24, 56, 128), F32), pltpu.VMEM((3, 20, 40, 128), F32),
            pltpu.VMEM((6, 40, 128), F32), pltpu.VMEM((6, 40, 128), F32), pltpu.VMEM((3, 20, 56, 128), F32),
        ],
        compiler_params=params(), cost_estimate=cost(1 << 25), name="main_work",
    )(*own, *rx, *ry, prefactor, yield_stress)
    ve, ue, re, total = pl.pallas_call(
        edge_work,
        out_shape=[sds(6, 40, 128), sds(3, 6, 32, 128), sds(3, 6, 32, 128), sds(1, 128)],
        in_specs=[VMEM] * 8 + [SMEM] * 2, out_specs=[VMEM] * 4,
        scratch_shapes=[
            pltpu.VMEM((3, 8, 56, 128), F32), pltpu.VMEM((3, 6, 40, 128), F32),
            *[pltpu.VMEM((6, 40, 128), F32)] * 4,
            pltpu.VMEM((8, 56, 128), F32), pltpu.VMEM((3, 8, 56, 128), F32), pltpu.VMEM((3, 8, 56, 128), F32),
        ],
        compiler_params=params(), cost_estimate=cost(1 << 23), name="edge_work",
    )(*rz, eu, ef, eu4, ef4, tiles, square, prefactor, yield_stress)
    total = total + far("gx", total)
    total = total + far("gz", total)
    smoothed, visc, one, two, residual, partial = pl.pallas_call(
        collect,
        out_shape=[
            sds(3, NX, NY, NZ), sds(NX, NY, NZ), sds(8, 16, 64), sds(4, 8, 32), sds(3, NX, NY, NZ), sds(4, 8, 128),
        ],
        in_specs=[VMEM] * 6, out_specs=[VMEM] * 6,
        scratch_shapes=[
            pltpu.VMEM((22, 56, 128), F32), pltpu.VMEM((22, 56, 128), F32),
            pltpu.VMEM((10, 56, 128), F32), pltpu.VMEM((10, 56, 128), F32), pltpu.VMEM((10, 24, 256), F32),
            pltpu.VMEM((10, 24, 128), F32), pltpu.VMEM((24, 128), F32), pltpu.VMEM((24, 128), F32),
        ],
        compiler_params=params(), cost_estimate=cost(1 << 23), name="collect",
    )(v, u2, res, ve, ue, re)
    total, three = finish(partial, total)
    cells = 3.0 * NX * NY * NZ
    for axis in AX:
        cells = cells * lax.axis_size(axis)
    return smoothed, visc, one, two, three, residual, jnp.sqrt(total / cells)


def solution(mesh):
    field, cell = P(None, *AX), P(*AX)
    return jax.shard_map(
        per_device,
        mesh=mesh,
        in_specs=(field, field, cell, P(), P()),
        out_specs=(field, cell, cell, cell, cell, field, P()),
        check_vma=False,
    )
```

```python
import functools

import jax
import jax.numpy as jnp
from jax import lax
from jax.experimental import pallas as pl
from jax.experimental.pallas import tpu as pltpu
from jax.sharding import PartitionSpec as P

F32 = jnp.float32
BLOCK = 4
AX = ("gx", "gy", "gz")
NX, NY, NZ = 16, 32, 128
VMEM = pl.BlockSpec(memory_space=pltpu.VMEM)
LIM = 8
SMEM = pl.BlockSpec(memory_space=pltpu.SMEM)


def sds(*shape):
    return jax.ShapeDtypeStruct(shape, F32)


def position(axis):
    index = lax.axis_index(axis)
    return lax.rem(index, 2) == 0, index > 0, index < lax.axis_size(axis) - 1


def lanes(rows=8, width=128):
    return lax.broadcasted_iota(jnp.int32, (rows, width), 1)


def subs(rows=8, width=128):
    return lax.broadcasted_iota(jnp.int32, (rows, width), 0)


def roll(value, shift, axis):
    size = value.shape[axis]
    shift = shift % size
    return pltpu.roll(value, shift, axis) if shift else value


def pair_a(value, axis):
    count = lax.axis_size(axis)
    return lax.ppermute(value, axis, [(i, i ^ 1) for i in range(count)])


def pair_b(value, axis):
    count = lax.axis_size(axis)
    return lax.ppermute(
        value, axis, [(i, (i + 1) % count if i % 2 else (i - 1) % count) for i in range(count)]
    )


def params(mib):
    return pltpu.CompilerParams(vmem_limit_bytes=mib << 20)


def cost(flops):
    return pl.CostEstimate(flops=flops, bytes_accessed=1 << 20, transcendentals=0)


def put_pair(pair, axis, index, lo, hi):
    even = position(axis)[0]
    pair[0][index] = jnp.where(even, hi, lo)
    pair[1][index] = jnp.where(even, lo, hi)


def pack_rows4(pair, index, tile, p, q):
    sub = subs()
    lo = jnp.where(sub < 4, tile(p, 0), roll(tile(q, 0), 4, 0))
    hi = jnp.where(sub < 4, roll(tile(p, 3), 4, 0), tile(q, 3))
    put_pair(pair, "gy", index, lo, hi)


def pack_rows2(pair, index, tile, planes):
    sub = subs()
    lo = tile(planes[0], 0)
    hi = roll(tile(planes[0], 3), 2, 0)
    for k in range(1, 4):
        here = (sub >> 1) == k
        lo = jnp.where(here, roll(tile(planes[k], 0), 2 * k, 0), lo)
        hi = jnp.where(here, roll(tile(planes[k], 3), 2 * k + 2, 0), hi)
    put_pair(pair, "gy", index, lo, hi)


def pack_phase(pair, index, tiles):
    sub = subs()
    lo = jnp.zeros((8, 128), F32)
    hi = lo
    for b, tile in enumerate(tiles):
        lo = jnp.where(sub == b, tile[0:1], lo)
        hi = jnp.where(sub == b, tile[7:8], hi)
    put_pair(pair, "gy", index, lo, hi)


def pack_xy(vel, forc, blocks, send_a, send_b, own_a, own_b, phase):
    even, _, _ = position("gx")
    phase[...] = jnp.zeros(phase.shape, F32)
    for b in range(4):
        phase[b, :, 0:32] = blocks[b].astype(F32)
    for out, first in ((send_a, jnp.where(even, 1, 0)), (send_b, jnp.where(even, 0, 1))):
        for c in range(3):
            for i in range(4):
                out[4 * c + i] = vel[c, 12 * first + i]
            for i in range(2):
                out[12 + 2 * c + i] = forc[c, 14 * first + i]
        out[18, 0:8] = phase[3 * first]
    pair = (own_a, own_b)
    for c in range(3):
        for g in range(8):
            pack_rows4(pair, 8 * c + g, lambda p, o: vel[c, p, 8 * o : 8 * o + 8], g, g + 8)
        for g in range(4):
            pack_rows2(pair, 24 + 4 * c + g, lambda p, o: forc[c, p, 8 * o : 8 * o + 8], [g + 4 * k for k in range(4)])
    pack_phase(pair, 36, [phase[b] for b in range(4)])


def pack_y(rx_a, rx_b, corner_a, corner_b):
    rx, pair = (rx_a, rx_b), (corner_a, corner_b)
    for c in range(3):
        for i in range(4):
            pack_rows4(pair, 4 * c + i, lambda p, o: tile_of(None, c, p, o, 4, rx, 0, None), i, 20 + i)
        pack_rows2(pair, 12 + c, lambda p, o: tile_of(None, c, p, o, 2, rx, 12, None), [0, 1, 18, 19])
    pack_phase(pair, 15, [phase_rows(None, rx, 0), phase_rows(None, rx, 5)])


def halo(pair, axis, index):
    even, has_lo, has_hi = position(axis)
    a, b = pair[0][index], pair[1][index]
    lo = jnp.where(has_lo, jnp.where(even, b, a), 0.0)
    hi = jnp.where(has_hi, jnp.where(even, a, b), 0.0)
    return lo, hi


def tile_of(own, c, plane, o, width, rx, base, ry):
    rows = slice(8 * o, 8 * o + 8)
    if o == 4:
        sub = subs()
        inside = width <= plane < NX + width
        pair = ry[0] if inside else ry[1]
        at = plane - width if inside else plane if plane < width else plane - NX
        if width == 4:
            half = 8 if inside else 4
            lo, hi = halo(pair, "gy", half * c + at % half)
            if at < half:
                return jnp.where(sub < 4, hi, roll(lo, 4, 0))
            return jnp.where(sub < 4, roll(hi, 4, 0), lo)
        lo, hi = halo(pair, "gy", 24 + 4 * c + at % 4 if inside else 12 + c)
        k = at // 4 if inside else at
        return jnp.where(sub < 4, roll(hi, -2 * k, 0), roll(lo, 6 - 2 * k, 0))
    if plane < width:
        return halo(rx, "gx", (base + width * c + plane, rows))[0]
    if plane >= NX + width:
        return halo(rx, "gx", (base + width * c + plane - NX - width, rows))[1]
    return own[c, plane - width, rows]


def phase_rows(phase, rx, b):
    if b == 0:
        return halo(rx, "gx", (18, slice(0, 8)))[0]
    if b == 5:
        return halo(rx, "gx", (18, slice(0, 8)))[1]
    return phase[b - 1]


def phase_tiles(phase, rx, ry):
    own, corner = halo(ry[0], "gy", 36), halo(ry[1], "gy", 15)
    sub = subs()
    tiles = []
    for b in range(6):
        tiles.append(phase_rows(phase, rx, b))
        lo, hi = own if 0 < b < 5 else corner
        row = b - 1 if 0 < b < 5 else b // 5
        outer = jnp.where(sub == 0, hi[row : row + 1], jnp.where(sub == 1, lo[row : row + 1], 0.0))
        tiles.append(outer)
    return tiles


def slots():
    lane = lanes()
    return lane >> 5, lane & 31


def edge_tile(tile, i, low_plane, planes):
    slot, pos = slots()
    value = jnp.zeros((8, 128), F32)
    for g in range(4):
        plane = 6 * g + i - low_plane
        if not 0 <= plane < planes:
            continue
        own = tile(plane)
        here = slot == g
        value = jnp.where(here & (pos < 16), roll(own, 32 * g + 4, 1), value)
        value = jnp.where(here & (pos >= 16), roll(own, 32 * g + 28, 1), value)
    return jnp.where(((pos >= 4) & (pos < 12)) | ((pos >= 20) & (pos < 28)), value, 0.0)


def edge_own(vel, forc, rx_a, rx_b, eu, ef):
    rx = (rx_a, rx_b)
    for c in range(3):
        for i in range(6):
            for o in range(4):
                rows = slice(8 * o, 8 * o + 8)
                eu[c, i, rows] = edge_tile(lambda p: tile_of(vel, c, p, o, 4, rx, 0, None), i, 0, 24)
                ef[c, i, rows] = edge_tile(lambda p: tile_of(forc, c, p, o, 2, rx, 12, None), i, 2, 20)


def pack_z(phase, rx_a, rx_b, ryo_a, ryo_b, ryc_a, ryc_b, eu, ef, send_a, send_b, eu4, ef4, tiles):
    rx, ry = (rx_a, rx_b), ((ryo_a, ryo_b), (ryc_a, ryc_b))
    even, _, _ = position("gz")

    def put(index, lo, hi):
        send_a[index] = jnp.where(even, hi, lo)
        send_b[index] = jnp.where(even, lo, hi)

    lane = lanes()
    place = (lane & 31) >> 2
    for c in range(3):
        for i in range(6):
            eu4[c, i] = edge_tile(lambda p: tile_of(None, c, p, 4, 4, rx, 0, ry), i, 0, 24)
            ef4[c, i] = edge_tile(lambda p: tile_of(None, c, p, 4, 2, rx, 12, ry), i, 2, 20)
    for base, own, own4 in ((0, eu, eu4), (12, ef, ef4)):
        for w in range(12):
            lo = jnp.zeros((8, 128), F32)
            hi = lo
            for k in range(min(8, 90 - 8 * w)):
                n = 8 * w + k
                c, i, o = n // 30, n // 5 % 6, n % 5
                tile = own4[c, i] if o == 4 else own[c, i, 8 * o : 8 * o + 8]
                lo = jnp.where(place == k, roll(tile, 4 * k - 4, 1), lo)
                hi = jnp.where(place == k, roll(tile, 4 * k - 24, 1), hi)
            put(base + w, lo, hi)
    lo = jnp.zeros((8, 128), F32)
    hi = lo
    for j, tile in enumerate(phase_tiles(phase, rx, ry)):
        tiles[j] = tile
        lo = jnp.where(lane == j, roll(tile, j, 1), lo)
        hi = jnp.where(lane == j, roll(tile, j - 31, 1), hi)
    put(24, lo, hi)


def exact_dot(a, b):
    return jnp.dot(a, b, preferred_element_type=F32, precision=lax.Precision.HIGHEST)


def four(a, b, c, d):
    return (a + 3.0 * b + 3.0 * c + d) * 0.125


def put_rows(ref, index, o, value):
    ref[index + (slice(8 + 8 * o, 16 + 8 * o),)] = value
    if o == 0:
        ref[index + (slice(48, 56),)] = value
    if o == 4:
        ref[index + (slice(0, 8),)] = value


def tables(tiles, wide, pre, yld, creep, limit):
    block = lax.broadcasted_iota(jnp.int32, (128, 128), 0)
    spread = jnp.dot(
        jnp.concatenate(tiles, axis=0), (wide == block).astype(F32), preferred_element_type=F32
    )
    row = lax.broadcasted_iota(jnp.int32, (40, 16), 0)
    by = lax.broadcasted_iota(jnp.int32, (40, 16), 1)
    tall = (jnp.where(row < 32, row >> 2, jnp.where(row < 36, 8, 9)) == by).astype(F32)
    for b in range(6):
        phase = jnp.dot(tall, spread[16 * b : 16 * b + 16], preferred_element_type=F32)
        first = jnp.full(phase.shape, pre[0], F32)
        second = jnp.full(phase.shape, yld[0], F32)
        for k in range(1, 8):
            here = phase == float(k)
            first = jnp.where(here, pre[k], first)
            second = jnp.where(here, yld[k], second)
        creep[b] = first
        limit[b] = 0.5 * second


def viscosity_tile(u, creep, limit):
    d = []
    for c in range(3):
        mid = u(c, 0, 0)
        d.append((u(c, 1, 0) - u(c, -1, 0), u(c, 0, 1) - u(c, 0, -1), roll(mid, 127, 1) - roll(mid, 1, 1)))
    a01, a02, a12 = d[0][1] + d[1][0], d[0][2] + d[2][0], d[1][2] + d[2][1]
    own = d[0][0] * d[0][0] + d[1][1] * d[1][1] + d[2][2] * d[2][2]
    off = a01 * a01 + a02 * a02 + a12 * a12
    invariant = 1.0 + (own * 0.125 + off * 0.0625)
    return jnp.minimum(creep * jnp.exp(jnp.log(invariant) * (-1.0 / 3.0)), limit * lax.rsqrt(invariant))


def around(ref, index, o):
    head, p = index[:-1], index[-1]
    mid = ref[head + (p, slice(8 + 8 * o, 16 + 8 * o))]
    return mid, (
        ref[head + (p + 1, slice(8 + 8 * o, 16 + 8 * o))],
        ref[head + (p - 1, slice(8 + 8 * o, 16 + 8 * o))],
        ref[head + (p, slice(9 + 8 * o, 17 + 8 * o))],
        ref[head + (p, slice(7 + 8 * o, 15 + 8 * o))],
        roll(mid, 127, 1),
        roll(mid, 1, 1),
    )


def faces(v_ref, vx, o):
    mid, near = around(v_ref, (vx,), o)
    f = [mid + value for value in near]
    return mid, f, (f[0] + f[1]) + (f[2] + f[3]) + (f[4] + f[5])


def weighted(ref, index, o, f):
    mid, near = around(ref, index, o)
    total = f[0] * near[0]
    for k in range(1, 6):
        total = total + f[k] * near[k]
    return mid, total


def relax(mid_v, diag):
    return jnp.where(mid_v > 0.0, 0.8 / diag, 0.0)


def flags(axis):
    return tuple(flag.astype(F32) for flag in position(axis)[1:])


def main_work(
    vel, forc, phase_ref, rx_a, rx_b, ryo_a, ryo_b, ryc_a, ryc_b, pre, yld,
    v_ref, u2, residual, square,
    u_ref, f_ref, creep, limit, u1,
):
    rx, ry = (rx_a, rx_b), ((ryo_a, ryo_b), (ryc_a, ryc_b))
    lo_x, hi_x = flags("gx")
    lo_y, hi_y = flags("gy")
    for c in range(3):
        for p in range(24):
            for o in range(5):
                put_rows(u_ref, (c, p), o, tile_of(vel, c, p, o, 4, rx, 0, ry))
        for p in range(20):
            for o in range(5):
                f_ref[c, p, 8 * o : 8 * o + 8] = tile_of(forc, c, p, o, 2, rx, 12, ry)
    wide = lax.broadcasted_iota(jnp.int32, (128, 128), 1) >> 2
    tables(phase_tiles(phase_ref, rx, ry), wide, pre, yld, creep, limit)
    mask_y = jnp.where(subs() < 4, hi_y, lo_y)

    def viscosity(vx, _):
        mask_x = jnp.where(vx < 3, lo_x, jnp.where(vx >= 19, hi_x, 1.0))
        bx = (vx + 1) >> 2
        for o in range(5):
            value = viscosity_tile(
                lambda c, dx, dy: u_ref[c, vx + 1 + dx, 8 + 8 * o + dy : 16 + 8 * o + dy],
                creep[bx, 8 * o : 8 * o + 8], limit[bx, 8 * o : 8 * o + 8],
            )
            put_rows(v_ref, (vx,), o, value * (mask_y * mask_x if o == 4 else mask_x))
        return 0

    lax.fori_loop(0, 22, viscosity, 0, unroll=2)

    def sweep(source, target, first, first_u):
        def body(x, _):
            for o in range(5):
                mid_v, f, diag = faces(v_ref, x + first, o)
                rate = relax(mid_v, diag)
                for c in range(3):
                    mid, total = weighted(source, (c, x + first_u), o, f)
                    force = f_ref[c, x + first - 1, 8 * o : 8 * o + 8]
                    put_rows(target, (c, x), o, 0.2 * mid + rate * (2.0 * force + total))
            return 0

        return body

    lax.fori_loop(0, 20, sweep(u_ref, u1, 1, 2), 0, unroll=2)
    lax.fori_loop(0, 18, sweep(u1, u2, 2, 1), 0, unroll=2)

    def last(x, acc):
        for o in range(4):
            _, f, diag = faces(v_ref, x + 3, o)
            for c in range(3):
                mid, total = weighted(u2, (c, x + 1), o, f)
                value = f_ref[c, x + 2, 8 * o : 8 * o + 8] + 0.5 * (total - diag * mid)
                residual[c, x, 8 * o : 8 * o + 8] = value
                acc = acc + value * value
        return acc

    acc = lax.fori_loop(0, NX, last, jnp.zeros((8, 128), F32), unroll=2)
    lane = lanes()
    square[...] = jnp.where((lane >= 4) & (lane < 124), acc, 0.0)


def put_edge(ref, index, i, o, value):
    put_rows(ref, index + (i + 1,), o, value)


def wrap_planes(ref, lead):
    for index in lead:
        for r in range(7):
            rows = slice(8 * r, 8 * r + 8)
            ref[index + (0, rows)] = roll(ref[index + (6, rows)], 32, 1)
            ref[index + (7, rows)] = roll(ref[index + (1, rows)], -32, 1)


def edge_work(
    rz_a, rz_b, eu, ef, eu4, ef4, phases, square, pre, yld,
    v_out, u_out, r_out, total_out,
    u_ref, f_ref, creep, limit, creep_e, limit_e, v_ref, u1, u2,
):
    rz = (rz_a, rz_b)
    lo_x, hi_x = flags("gx")
    lo_y, hi_y = flags("gy")
    lo_z, hi_z = flags("gz")
    lane = lanes()
    slot, pos = slots()
    lead = ((0,), (1,), (2,))
    for base, own, own4 in ((0, eu, eu4), (12, ef, ef4)):
        for w in range(12):
            lo, hi = halo(rz, "gz", base + w)
            for k in range(min(8, 90 - 8 * w)):
                n = 8 * w + k
                c, i, o = n // 30, n // 5 % 6, n % 5
                tile = own4[c, i] if o == 4 else own[c, i, 8 * o : 8 * o + 8]
                tile = jnp.where(pos < 4, roll(lo, -4 * k, 1), tile)
                tile = jnp.where(pos >= 28, roll(hi, 28 - 4 * k, 1), tile)
                if base == 0:
                    put_edge(u_ref, (c,), i, o, tile)
                else:
                    f_ref[c, i, 8 * o : 8 * o + 8] = tile
    wrap_planes(u_ref, lead)

    lo, hi = halo(rz, "gz", 24)
    tiles = []
    for j in range(12):
        tile = jnp.where(lane == 32, roll(hi, 32 - j, 1), phases[j])
        tiles.append(jnp.where(lane == 33, roll(lo, 33 - j, 1), tile))
    at = lax.broadcasted_iota(jnp.int32, (128, 128), 1) & 31
    wide = jnp.where(at < 4, 33, jnp.where(at < 12, (at - 4) >> 2, jnp.where(at < 20, 127, 25 + (at >> 2))))
    tables(tiles, wide, pre, yld, creep, limit)
    for i in range(6):
        first, second = creep[i // 4], limit[i // 4]
        slot40 = lanes(40) >> 5
        for g in range(1, 4):
            b = (6 * g + i) // 4
            first = jnp.where(slot40 == g, creep[b], first)
            second = jnp.where(slot40 == g, limit[b], second)
        creep_e[i] = first
        limit_e[i] = second

    mask_z = jnp.where(pos < 4, lo_z, jnp.where(pos >= 28, hi_z, jnp.where((pos < 12) | (pos >= 20), 1.0, 0.0)))
    mask_y = jnp.where(subs() < 4, hi_y, lo_y)

    def viscosity(i, _):
        px = 6 * slot + i
        mask = mask_z * jnp.where(px < 4, lo_x, jnp.where(px >= 20, hi_x, 1.0))
        for o in range(5):
            value = viscosity_tile(
                lambda c, dx, dy: u_ref[c, i + 1 + dx, 8 + 8 * o + dy : 16 + 8 * o + dy],
                creep_e[i, 8 * o : 8 * o + 8], limit_e[i, 8 * o : 8 * o + 8],
            )
            value = value * (mask * mask_y if o == 4 else mask)
            put_edge(v_ref, (), i, o, value)
            v_out[i, 8 * o : 8 * o + 8] = value
        return 0

    lax.fori_loop(0, 6, viscosity, 0, unroll=3)
    wrap_planes(v_ref, ((),))

    def sweep(source, target):
        def body(i, _):
            for o in range(5):
                mid_v, f, diag = faces(v_ref, i + 1, o)
                rate = relax(mid_v, diag)
                for c in range(3):
                    mid, total = weighted(source, (c, i + 1), o, f)
                    force = f_ref[c, i, 8 * o : 8 * o + 8]
                    put_edge(target, (c,), i, o, 0.2 * mid + rate * (2.0 * force + total))
            return 0

        lax.fori_loop(0, 6, body, 0, unroll=3)
        wrap_planes(target, lead)

    sweep(u_ref, u1)
    sweep(u1, u2)

    def last(i, acc):
        px = 6 * slot + i
        count = (px >= 4) & (px < 20) & (((pos >= 4) & (pos < 8)) | ((pos >= 24) & (pos < 28)))
        for o in range(4):
            _, f, diag = faces(v_ref, i + 1, o)
            for c in range(3):
                mid, total = weighted(u2, (c, i + 1), o, f)
                value = f_ref[c, i, 8 * o : 8 * o + 8] + 0.5 * (total - diag * mid)
                r_out[c, i, 8 * o : 8 * o + 8] = value
                u_out[c, i, 8 * o : 8 * o + 8] = mid
                acc = acc + jnp.where(count, value * value, 0.0)
        return acc

    acc = lax.fori_loop(0, 6, last, square[...], unroll=3)
    total = jnp.sum(jnp.sum(acc, axis=1, keepdims=True), axis=0, keepdims=True)
    total_out[...] = jnp.broadcast_to(total, (1, 128))


def band(rows, row_z, col_m):
    row = row_z(lax.broadcasted_iota(jnp.int32, (rows, 128), 0))
    col = col_m(lax.broadcasted_iota(jnp.int32, (rows, 128), 1))
    at = row - 2 * col + 1
    return jnp.where((at == 0) | (at == 3), 0.125, jnp.where((at == 1) | (at == 2), 0.375, 0.0)).astype(F32)


def merge(own, edge, g):
    lane = lanes()
    value = jnp.where(lane < 4, roll(edge, -32 * g - 4, 1), own)
    return jnp.where(lane >= 124, roll(edge, 100 - 32 * g, 1), value)


def collect(
    v_ref, u2, residual_in, ve, ue, re,
    smoothed, visc_out, one_out, two_out, residual, partial,
    v_m, v_s, w_m, w_s, y1, c1, t2, t3,
):
    lo_x, hi_x = flags("gx")
    lo_y, hi_y = flags("gy")
    lo_z, hi_z = flags("gz")
    lane = lanes()
    for vx in range(22):
        g, i = (vx + 1) // 6, (vx + 1) % 6
        for o in range(5):
            edge = ve[i, 8 * o : 8 * o + 8]
            value = merge(v_ref[vx, 8 + 8 * o : 16 + 8 * o], edge, g)
            put_rows(v_m, (vx,), o, value)
            side = jnp.where(lane < 4, roll(edge, -28 - 32 * g, 1), 0.0)
            put_rows(v_s, (vx,), o, jnp.where(lane >= 124, roll(edge, 124 - 32 * g, 1), side))
            if 3 <= vx < 19 and o < 4:
                visc_out[vx - 3, 8 * o : 8 * o + 8] = value
    for x in range(NX):
        g, i = (x + 4) // 6, (x + 4) % 6
        for c in range(3):
            for o in range(4):
                rows = slice(8 * o, 8 * o + 8)
                smoothed[c, x, rows] = merge(u2[c, x + 1, 8 + 8 * o : 16 + 8 * o], ue[c, i, rows], g)
                residual[c, x, rows] = merge(residual_in[c, x, rows], re[c, i, rows], g)

    def coarse_x(k, _):
        w_m[k] = four(v_m[2 * k], v_m[2 * k + 1], v_m[2 * k + 2], v_m[2 * k + 3])
        w_s[k] = four(v_s[2 * k], v_s[2 * k + 1], v_s[2 * k + 2], v_s[2 * k + 3])
        return 0

    lax.fori_loop(0, 10, coarse_x, 0)
    y1[...] = jnp.zeros(y1.shape, F32)
    for k in range(10):
        for ref, at in ((w_m, 0), (w_s, 128)):
            y1[k, 0:18, at : at + 128] = four(*(ref[k, pl.ds(5 + i, 18, stride=2)] for i in range(4)))
    band1 = band(256, lambda r: jnp.where(r < 192, r, r - 256), lambda m: jnp.where(m < 65, m, jnp.where(m == 65, -1, 1000)))
    coarse = exact_dot(y1[...].reshape(240, 256), band1).reshape(10, 24, 128)
    row24, lane24 = subs(24), lanes(24)
    mask_yz = jnp.where(row24 == 0, lo_y, jnp.where(row24 == 17, hi_y, 1.0)) * jnp.where(
        lane24 == 64, hi_z, jnp.where(lane24 == 65, lo_z, 1.0)
    )
    for k in range(10):
        mask = mask_yz * (lo_x if k == 0 else hi_x if k == 9 else 1.0)
        c1[k] = coarse[k] * mask
    for k in range(8):
        one_out[k] = c1[k + 1, 1:17, 0:64]
    rows = []
    for k in range(4):
        t2[...] = four(c1[2 * k], c1[2 * k + 1], c1[2 * k + 2], c1[2 * k + 3])
        rows.append(four(*(t2[pl.ds(i, 8, stride=2)] for i in range(4))))
    band2 = band(128, lambda r: jnp.where(r < 65, r, jnp.where(r == 65, -1, 100000)), lambda m: jnp.where(m < 32, m, 1000))
    coarse = exact_dot(jnp.concatenate(rows, axis=0), band2)
    planes = [coarse[8 * k : 8 * k + 8] for k in range(4)]
    for k in range(4):
        two_out[k] = planes[k][:, 0:32]
    thirds = (
        0.125 * planes[0],
        0.125 * (3.0 * planes[0] + 3.0 * planes[1] + planes[2]),
        0.125 * (planes[1] + 3.0 * planes[2] + 3.0 * planes[3]),
        0.125 * planes[3],
    )
    rows = []
    t3[...] = jnp.zeros(t3.shape, F32)
    for k in range(4):
        t3[4:12] = thirds[k]
        rows.append(four(*(t3[pl.ds(1 + i, 8, stride=2)] for i in range(4))))
    band3 = band(128, lambda r: jnp.where(r < 32, r, 100000), lambda m: jnp.where(m < 18, m - 1, 1000))
    coarse = exact_dot(jnp.concatenate(rows, axis=0), band3)
    for k in range(4):
        partial[k] = coarse[8 * k : 8 * k + 8]


def with_sum(tile, total):
    row = lax.broadcasted_iota(jnp.int32, tile.shape, tile.ndim - 2)
    return jnp.where(row == 7, total, tile)


def finish(partial, total):
    even, has_lo, has_hi = position("gx")
    got_a = pair_a(with_sum(jnp.where(even, partial[3], partial[0]), total), "gx")
    total = total + got_a[7:8]
    got_b = pair_b(with_sum(jnp.where(even, partial[0], partial[3]), total), "gx")
    total = total + got_b[7:8]
    lo, hi = jnp.where(even, got_b, got_a), jnp.where(even, got_a, got_b)
    inner = jnp.stack(
        [partial[1] + jnp.where(has_lo, lo, 0.0), partial[2] + jnp.where(has_hi, hi, 0.0)]
    )
    even, has_lo, has_hi = position("gy")
    got_a = pair_a(with_sum(inner, total), "gy")
    total = total + got_a[0, 7:8]
    got_b = pair_b(with_sum(inner, total), "gy")
    total = total + got_b[0, 7:8]
    lo, hi = jnp.where(even, got_b, got_a), jnp.where(even, got_a, got_b)
    row = lax.broadcasted_iota(jnp.int32, inner.shape, 1)
    inner = (
        inner
        + jnp.where((row == 1) & has_lo, jnp.roll(lo, -4, 1), 0.0)
        + jnp.where((row == 4) & has_hi, jnp.roll(hi, 4, 1), 0.0)
    )
    even, has_lo, has_hi = position("gz")
    got_a = pair_a(with_sum(inner, total), "gz")
    total = total + got_a[0, 7:8]
    got_b = pair_b(with_sum(inner, total), "gz")
    total = total + got_b[0, 7:8]
    lo, hi = jnp.where(even, got_b, got_a), jnp.where(even, got_a, got_b)
    three = inner[:, 1:5, 1:17]
    z = lax.broadcasted_iota(jnp.int32, three.shape, 2)
    three = (
        three
        + jnp.where((z == 0) & has_lo, lo[:, 1:5, 17:18], 0.0)
        + jnp.where((z == 15) & has_hi, hi[:, 1:5, 0:1], 0.0)
    )
    return total[0, 0], three


def far(axis, total):
    count = lax.axis_size(axis)
    if count == 4:
        return jnp.zeros_like(total)
    return lax.ppermute(total, axis, [(i, (i + count // 2) % count) for i in range(count)])


def per_device(velocity, forcing, phase_block, prefactor, yield_stress):
    send_a, send_b, own_a, own_b, phase = pl.pallas_call(
        pack_xy, out_shape=[sds(19, 32, 128)] * 2 + [sds(37, 8, 128)] * 2 + [sds(4, 8, 128)],
        in_specs=[VMEM] * 3, out_specs=[VMEM] * 5, compiler_params=params(LIM), name="pack_xy",
    )(velocity, forcing, phase_block)
    own = (velocity, forcing, phase)
    rx = (pair_a(send_a, "gx"), pair_b(send_b, "gx"))
    ry = (pair_a(own_a, "gy"), pair_b(own_b, "gy"))
    corner_a, corner_b = pl.pallas_call(
        pack_y, out_shape=[sds(16, 8, 128)] * 2, in_specs=[VMEM] * 2, out_specs=[VMEM] * 2,
        compiler_params=params(LIM), name="pack_y",
    )(*rx)
    ry = ry + (pair_a(corner_a, "gy"), pair_b(corner_b, "gy"))
    eu, ef = pl.pallas_call(
        edge_own, out_shape=[sds(3, 6, 32, 128)] * 2, in_specs=[VMEM] * 4, out_specs=[VMEM] * 2,
        compiler_params=params(LIM), cost_estimate=cost(3 << 23), name="edge_own",
    )(velocity, forcing, *rx)
    send_a, send_b, eu4, ef4, tiles = pl.pallas_call(
        pack_z, out_shape=[sds(25, 8, 128)] * 2 + [sds(3, 6, 8, 128)] * 2 + [sds(12, 8, 128)],
        in_specs=[VMEM] * 9, out_specs=[VMEM] * 5, compiler_params=params(LIM), name="pack_z",
    )(phase, *rx, *ry, eu, ef)
    rz = (pair_a(send_a, "gz"), pair_b(send_b, "gz"))
    v, u2, res, square = pl.pallas_call(
        main_work,
        out_shape=[sds(22, 56, 128), sds(3, 18, 56, 128), sds(3, NX, NY, NZ), sds(8, 128)],
        in_specs=[VMEM] * 9 + [SMEM] * 2, out_specs=[VMEM] * 4,
        scratch_shapes=[
            pltpu.VMEM((3, 24, 56, 128), F32), pltpu.VMEM((3, 20, 40, 128), F32),
            pltpu.VMEM((6, 40, 128), F32), pltpu.VMEM((6, 40, 128), F32), pltpu.VMEM((3, 20, 56, 128), F32),
        ],
        compiler_params=params(LIM), cost_estimate=cost(1 << 25), name="main_work",
    )(*own, *rx, *ry, prefactor, yield_stress)
    ve, ue, re, total = pl.pallas_call(
        edge_work,
        out_shape=[sds(6, 40, 128), sds(3, 6, 32, 128), sds(3, 6, 32, 128), sds(1, 128)],
        in_specs=[VMEM] * 8 + [SMEM] * 2, out_specs=[VMEM] * 4,
        scratch_shapes=[
            pltpu.VMEM((3, 8, 56, 128), F32), pltpu.VMEM((3, 6, 40, 128), F32),
            *[pltpu.VMEM((6, 40, 128), F32)] * 4,
            pltpu.VMEM((8, 56, 128), F32), pltpu.VMEM((3, 8, 56, 128), F32), pltpu.VMEM((3, 8, 56, 128), F32),
        ],
        compiler_params=params(LIM), cost_estimate=cost(1 << 23), name="edge_work",
    )(*rz, eu, ef, eu4, ef4, tiles, square, prefactor, yield_stress)
    total = total + far("gx", total)
    total = total + far("gz", total)
    smoothed, visc, one, two, residual, partial = pl.pallas_call(
        collect,
        out_shape=[
            sds(3, NX, NY, NZ), sds(NX, NY, NZ), sds(8, 16, 64), sds(4, 8, 32), sds(3, NX, NY, NZ), sds(4, 8, 128),
        ],
        in_specs=[VMEM] * 6, out_specs=[VMEM] * 6,
        scratch_shapes=[
            pltpu.VMEM((22, 56, 128), F32), pltpu.VMEM((22, 56, 128), F32),
            pltpu.VMEM((10, 56, 128), F32), pltpu.VMEM((10, 56, 128), F32), pltpu.VMEM((10, 24, 256), F32),
            pltpu.VMEM((10, 24, 128), F32), pltpu.VMEM((24, 128), F32), pltpu.VMEM((24, 128), F32),
        ],
        compiler_params=params(LIM), cost_estimate=cost(1 << 23), name="collect",
    )(v, u2, res, ve, ue, re)
    total, three = finish(partial, total)
    cells = 3.0 * NX * NY * NZ
    for axis in AX:
        cells = cells * lax.axis_size(axis)
    return smoothed, visc, one, two, three, residual, jnp.sqrt(total / cells)


def solution(mesh):
    field, cell = P(None, *AX), P(*AX)
    return jax.shard_map(
        per_device,
        mesh=mesh,
        in_specs=(field, field, cell, P(), P()),
        out_specs=(field, cell, cell, cell, cell, field, P()),
        check_vma=False,
    )
```

```python
import functools

import jax
import jax.numpy as jnp
from jax import lax
from jax.experimental import pallas as pl
from jax.experimental.pallas import tpu as pltpu
from jax.sharding import PartitionSpec as P

F32 = jnp.float32
BLOCK = 4
AX = ("gx", "gy", "gz")
NX, NY, NZ = 16, 32, 128
VMEM = pl.BlockSpec(memory_space=pltpu.VMEM)
HBM = pl.BlockSpec(memory_space=pltpu.HBM)
LIM = 9
SMEM = pl.BlockSpec(memory_space=pltpu.SMEM)


def sds(*shape):
    return jax.ShapeDtypeStruct(shape, F32)


def position(axis):
    index = lax.axis_index(axis)
    return lax.rem(index, 2) == 0, index > 0, index < lax.axis_size(axis) - 1


def lanes(rows=8, width=128):
    return lax.broadcasted_iota(jnp.int32, (rows, width), 1)


def subs(rows=8, width=128):
    return lax.broadcasted_iota(jnp.int32, (rows, width), 0)


def roll(value, shift, axis):
    size = value.shape[axis]
    shift = shift % size
    return pltpu.roll(value, shift, axis) if shift else value


def pair_a(value, axis):
    count = lax.axis_size(axis)
    return lax.ppermute(value, axis, [(i, i ^ 1) for i in range(count)])


def pair_b(value, axis):
    count = lax.axis_size(axis)
    return lax.ppermute(
        value, axis, [(i, (i + 1) % count if i % 2 else (i - 1) % count) for i in range(count)]
    )


def params(mib):
    return pltpu.CompilerParams(vmem_limit_bytes=mib << 20)


def cost(flops):
    return pl.CostEstimate(flops=flops, bytes_accessed=1 << 20, transcendentals=0)


def put_pair(pair, axis, index, lo, hi):
    even = position(axis)[0]
    pair[0][index] = jnp.where(even, hi, lo)
    pair[1][index] = jnp.where(even, lo, hi)


def pack_rows4(pair, index, tile, p, q):
    sub = subs()
    lo = jnp.where(sub < 4, tile(p, 0), roll(tile(q, 0), 4, 0))
    hi = jnp.where(sub < 4, roll(tile(p, 3), 4, 0), tile(q, 3))
    put_pair(pair, "gy", index, lo, hi)


def pack_rows2(pair, index, tile, planes):
    sub = subs()
    lo = tile(planes[0], 0)
    hi = roll(tile(planes[0], 3), 2, 0)
    for k in range(1, 4):
        here = (sub >> 1) == k
        lo = jnp.where(here, roll(tile(planes[k], 0), 2 * k, 0), lo)
        hi = jnp.where(here, roll(tile(planes[k], 3), 2 * k + 2, 0), hi)
    put_pair(pair, "gy", index, lo, hi)


def pack_phase(pair, index, tiles):
    sub = subs()
    lo = jnp.zeros((8, 128), F32)
    hi = lo
    for b, tile in enumerate(tiles):
        lo = jnp.where(sub == b, tile[0:1], lo)
        hi = jnp.where(sub == b, tile[7:8], hi)
    put_pair(pair, "gy", index, lo, hi)


def pack_xy(vel, forc, blocks_in, send_a, send_b, own_a, own_b, phase, blocks, vel_y, forc_y, sems):
    even, _, _ = position("gx")
    pairs = [(blocks_in, blocks)]
    for k in range(2):
        pairs.append((vel.at[:, :, 24 * k : 24 * k + 8], vel_y.at[k]))
        pairs.append((forc.at[:, :, 24 * k : 24 * k + 8], forc_y.at[k]))
    for out, first in ((send_a, jnp.where(even, 1, 0)), (send_b, jnp.where(even, 0, 1))):
        for c in range(3):
            pairs.append((vel.at[c, pl.ds(12 * first, 4)], out.at[4 * c : 4 * c + 4]))
            pairs.append((forc.at[c, pl.ds(14 * first, 2)], out.at[12 + 2 * c : 14 + 2 * c]))
    copies = [pltpu.make_async_copy(source, target, sems.at[k]) for k, (source, target) in enumerate(pairs)]
    for copy in copies:
        copy.start()
    phase[...] = jnp.zeros(phase.shape, F32)
    copies[0].wait()
    for b in range(4):
        phase[b, :, 0:32] = blocks[b].astype(F32)
    send_a[18, 0:8] = jnp.where(even, phase[3], phase[0])
    send_b[18, 0:8] = jnp.where(even, phase[0], phase[3])
    for copy in copies[1:5]:
        copy.wait()
    pair = (own_a, own_b)
    for c in range(3):
        for g in range(8):
            pack_rows4(pair, 8 * c + g, lambda p, o: vel_y[o // 3, c, p], g, g + 8)
        for g in range(4):
            pack_rows2(pair, 24 + 4 * c + g, lambda p, o: forc_y[o // 3, c, p], [g + 4 * k for k in range(4)])
    pack_phase(pair, 36, [phase[b] for b in range(4)])
    for copy in copies[5:]:
        copy.wait()


def pack_y(rx_a, rx_b, corner_a, corner_b):
    rx, pair = (rx_a, rx_b), (corner_a, corner_b)
    for c in range(3):
        for i in range(4):
            pack_rows4(pair, 4 * c + i, lambda p, o: tile_of(None, c, p, o, 4, rx, 0, None), i, 20 + i)
        pack_rows2(pair, 12 + c, lambda p, o: tile_of(None, c, p, o, 2, rx, 12, None), [0, 1, 18, 19])
    pack_phase(pair, 15, [phase_rows(None, rx, 0), phase_rows(None, rx, 5)])


def halo(pair, axis, index):
    even, has_lo, has_hi = position(axis)
    a, b = pair[0][index], pair[1][index]
    lo = jnp.where(has_lo, jnp.where(even, b, a), 0.0)
    hi = jnp.where(has_hi, jnp.where(even, a, b), 0.0)
    return lo, hi


def tile_of(own, c, plane, o, width, rx, base, ry):
    rows = slice(8 * o, 8 * o + 8)
    if o == 4:
        sub = subs()
        inside = width <= plane < NX + width
        pair = ry[0] if inside else ry[1]
        at = plane - width if inside else plane if plane < width else plane - NX
        if width == 4:
            half = 8 if inside else 4
            lo, hi = halo(pair, "gy", half * c + at % half)
            if at < half:
                return jnp.where(sub < 4, hi, roll(lo, 4, 0))
            return jnp.where(sub < 4, roll(hi, 4, 0), lo)
        lo, hi = halo(pair, "gy", 24 + 4 * c + at % 4 if inside else 12 + c)
        k = at // 4 if inside else at
        return jnp.where(sub < 4, roll(hi, -2 * k, 0), roll(lo, 6 - 2 * k, 0))
    if plane < width:
        return halo(rx, "gx", (base + width * c + plane, rows))[0]
    if plane >= NX + width:
        return halo(rx, "gx", (base + width * c + plane - NX - width, rows))[1]
    return own[c, plane - width, rows]


def phase_rows(phase, rx, b):
    if b == 0:
        return halo(rx, "gx", (18, slice(0, 8)))[0]
    if b == 5:
        return halo(rx, "gx", (18, slice(0, 8)))[1]
    return phase[b - 1]


def phase_tiles(phase, rx, ry):
    own, corner = halo(ry[0], "gy", 36), halo(ry[1], "gy", 15)
    sub = subs()
    tiles = []
    for b in range(6):
        tiles.append(phase_rows(phase, rx, b))
        lo, hi = own if 0 < b < 5 else corner
        row = b - 1 if 0 < b < 5 else b // 5
        outer = jnp.where(sub == 0, hi[row : row + 1], jnp.where(sub == 1, lo[row : row + 1], 0.0))
        tiles.append(outer)
    return tiles


def slots():
    lane = lanes()
    return lane >> 5, lane & 31


def edge_tile(tile, i, low_plane, planes):
    slot, pos = slots()
    value = jnp.zeros((8, 128), F32)
    for g in range(4):
        plane = 6 * g + i - low_plane
        if not 0 <= plane < planes:
            continue
        own = tile(plane)
        here = slot == g
        value = jnp.where(here & (pos < 16), roll(own, 32 * g + 4, 1), value)
        value = jnp.where(here & (pos >= 16), roll(own, 32 * g + 28, 1), value)
    return jnp.where(((pos >= 4) & (pos < 12)) | ((pos >= 20) & (pos < 28)), value, 0.0)


def edge_own(vel, forc, rx_a, rx_b, eu, ef):
    rx = (rx_a, rx_b)
    for c in range(3):
        for i in range(6):
            for o in range(4):
                rows = slice(8 * o, 8 * o + 8)
                eu[c, i, rows] = edge_tile(lambda p: tile_of(vel, c, p, o, 4, rx, 0, None), i, 0, 24)
                ef[c, i, rows] = edge_tile(lambda p: tile_of(forc, c, p, o, 2, rx, 12, None), i, 2, 20)


def pack_z(phase, rx_a, rx_b, ryo_a, ryo_b, ryc_a, ryc_b, eu, ef, send_a, send_b, eu4, ef4, tiles):
    rx, ry = (rx_a, rx_b), ((ryo_a, ryo_b), (ryc_a, ryc_b))
    even, _, _ = position("gz")

    def put(index, lo, hi):
        send_a[index] = jnp.where(even, hi, lo)
        send_b[index] = jnp.where(even, lo, hi)

    lane = lanes()
    place = (lane & 31) >> 2
    for c in range(3):
        for i in range(6):
            eu4[c, i] = edge_tile(lambda p: tile_of(None, c, p, 4, 4, rx, 0, ry), i, 0, 24)
            ef4[c, i] = edge_tile(lambda p: tile_of(None, c, p, 4, 2, rx, 12, ry), i, 2, 20)
    for base, own, own4 in ((0, eu, eu4), (12, ef, ef4)):
        for w in range(12):
            lo = jnp.zeros((8, 128), F32)
            hi = lo
            for k in range(min(8, 90 - 8 * w)):
                n = 8 * w + k
                c, i, o = n // 30, n // 5 % 6, n % 5
                tile = own4[c, i] if o == 4 else own[c, i, 8 * o : 8 * o + 8]
                lo = jnp.where(place == k, roll(tile, 4 * k - 4, 1), lo)
                hi = jnp.where(place == k, roll(tile, 4 * k - 24, 1), hi)
            put(base + w, lo, hi)
    lo = jnp.zeros((8, 128), F32)
    hi = lo
    for j, tile in enumerate(phase_tiles(phase, rx, ry)):
        tiles[j] = tile
        lo = jnp.where(lane == j, roll(tile, j, 1), lo)
        hi = jnp.where(lane == j, roll(tile, j - 31, 1), hi)
    put(24, lo, hi)


def exact_dot(a, b):
    return jnp.dot(a, b, preferred_element_type=F32, precision=lax.Precision.HIGHEST)


def four(a, b, c, d):
    return (a + 3.0 * b + 3.0 * c + d) * 0.125


def put_rows(ref, index, o, value):
    ref[index + (slice(8 + 8 * o, 16 + 8 * o),)] = value
    if o == 0:
        ref[index + (slice(48, 56),)] = value
    if o == 4:
        ref[index + (slice(0, 8),)] = value


def tables(tiles, wide, pre, yld, creep, limit):
    block = lax.broadcasted_iota(jnp.int32, (128, 128), 0)
    spread = jnp.dot(
        jnp.concatenate(tiles, axis=0), (wide == block).astype(F32), preferred_element_type=F32
    )
    row = lax.broadcasted_iota(jnp.int32, (40, 16), 0)
    by = lax.broadcasted_iota(jnp.int32, (40, 16), 1)
    tall = (jnp.where(row < 32, row >> 2, jnp.where(row < 36, 8, 9)) == by).astype(F32)
    for b in range(6):
        phase = jnp.dot(tall, spread[16 * b : 16 * b + 16], preferred_element_type=F32)
        first = jnp.full(phase.shape, pre[0], F32)
        second = jnp.full(phase.shape, yld[0], F32)
        for k in range(1, 8):
            here = phase == float(k)
            first = jnp.where(here, pre[k], first)
            second = jnp.where(here, yld[k], second)
        creep[b] = first
        limit[b] = 0.5 * second


def viscosity_tile(u, creep, limit):
    d = []
    for c in range(3):
        mid = u(c, 0, 0)
        d.append((u(c, 1, 0) - u(c, -1, 0), u(c, 0, 1) - u(c, 0, -1), roll(mid, 127, 1) - roll(mid, 1, 1)))
    a01, a02, a12 = d[0][1] + d[1][0], d[0][2] + d[2][0], d[1][2] + d[2][1]
    own = d[0][0] * d[0][0] + d[1][1] * d[1][1] + d[2][2] * d[2][2]
    off = a01 * a01 + a02 * a02 + a12 * a12
    invariant = 1.0 + (own * 0.125 + off * 0.0625)
    return jnp.minimum(creep * jnp.exp(jnp.log(invariant) * (-1.0 / 3.0)), limit * lax.rsqrt(invariant))


def around(ref, index, o):
    head, p = index[:-1], index[-1]
    mid = ref[head + (p, slice(8 + 8 * o, 16 + 8 * o))]
    return mid, (
        ref[head + (p + 1, slice(8 + 8 * o, 16 + 8 * o))],
        ref[head + (p - 1, slice(8 + 8 * o, 16 + 8 * o))],
        ref[head + (p, slice(9 + 8 * o, 17 + 8 * o))],
        ref[head + (p, slice(7 + 8 * o, 15 + 8 * o))],
        roll(mid, 127, 1),
        roll(mid, 1, 1),
    )


def faces(v_ref, vx, o):
    mid, near = around(v_ref, (vx,), o)
    f = [mid + value for value in near]
    return mid, f, (f[0] + f[1]) + (f[2] + f[3]) + (f[4] + f[5])


def weighted(ref, index, o, f):
    mid, near = around(ref, index, o)
    total = f[0] * near[0]
    for k in range(1, 6):
        total = total + f[k] * near[k]
    return mid, total


def relax(mid_v, diag):
    return jnp.where(mid_v > 0.0, 0.8 / diag, 0.0)


def flags(axis):
    return tuple(flag.astype(F32) for flag in position(axis)[1:])


def main_work(
    vel, forc, phase_ref, rx_a, rx_b, ryo_a, ryo_b, ryc_a, ryc_b, pre, yld,
    v_own, u_own, residual, square,
    u_ref, f_ref, creep, limit, v_ref, u1, u2, sems,
):
    rx, ry = (rx_a, rx_b), ((ryo_a, ryo_b), (ryc_a, ryc_b))
    lo_x, hi_x = flags("gx")
    lo_y, hi_y = flags("gy")
    for c in range(3):
        for p in range(24):
            for o in range(5):
                put_rows(u_ref, (c, p), o, tile_of(vel, c, p, o, 4, rx, 0, ry))
        for p in range(20):
            for o in range(5):
                f_ref[c, p, 8 * o : 8 * o + 8] = tile_of(forc, c, p, o, 2, rx, 12, ry)
    wide = lax.broadcasted_iota(jnp.int32, (128, 128), 1) >> 2
    tables(phase_tiles(phase_ref, rx, ry), wide, pre, yld, creep, limit)
    mask_y = jnp.where(subs() < 4, hi_y, lo_y)

    def viscosity(vx, _):
        mask_x = jnp.where(vx < 3, lo_x, jnp.where(vx >= 19, hi_x, 1.0))
        bx = (vx + 1) >> 2
        for o in range(5):
            value = viscosity_tile(
                lambda c, dx, dy: u_ref[c, vx + 1 + dx, 8 + 8 * o + dy : 16 + 8 * o + dy],
                creep[bx, 8 * o : 8 * o + 8], limit[bx, 8 * o : 8 * o + 8],
            )
            value = value * (mask_y * mask_x if o == 4 else mask_x)
            put_rows(v_ref, (vx,), o, value)
        return 0

    lax.fori_loop(0, 22, viscosity, 0, unroll=2)
    copy_v = pltpu.make_async_copy(v_ref.at[:, 8:48], v_own, sems.at[0])
    copy_v.start()

    def sweep(source, target, first, first_u):
        def body(x, _):
            for o in range(5):
                mid_v, f, diag = faces(v_ref, x + first, o)
                rate = relax(mid_v, diag)
                for c in range(3):
                    mid, total = weighted(source, (c, x + first_u), o, f)
                    force = f_ref[c, x + first - 1, 8 * o : 8 * o + 8]
                    put_rows(target, (c, x), o, 0.2 * mid + rate * (2.0 * force + total))
            return 0

        return body

    lax.fori_loop(0, 20, sweep(u_ref, u1, 1, 2), 0, unroll=4)
    lax.fori_loop(0, 18, sweep(u1, u2, 2, 1), 0, unroll=3)
    copy_u = pltpu.make_async_copy(u2.at[:, 1:17, 8:40], u_own, sems.at[1])
    copy_u.start()

    def last(x, acc):
        for o in range(4):
            _, f, diag = faces(v_ref, x + 3, o)
            for c in range(3):
                mid, total = weighted(u2, (c, x + 1), o, f)
                value = f_ref[c, x + 2, 8 * o : 8 * o + 8] + 0.5 * (total - diag * mid)
                residual[c, x, 8 * o : 8 * o + 8] = value
                acc = acc + value * value
        return acc

    acc = lax.fori_loop(0, NX, last, jnp.zeros((8, 128), F32), unroll=4)
    lane = lanes()
    square[...] = jnp.where((lane >= 4) & (lane < 124), acc, 0.0)
    copy_v.wait()
    copy_u.wait()


def put_edge(ref, index, i, o, value):
    put_rows(ref, index + (i + 1,), o, value)


def wrap_planes(ref, lead):
    for index in lead:
        for r in range(7):
            rows = slice(8 * r, 8 * r + 8)
            ref[index + (0, rows)] = roll(ref[index + (6, rows)], 32, 1)
            ref[index + (7, rows)] = roll(ref[index + (1, rows)], -32, 1)


def edge_work(
    rz_a, rz_b, eu, ef, eu4, ef4, phases, square, pre, yld,
    v_out, u_out, r_out, total_out,
    u_ref, f_ref, creep, limit, creep_e, limit_e, v_ref, u1, u2,
):
    rz = (rz_a, rz_b)
    lo_x, hi_x = flags("gx")
    lo_y, hi_y = flags("gy")
    lo_z, hi_z = flags("gz")
    lane = lanes()
    slot, pos = slots()
    lead = ((0,), (1,), (2,))
    for base, own, own4 in ((0, eu, eu4), (12, ef, ef4)):
        for w in range(12):
            lo, hi = halo(rz, "gz", base + w)
            for k in range(min(8, 90 - 8 * w)):
                n = 8 * w + k
                c, i, o = n // 30, n // 5 % 6, n % 5
                tile = own4[c, i] if o == 4 else own[c, i, 8 * o : 8 * o + 8]
                tile = jnp.where(pos < 4, roll(lo, -4 * k, 1), tile)
                tile = jnp.where(pos >= 28, roll(hi, 28 - 4 * k, 1), tile)
                if base == 0:
                    put_edge(u_ref, (c,), i, o, tile)
                else:
                    f_ref[c, i, 8 * o : 8 * o + 8] = tile
    wrap_planes(u_ref, lead)

    lo, hi = halo(rz, "gz", 24)
    tiles = []
    for j in range(12):
        tile = jnp.where(lane == 32, roll(hi, 32 - j, 1), phases[j])
        tiles.append(jnp.where(lane == 33, roll(lo, 33 - j, 1), tile))
    at = lax.broadcasted_iota(jnp.int32, (128, 128), 1) & 31
    wide = jnp.where(at < 4, 33, jnp.where(at < 12, (at - 4) >> 2, jnp.where(at < 20, 127, 25 + (at >> 2))))
    tables(tiles, wide, pre, yld, creep, limit)
    for i in range(6):
        first, second = creep[i // 4], limit[i // 4]
        slot40 = lanes(40) >> 5
        for g in range(1, 4):
            b = (6 * g + i) // 4
            first = jnp.where(slot40 == g, creep[b], first)
            second = jnp.where(slot40 == g, limit[b], second)
        creep_e[i] = first
        limit_e[i] = second

    mask_z = jnp.where(pos < 4, lo_z, jnp.where(pos >= 28, hi_z, jnp.where((pos < 12) | (pos >= 20), 1.0, 0.0)))
    mask_y = jnp.where(subs() < 4, hi_y, lo_y)

    def viscosity(i, _):
        px = 6 * slot + i
        mask = mask_z * jnp.where(px < 4, lo_x, jnp.where(px >= 20, hi_x, 1.0))
        for o in range(5):
            value = viscosity_tile(
                lambda c, dx, dy: u_ref[c, i + 1 + dx, 8 + 8 * o + dy : 16 + 8 * o + dy],
                creep_e[i, 8 * o : 8 * o + 8], limit_e[i, 8 * o : 8 * o + 8],
            )
            value = value * (mask * mask_y if o == 4 else mask)
            put_edge(v_ref, (), i, o, value)
            v_out[i, 8 * o : 8 * o + 8] = value
        return 0

    lax.fori_loop(0, 6, viscosity, 0, unroll=6)
    wrap_planes(v_ref, ((),))

    def sweep(source, target):
        def body(i, _):
            for o in range(5):
                mid_v, f, diag = faces(v_ref, i + 1, o)
                rate = relax(mid_v, diag)
                for c in range(3):
                    mid, total = weighted(source, (c, i + 1), o, f)
                    force = f_ref[c, i, 8 * o : 8 * o + 8]
                    put_edge(target, (c,), i, o, 0.2 * mid + rate * (2.0 * force + total))
            return 0

        lax.fori_loop(0, 6, body, 0, unroll=6)
        wrap_planes(target, lead)

    sweep(u_ref, u1)
    sweep(u1, u2)

    def last(i, acc):
        px = 6 * slot + i
        count = (px >= 4) & (px < 20) & (((pos >= 4) & (pos < 8)) | ((pos >= 24) & (pos < 28)))
        for o in range(4):
            _, f, diag = faces(v_ref, i + 1, o)
            for c in range(3):
                mid, total = weighted(u2, (c, i + 1), o, f)
                value = f_ref[c, i, 8 * o : 8 * o + 8] + 0.5 * (total - diag * mid)
                r_out[c, i, 8 * o : 8 * o + 8] = value
                u_out[c, i, 8 * o : 8 * o + 8] = mid
                acc = acc + jnp.where(count, value * value, 0.0)
        return acc

    acc = lax.fori_loop(0, 6, last, square[...], unroll=6)
    total = jnp.sum(jnp.sum(acc, axis=1, keepdims=True), axis=0, keepdims=True)
    total_out[...] = jnp.broadcast_to(total, (1, 128))


def band(rows, row_z, col_m):
    row = row_z(lax.broadcasted_iota(jnp.int32, (rows, 128), 0))
    col = col_m(lax.broadcasted_iota(jnp.int32, (rows, 128), 1))
    at = row - 2 * col + 1
    return jnp.where((at == 0) | (at == 3), 0.125, jnp.where((at == 1) | (at == 2), 0.375, 0.0)).astype(F32)


def merge(own, edge, g):
    lane = lanes()
    value = jnp.where(lane < 4, roll(edge, -32 * g - 4, 1), own)
    return jnp.where(lane >= 124, roll(edge, 100 - 32 * g, 1), value)


def collect(
    v_own, u_own, residual_in, ve, ue, re,
    smoothed, visc_out, one_out, two_out, residual, partial,
    v_m, v_s, w_m, w_s, y1, c1, t2, t3,
):
    lo_x, hi_x = flags("gx")
    lo_y, hi_y = flags("gy")
    lo_z, hi_z = flags("gz")
    lane = lanes()
    for vx in range(22):
        g, i = (vx + 1) // 6, (vx + 1) % 6
        for o in range(5):
            edge = ve[i, 8 * o : 8 * o + 8]
            value = merge(v_own[vx, 8 * o : 8 * o + 8], edge, g)
            put_rows(v_m, (vx,), o, value)
            side = jnp.where(lane < 4, roll(edge, -28 - 32 * g, 1), 0.0)
            put_rows(v_s, (vx,), o, jnp.where(lane >= 124, roll(edge, 124 - 32 * g, 1), side))
            if 3 <= vx < 19 and o < 4:
                visc_out[vx - 3, 8 * o : 8 * o + 8] = value
    for x in range(NX):
        g, i = (x + 4) // 6, (x + 4) % 6
        for c in range(3):
            for o in range(4):
                rows = slice(8 * o, 8 * o + 8)
                smoothed[c, x, rows] = merge(u_own[c, x, rows], ue[c, i, rows], g)
                residual[c, x, rows] = merge(residual_in[c, x, rows], re[c, i, rows], g)

    def coarse_x(k, _):
        w_m[k] = four(v_m[2 * k], v_m[2 * k + 1], v_m[2 * k + 2], v_m[2 * k + 3])
        w_s[k] = four(v_s[2 * k], v_s[2 * k + 1], v_s[2 * k + 2], v_s[2 * k + 3])
        return 0

    lax.fori_loop(0, 10, coarse_x, 0)
    y1[...] = jnp.zeros(y1.shape, F32)
    for k in range(10):
        for ref, at in ((w_m, 0), (w_s, 128)):
            y1[k, 0:18, at : at + 128] = four(*(ref[k, pl.ds(5 + i, 18, stride=2)] for i in range(4)))
    band1 = band(256, lambda r: jnp.where(r < 192, r, r - 256), lambda m: jnp.where(m < 65, m, jnp.where(m == 65, -1, 1000)))
    coarse = exact_dot(y1[...].reshape(240, 256), band1).reshape(10, 24, 128)
    row24, lane24 = subs(24), lanes(24)
    mask_yz = jnp.where(row24 == 0, lo_y, jnp.where(row24 == 17, hi_y, 1.0)) * jnp.where(
        lane24 == 64, hi_z, jnp.where(lane24 == 65, lo_z, 1.0)
    )
    for k in range(10):
        mask = mask_yz * (lo_x if k == 0 else hi_x if k == 9 else 1.0)
        c1[k] = coarse[k] * mask
    for k in range(8):
        one_out[k] = c1[k + 1, 1:17, 0:64]
    rows = []
    for k in range(4):
        t2[...] = four(c1[2 * k], c1[2 * k + 1], c1[2 * k + 2], c1[2 * k + 3])
        rows.append(four(*(t2[pl.ds(i, 8, stride=2)] for i in range(4))))
    band2 = band(128, lambda r: jnp.where(r < 65, r, jnp.where(r == 65, -1, 100000)), lambda m: jnp.where(m < 32, m, 1000))
    coarse = exact_dot(jnp.concatenate(rows, axis=0), band2)
    planes = [coarse[8 * k : 8 * k + 8] for k in range(4)]
    for k in range(4):
        two_out[k] = planes[k][:, 0:32]
    thirds = (
        0.125 * planes[0],
        0.125 * (3.0 * planes[0] + 3.0 * planes[1] + planes[2]),
        0.125 * (planes[1] + 3.0 * planes[2] + 3.0 * planes[3]),
        0.125 * planes[3],
    )
    rows = []
    t3[...] = jnp.zeros(t3.shape, F32)
    for k in range(4):
        t3[4:12] = thirds[k]
        rows.append(four(*(t3[pl.ds(1 + i, 8, stride=2)] for i in range(4))))
    band3 = band(128, lambda r: jnp.where(r < 32, r, 100000), lambda m: jnp.where(m < 18, m - 1, 1000))
    coarse = exact_dot(jnp.concatenate(rows, axis=0), band3)
    for k in range(4):
        partial[k] = coarse[8 * k : 8 * k + 8]


def with_sum(tile, total):
    row = lax.broadcasted_iota(jnp.int32, tile.shape, tile.ndim - 2)
    return jnp.where(row == 7, total, tile)


def finish(partial, total):
    even, has_lo, has_hi = position("gx")
    got_a = pair_a(with_sum(jnp.where(even, partial[3], partial[0]), total), "gx")
    total = total + got_a[7:8]
    got_b = pair_b(with_sum(jnp.where(even, partial[0], partial[3]), total), "gx")
    total = total + got_b[7:8]
    lo, hi = jnp.where(even, got_b, got_a), jnp.where(even, got_a, got_b)
    inner = jnp.stack(
        [partial[1] + jnp.where(has_lo, lo, 0.0), partial[2] + jnp.where(has_hi, hi, 0.0)]
    )
    even, has_lo, has_hi = position("gy")
    got_a = pair_a(with_sum(inner, total), "gy")
    total = total + got_a[0, 7:8]
    got_b = pair_b(with_sum(inner, total), "gy")
    total = total + got_b[0, 7:8]
    lo, hi = jnp.where(even, got_b, got_a), jnp.where(even, got_a, got_b)
    row = lax.broadcasted_iota(jnp.int32, inner.shape, 1)
    inner = (
        inner
        + jnp.where((row == 1) & has_lo, jnp.roll(lo, -4, 1), 0.0)
        + jnp.where((row == 4) & has_hi, jnp.roll(hi, 4, 1), 0.0)
    )
    even, has_lo, has_hi = position("gz")
    got_a = pair_a(with_sum(inner, total), "gz")
    total = total + got_a[0, 7:8]
    got_b = pair_b(with_sum(inner, total), "gz")
    total = total + got_b[0, 7:8]
    lo, hi = jnp.where(even, got_b, got_a), jnp.where(even, got_a, got_b)
    three = inner[:, 1:5, 1:17]
    z = lax.broadcasted_iota(jnp.int32, three.shape, 2)
    three = (
        three
        + jnp.where((z == 0) & has_lo, lo[:, 1:5, 17:18], 0.0)
        + jnp.where((z == 15) & has_hi, hi[:, 1:5, 0:1], 0.0)
    )
    return total[0, 0], three


def far(axis, total):
    count = lax.axis_size(axis)
    if count == 4:
        return jnp.zeros_like(total)
    return lax.ppermute(total, axis, [(i, (i + count // 2) % count) for i in range(count)])


def per_device(velocity, forcing, phase_block, prefactor, yield_stress):
    send_a, send_b, own_a, own_b, phase = pl.pallas_call(
        pack_xy, out_shape=[sds(19, 32, 128)] * 2 + [sds(37, 8, 128)] * 2 + [sds(4, 8, 128)],
        in_specs=[HBM] * 3, out_specs=[VMEM] * 5,
        scratch_shapes=[
            pltpu.VMEM((4, 8, 32), jnp.int32), pltpu.VMEM((2, 3, 16, 8, 128), F32),
            pltpu.VMEM((2, 3, 16, 8, 128), F32), pltpu.SemaphoreType.DMA((17,)),
        ],
        compiler_params=params(LIM), name="pack_xy",
    )(*(pltpu.with_memory_space_constraint(value, pltpu.HBM) for value in (velocity, forcing, phase_block)))
    own = (velocity, forcing, phase)
    rx = (pair_a(send_a, "gx"), pair_b(send_b, "gx"))
    ry = (pair_a(own_a, "gy"), pair_b(own_b, "gy"))
    corner_a, corner_b = pl.pallas_call(
        pack_y, out_shape=[sds(16, 8, 128)] * 2, in_specs=[VMEM] * 2, out_specs=[VMEM] * 2,
        compiler_params=params(LIM), name="pack_y",
    )(*rx)
    ry = ry + (pair_a(corner_a, "gy"), pair_b(corner_b, "gy"))
    eu, ef = pl.pallas_call(
        edge_own, out_shape=[sds(3, 6, 32, 128)] * 2, in_specs=[VMEM] * 4, out_specs=[VMEM] * 2,
        compiler_params=params(LIM), cost_estimate=cost(3 << 23), name="edge_own",
    )(velocity, forcing, *rx)
    send_a, send_b, eu4, ef4, tiles = pl.pallas_call(
        pack_z, out_shape=[sds(25, 8, 128)] * 2 + [sds(3, 6, 8, 128)] * 2 + [sds(12, 8, 128)],
        in_specs=[VMEM] * 9, out_specs=[VMEM] * 5, compiler_params=params(LIM), name="pack_z",
    )(phase, *rx, *ry, eu, ef)
    rz = (pair_a(send_a, "gz"), pair_b(send_b, "gz"))
    v, u2, res, square = pl.pallas_call(
        main_work,
        out_shape=[pltpu.HBM((22, 40, 128), F32), pltpu.HBM((3, NX, NY, NZ), F32), sds(3, NX, NY, NZ), sds(8, 128)],
        in_specs=[VMEM] * 9 + [SMEM] * 2, out_specs=[HBM] * 2 + [VMEM] * 2,
        scratch_shapes=[
            pltpu.VMEM((3, 24, 56, 128), F32), pltpu.VMEM((3, 20, 40, 128), F32),
            pltpu.VMEM((6, 40, 128), F32), pltpu.VMEM((6, 40, 128), F32), pltpu.VMEM((22, 56, 128), F32),
            pltpu.VMEM((3, 20, 56, 128), F32), pltpu.VMEM((3, 18, 56, 128), F32), pltpu.SemaphoreType.DMA((2,)),
        ],
        compiler_params=params(LIM), cost_estimate=cost(1 << 25), name="main_work",
    )(*own, *rx, *ry, prefactor, yield_stress)
    ve, ue, re, total = pl.pallas_call(
        edge_work,
        out_shape=[sds(6, 40, 128), sds(3, 6, 32, 128), sds(3, 6, 32, 128), sds(1, 128)],
        in_specs=[VMEM] * 8 + [SMEM] * 2, out_specs=[VMEM] * 4,
        scratch_shapes=[
            pltpu.VMEM((3, 8, 56, 128), F32), pltpu.VMEM((3, 6, 40, 128), F32),
            *[pltpu.VMEM((6, 40, 128), F32)] * 4,
            pltpu.VMEM((8, 56, 128), F32), pltpu.VMEM((3, 8, 56, 128), F32), pltpu.VMEM((3, 8, 56, 128), F32),
        ],
        compiler_params=params(LIM), cost_estimate=cost(1 << 23), name="edge_work",
    )(*rz, eu, ef, eu4, ef4, tiles, square, prefactor, yield_stress)
    total = total + far("gx", total)
    total = total + far("gz", total)
    smoothed, visc, one, two, residual, partial = pl.pallas_call(
        collect,
        out_shape=[
            sds(3, NX, NY, NZ), sds(NX, NY, NZ), sds(8, 16, 64), sds(4, 8, 32), sds(3, NX, NY, NZ), sds(4, 8, 128),
        ],
        in_specs=[VMEM] * 6, out_specs=[VMEM] * 6,
        scratch_shapes=[
            pltpu.VMEM((22, 56, 128), F32), pltpu.VMEM((22, 56, 128), F32),
            pltpu.VMEM((10, 56, 128), F32), pltpu.VMEM((10, 56, 128), F32), pltpu.VMEM((10, 24, 256), F32),
            pltpu.VMEM((10, 24, 128), F32), pltpu.VMEM((24, 128), F32), pltpu.VMEM((24, 128), F32),
        ],
        compiler_params=params(LIM), cost_estimate=cost(1 << 23), name="collect",
    )(v, u2, res, ve, ue, re)
    total, three = finish(partial, total)
    cells = 3.0 * NX * NY * NZ
    for axis in AX:
        cells = cells * lax.axis_size(axis)
    return smoothed, visc, one, two, three, residual, jnp.sqrt(total / cells)


def solution(mesh):
    field, cell = P(None, *AX), P(*AX)
    return jax.shard_map(
        per_device,
        mesh=mesh,
        in_specs=(field, field, cell, P(), P()),
        out_specs=(field, cell, cell, cell, cell, field, P()),
        check_vma=False,
    )
```

```python
import functools

import jax
import jax.numpy as jnp
from jax import lax
from jax.experimental import pallas as pl
from jax.experimental.pallas import tpu as pltpu
from jax.sharding import PartitionSpec as P

F32 = jnp.float32
BLOCK = 4
AX = ("gx", "gy", "gz")
NX, NY, NZ = 16, 32, 128
VMEM = pl.BlockSpec(memory_space=pltpu.VMEM)
HBM = pl.BlockSpec(memory_space=pltpu.HBM)
LIM = 9
SMEM = pl.BlockSpec(memory_space=pltpu.SMEM)


def sds(*shape):
    return jax.ShapeDtypeStruct(shape, F32)


def position(axis):
    index = lax.axis_index(axis)
    return lax.rem(index, 2) == 0, index > 0, index < lax.axis_size(axis) - 1


def lanes(rows=8, width=128):
    return lax.broadcasted_iota(jnp.int32, (rows, width), 1)


def subs(rows=8, width=128):
    return lax.broadcasted_iota(jnp.int32, (rows, width), 0)


def roll(value, shift, axis):
    size = value.shape[axis]
    shift = shift % size
    return pltpu.roll(value, shift, axis) if shift else value


def pair_a(value, axis):
    count = lax.axis_size(axis)
    return lax.ppermute(value, axis, [(i, i ^ 1) for i in range(count)])


def pair_b(value, axis):
    count = lax.axis_size(axis)
    return lax.ppermute(
        value, axis, [(i, (i + 1) % count if i % 2 else (i - 1) % count) for i in range(count)]
    )


def params(mib):
    return pltpu.CompilerParams(vmem_limit_bytes=mib << 20)


def cost(flops):
    return pl.CostEstimate(flops=flops, bytes_accessed=1 << 20, transcendentals=0)


def put_pair(pair, axis, index, lo, hi):
    even = position(axis)[0]
    pair[0][index] = jnp.where(even, hi, lo)
    pair[1][index] = jnp.where(even, lo, hi)


def pack_rows4(pair, index, tile, p, q):
    sub = subs()
    lo = jnp.where(sub < 4, tile(p, 0), roll(tile(q, 0), 4, 0))
    hi = jnp.where(sub < 4, roll(tile(p, 3), 4, 0), tile(q, 3))
    put_pair(pair, "gy", index, lo, hi)


def pack_rows2(pair, index, tile, planes):
    sub = subs()
    lo = tile(planes[0], 0)
    hi = roll(tile(planes[0], 3), 2, 0)
    for k in range(1, 4):
        here = (sub >> 1) == k
        lo = jnp.where(here, roll(tile(planes[k], 0), 2 * k, 0), lo)
        hi = jnp.where(here, roll(tile(planes[k], 3), 2 * k + 2, 0), hi)
    put_pair(pair, "gy", index, lo, hi)


def pack_phase(pair, index, tiles):
    sub = subs()
    lo = jnp.zeros((8, 128), F32)
    hi = lo
    for b, tile in enumerate(tiles):
        lo = jnp.where(sub == b, tile[0:1], lo)
        hi = jnp.where(sub == b, tile[7:8], hi)
    put_pair(pair, "gy", index, lo, hi)


def pack_xy(vel, forc, blocks_in, send_a, send_b, own_a, own_b, phase, blocks, vel_y, forc_y, sems):
    even, _, _ = position("gx")
    pairs = [(blocks_in, blocks)]
    for k in range(2):
        pairs.append((vel.at[:, :, 24 * k : 24 * k + 8], vel_y.at[k]))
        pairs.append((forc.at[:, :, 24 * k : 24 * k + 8], forc_y.at[k]))
    for out, first in ((send_a, jnp.where(even, 1, 0)), (send_b, jnp.where(even, 0, 1))):
        for c in range(3):
            pairs.append((vel.at[c, pl.ds(12 * first, 4)], out.at[4 * c : 4 * c + 4]))
            pairs.append((forc.at[c, pl.ds(14 * first, 2)], out.at[12 + 2 * c : 14 + 2 * c]))
    copies = [pltpu.make_async_copy(source, target, sems.at[k]) for k, (source, target) in enumerate(pairs)]
    for copy in copies:
        copy.start()
    phase[...] = jnp.zeros(phase.shape, F32)
    copies[0].wait()
    for b in range(4):
        phase[b, :, 0:32] = blocks[b].astype(F32)
    send_a[18, 0:8] = jnp.where(even, phase[3], phase[0])
    send_b[18, 0:8] = jnp.where(even, phase[0], phase[3])
    for copy in copies[1:5]:
        copy.wait()
    pair = (own_a, own_b)
    for c in range(3):
        for g in range(8):
            pack_rows4(pair, 8 * c + g, lambda p, o: vel_y[o // 3, c, p], g, g + 8)
        for g in range(4):
            pack_rows2(pair, 24 + 4 * c + g, lambda p, o: forc_y[o // 3, c, p], [g + 4 * k for k in range(4)])
    pack_phase(pair, 36, [phase[b] for b in range(4)])
    for copy in copies[5:]:
        copy.wait()


def pack_y(rx_a, rx_b, corner_a, corner_b):
    rx, pair = (rx_a, rx_b), (corner_a, corner_b)
    for c in range(3):
        for i in range(4):
            pack_rows4(pair, 4 * c + i, lambda p, o: tile_of(None, c, p, o, 4, rx, 0, None), i, 20 + i)
        pack_rows2(pair, 12 + c, lambda p, o: tile_of(None, c, p, o, 2, rx, 12, None), [0, 1, 18, 19])
    pack_phase(pair, 15, [phase_rows(None, rx, 0), phase_rows(None, rx, 5)])


def halo(pair, axis, index):
    even, has_lo, has_hi = position(axis)
    a, b = pair[0][index], pair[1][index]
    lo = jnp.where(has_lo, jnp.where(even, b, a), 0.0)
    hi = jnp.where(has_hi, jnp.where(even, a, b), 0.0)
    return lo, hi


def tile_of(own, c, plane, o, width, rx, base, ry):
    rows = slice(8 * o, 8 * o + 8)
    if o == 4:
        sub = subs()
        inside = width <= plane < NX + width
        pair = ry[0] if inside else ry[1]
        at = plane - width if inside else plane if plane < width else plane - NX
        if width == 4:
            half = 8 if inside else 4
            lo, hi = halo(pair, "gy", half * c + at % half)
            if at < half:
                return jnp.where(sub < 4, hi, roll(lo, 4, 0))
            return jnp.where(sub < 4, roll(hi, 4, 0), lo)
        lo, hi = halo(pair, "gy", 24 + 4 * c + at % 4 if inside else 12 + c)
        k = at // 4 if inside else at
        return jnp.where(sub < 4, roll(hi, -2 * k, 0), roll(lo, 6 - 2 * k, 0))
    if plane < width:
        return halo(rx, "gx", (base + width * c + plane, rows))[0]
    if plane >= NX + width:
        return halo(rx, "gx", (base + width * c + plane - NX - width, rows))[1]
    return own[c, plane - width, rows]


def phase_rows(phase, rx, b):
    if b == 0:
        return halo(rx, "gx", (18, slice(0, 8)))[0]
    if b == 5:
        return halo(rx, "gx", (18, slice(0, 8)))[1]
    return phase[b - 1]


def phase_tiles(phase, rx, ry):
    own, corner = halo(ry[0], "gy", 36), halo(ry[1], "gy", 15)
    sub = subs()
    tiles = []
    for b in range(6):
        tiles.append(phase_rows(phase, rx, b))
        lo, hi = own if 0 < b < 5 else corner
        row = b - 1 if 0 < b < 5 else b // 5
        outer = jnp.where(sub == 0, hi[row : row + 1], jnp.where(sub == 1, lo[row : row + 1], 0.0))
        tiles.append(outer)
    return tiles


def slots():
    lane = lanes()
    return lane >> 5, lane & 31


def edge_tile(tile, i, low_plane, planes):
    slot, pos = slots()
    value = jnp.zeros((8, 128), F32)
    for g in range(4):
        plane = 6 * g + i - low_plane
        if not 0 <= plane < planes:
            continue
        own = tile(plane)
        here = slot == g
        value = jnp.where(here & (pos < 16), roll(own, 32 * g + 4, 1), value)
        value = jnp.where(here & (pos >= 16), roll(own, 32 * g + 28, 1), value)
    return jnp.where(((pos >= 4) & (pos < 12)) | ((pos >= 20) & (pos < 28)), value, 0.0)


def edge_own(vel, forc, rx_a, rx_b, eu, ef):
    rx = (rx_a, rx_b)
    for c in range(3):
        for i in range(6):
            for o in range(4):
                rows = slice(8 * o, 8 * o + 8)
                eu[c, i, rows] = edge_tile(lambda p: tile_of(vel, c, p, o, 4, rx, 0, None), i, 0, 24)
                ef[c, i, rows] = edge_tile(lambda p: tile_of(forc, c, p, o, 2, rx, 12, None), i, 2, 20)


def pack_z(phase, rx_a, rx_b, ryo_a, ryo_b, ryc_a, ryc_b, eu, ef, send_a, send_b, eu4, ef4, tiles):
    rx, ry = (rx_a, rx_b), ((ryo_a, ryo_b), (ryc_a, ryc_b))
    even, _, _ = position("gz")

    def put(index, lo, hi):
        send_a[index] = jnp.where(even, hi, lo)
        send_b[index] = jnp.where(even, lo, hi)

    lane = lanes()
    place = (lane & 31) >> 2
    for c in range(3):
        for i in range(6):
            eu4[c, i] = edge_tile(lambda p: tile_of(None, c, p, 4, 4, rx, 0, ry), i, 0, 24)
            ef4[c, i] = edge_tile(lambda p: tile_of(None, c, p, 4, 2, rx, 12, ry), i, 2, 20)
    for base, own, own4 in ((0, eu, eu4), (12, ef, ef4)):
        for w in range(12):
            lo = jnp.zeros((8, 128), F32)
            hi = lo
            for k in range(min(8, 90 - 8 * w)):
                n = 8 * w + k
                c, i, o = n // 30, n // 5 % 6, n % 5
                tile = own4[c, i] if o == 4 else own[c, i, 8 * o : 8 * o + 8]
                lo = jnp.where(place == k, roll(tile, 4 * k - 4, 1), lo)
                hi = jnp.where(place == k, roll(tile, 4 * k - 24, 1), hi)
            put(base + w, lo, hi)
    lo = jnp.zeros((8, 128), F32)
    hi = lo
    for j, tile in enumerate(phase_tiles(phase, rx, ry)):
        tiles[j] = tile
        lo = jnp.where(lane == j, roll(tile, j, 1), lo)
        hi = jnp.where(lane == j, roll(tile, j - 31, 1), hi)
    put(24, lo, hi)


def exact_dot(a, b):
    return jnp.dot(a, b, preferred_element_type=F32, precision=lax.Precision.HIGHEST)


def four(a, b, c, d):
    return (a + 3.0 * b + 3.0 * c + d) * 0.125


def put_rows(ref, index, o, value):
    ref[index + (slice(8 + 8 * o, 16 + 8 * o),)] = value
    if o == 0:
        ref[index + (slice(48, 56),)] = value
    if o == 4:
        ref[index + (slice(0, 8),)] = value


def tables(tiles, wide, pre, yld, creep, limit):
    block = lax.broadcasted_iota(jnp.int32, (128, 128), 0)
    spread = jnp.dot(
        jnp.concatenate(tiles, axis=0), (wide == block).astype(F32), preferred_element_type=F32
    )
    row = lax.broadcasted_iota(jnp.int32, (40, 16), 0)
    by = lax.broadcasted_iota(jnp.int32, (40, 16), 1)
    tall = (jnp.where(row < 32, row >> 2, jnp.where(row < 36, 8, 9)) == by).astype(F32)
    for b in range(6):
        phase = jnp.dot(tall, spread[16 * b : 16 * b + 16], preferred_element_type=F32)
        first = jnp.full(phase.shape, pre[0], F32)
        second = jnp.full(phase.shape, yld[0], F32)
        for k in range(1, 8):
            here = phase == float(k)
            first = jnp.where(here, pre[k], first)
            second = jnp.where(here, yld[k], second)
        creep[b] = first
        limit[b] = 0.5 * second


def viscosity_tile(u, creep, limit):
    d = []
    for c in range(3):
        mid = u(c, 0, 0)
        d.append((u(c, 1, 0) - u(c, -1, 0), u(c, 0, 1) - u(c, 0, -1), roll(mid, 127, 1) - roll(mid, 1, 1)))
    a01, a02, a12 = d[0][1] + d[1][0], d[0][2] + d[2][0], d[1][2] + d[2][1]
    own = d[0][0] * d[0][0] + d[1][1] * d[1][1] + d[2][2] * d[2][2]
    off = a01 * a01 + a02 * a02 + a12 * a12
    invariant = 1.0 + (own * 0.125 + off * 0.0625)
    return jnp.minimum(creep * jnp.exp(jnp.log(invariant) * (-1.0 / 3.0)), limit * lax.rsqrt(invariant))


def around(ref, index, o):
    head, p = index[:-1], index[-1]
    mid = ref[head + (p, slice(8 + 8 * o, 16 + 8 * o))]
    return mid, (
        ref[head + (p + 1, slice(8 + 8 * o, 16 + 8 * o))],
        ref[head + (p - 1, slice(8 + 8 * o, 16 + 8 * o))],
        ref[head + (p, slice(9 + 8 * o, 17 + 8 * o))],
        ref[head + (p, slice(7 + 8 * o, 15 + 8 * o))],
        roll(mid, 127, 1),
        roll(mid, 1, 1),
    )


def faces(v_ref, vx, o):
    mid, near = around(v_ref, (vx,), o)
    f = [mid + value for value in near]
    return mid, f, (f[0] + f[1]) + (f[2] + f[3]) + (f[4] + f[5])


def weighted(ref, index, o, f):
    mid, near = around(ref, index, o)
    total = f[0] * near[0]
    for k in range(1, 6):
        total = total + f[k] * near[k]
    return mid, total


def relax(mid_v, diag):
    return jnp.where(mid_v > 0.0, 0.8 / diag, 0.0)


def flags(axis):
    return tuple(flag.astype(F32) for flag in position(axis)[1:])


def main_work(
    vel, forc, phase_ref, rx_a, rx_b, ryo_a, ryo_b, ryc_a, ryc_b, pre, yld,
    v_own, u_own, residual, square,
    u_ref, f_ref, creep, limit, v_ref, u1, u2, sems,
):
    rx, ry = (rx_a, rx_b), ((ryo_a, ryo_b), (ryc_a, ryc_b))
    lo_x, hi_x = flags("gx")
    lo_y, hi_y = flags("gy")
    for c in range(3):
        for p in range(24):
            for o in range(5):
                put_rows(u_ref, (c, p), o, tile_of(vel, c, p, o, 4, rx, 0, ry))
        for p in range(20):
            for o in range(5):
                f_ref[c, p, 8 * o : 8 * o + 8] = tile_of(forc, c, p, o, 2, rx, 12, ry)
    wide = lax.broadcasted_iota(jnp.int32, (128, 128), 1) >> 2
    tables(phase_tiles(phase_ref, rx, ry), wide, pre, yld, creep, limit)
    mask_y = jnp.where(subs() < 4, hi_y, lo_y)

    def viscosity(vx, _):
        mask_x = jnp.where(vx < 3, lo_x, jnp.where(vx >= 19, hi_x, 1.0))
        bx = (vx + 1) >> 2
        for o in range(5):
            value = viscosity_tile(
                lambda c, dx, dy: u_ref[c, vx + 1 + dx, 8 + 8 * o + dy : 16 + 8 * o + dy],
                creep[bx, 8 * o : 8 * o + 8], limit[bx, 8 * o : 8 * o + 8],
            )
            value = value * (mask_y * mask_x if o == 4 else mask_x)
            put_rows(v_ref, (vx,), o, value)
        return 0

    lax.fori_loop(0, 22, viscosity, 0, unroll=2)
    copy_v = pltpu.make_async_copy(v_ref.at[:, 8:48], v_own, sems.at[0])
    copy_v.start()

    def sweep(source, target, first, first_u):
        def body(x, _):
            for o in range(5):
                mid_v, f, diag = faces(v_ref, x + first, o)
                rate = relax(mid_v, diag)
                for c in range(3):
                    mid, total = weighted(source, (c, x + first_u), o, f)
                    force = f_ref[c, x + first - 1, 8 * o : 8 * o + 8]
                    put_rows(target, (c, x), o, 0.2 * mid + rate * (2.0 * force + total))
            return 0

        return body

    lax.fori_loop(0, 20, sweep(u_ref, u1, 1, 2), 0, unroll=4)
    lax.fori_loop(0, 18, sweep(u1, u2, 2, 1), 0, unroll=3)
    copy_u = pltpu.make_async_copy(u2.at[:, 1:17, 8:40], u_own, sems.at[1])
    copy_u.start()

    def last(x, acc):
        for o in range(4):
            _, f, diag = faces(v_ref, x + 3, o)
            for c in range(3):
                mid, total = weighted(u2, (c, x + 1), o, f)
                value = f_ref[c, x + 2, 8 * o : 8 * o + 8] + 0.5 * (total - diag * mid)
                residual[c, x, 8 * o : 8 * o + 8] = value
                acc = acc + value * value
        return acc

    acc = lax.fori_loop(0, NX, last, jnp.zeros((8, 128), F32), unroll=4)
    lane = lanes()
    square[...] = jnp.where((lane >= 4) & (lane < 124), acc, 0.0)
    copy_v.wait()
    copy_u.wait()


def put_edge(ref, index, i, o, value):
    put_rows(ref, index + (i + 1,), o, value)


def wrap_planes(ref, lead):
    for index in lead:
        for r in range(7):
            rows = slice(8 * r, 8 * r + 8)
            ref[index + (0, rows)] = roll(ref[index + (6, rows)], 32, 1)
            ref[index + (7, rows)] = roll(ref[index + (1, rows)], -32, 1)


def edge_work(
    rz_a, rz_b, eu, ef, eu4, ef4, phases, square, pre, yld,
    v_out, u_out, r_out, total_out,
    u_ref, f_ref, creep, limit, creep_e, limit_e, v_ref, u1, u2,
):
    rz = (rz_a, rz_b)
    lo_x, hi_x = flags("gx")
    lo_y, hi_y = flags("gy")
    lo_z, hi_z = flags("gz")
    lane = lanes()
    slot, pos = slots()
    lead = ((0,), (1,), (2,))
    for base, own, own4 in ((0, eu, eu4), (12, ef, ef4)):
        for w in range(12):
            lo, hi = halo(rz, "gz", base + w)
            for k in range(min(8, 90 - 8 * w)):
                n = 8 * w + k
                c, i, o = n // 30, n // 5 % 6, n % 5
                tile = own4[c, i] if o == 4 else own[c, i, 8 * o : 8 * o + 8]
                tile = jnp.where(pos < 4, roll(lo, -4 * k, 1), tile)
                tile = jnp.where(pos >= 28, roll(hi, 28 - 4 * k, 1), tile)
                if base == 0:
                    put_edge(u_ref, (c,), i, o, tile)
                else:
                    f_ref[c, i, 8 * o : 8 * o + 8] = tile
    wrap_planes(u_ref, lead)

    lo, hi = halo(rz, "gz", 24)
    tiles = []
    for j in range(12):
        tile = jnp.where(lane == 32, roll(hi, 32 - j, 1), phases[j])
        tiles.append(jnp.where(lane == 33, roll(lo, 33 - j, 1), tile))
    at = lax.broadcasted_iota(jnp.int32, (128, 128), 1) & 31
    wide = jnp.where(at < 4, 33, jnp.where(at < 12, (at - 4) >> 2, jnp.where(at < 20, 127, 25 + (at >> 2))))
    tables(tiles, wide, pre, yld, creep, limit)
    for i in range(6):
        first, second = creep[i // 4], limit[i // 4]
        slot40 = lanes(40) >> 5
        for g in range(1, 4):
            b = (6 * g + i) // 4
            first = jnp.where(slot40 == g, creep[b], first)
            second = jnp.where(slot40 == g, limit[b], second)
        creep_e[i] = first
        limit_e[i] = second

    mask_z = jnp.where(pos < 4, lo_z, jnp.where(pos >= 28, hi_z, jnp.where((pos < 12) | (pos >= 20), 1.0, 0.0)))
    mask_y = jnp.where(subs() < 4, hi_y, lo_y)

    def viscosity(i, _):
        px = 6 * slot + i
        mask = mask_z * jnp.where(px < 4, lo_x, jnp.where(px >= 20, hi_x, 1.0))
        for o in range(5):
            value = viscosity_tile(
                lambda c, dx, dy: u_ref[c, i + 1 + dx, 8 + 8 * o + dy : 16 + 8 * o + dy],
                creep_e[i, 8 * o : 8 * o + 8], limit_e[i, 8 * o : 8 * o + 8],
            )
            value = value * (mask * mask_y if o == 4 else mask)
            put_edge(v_ref, (), i, o, value)
            v_out[i, 8 * o : 8 * o + 8] = value
        return 0

    lax.fori_loop(0, 6, viscosity, 0, unroll=6)
    wrap_planes(v_ref, ((),))

    def sweep(source, target):
        def body(i, _):
            for o in range(5):
                mid_v, f, diag = faces(v_ref, i + 1, o)
                rate = relax(mid_v, diag)
                for c in range(3):
                    mid, total = weighted(source, (c, i + 1), o, f)
                    force = f_ref[c, i, 8 * o : 8 * o + 8]
                    put_edge(target, (c,), i, o, 0.2 * mid + rate * (2.0 * force + total))
            return 0

        lax.fori_loop(0, 6, body, 0, unroll=6)
        wrap_planes(target, lead)

    sweep(u_ref, u1)
    sweep(u1, u2)

    def last(i, acc):
        px = 6 * slot + i
        count = (px >= 4) & (px < 20) & (((pos >= 4) & (pos < 8)) | ((pos >= 24) & (pos < 28)))
        for o in range(4):
            _, f, diag = faces(v_ref, i + 1, o)
            for c in range(3):
                mid, total = weighted(u2, (c, i + 1), o, f)
                value = f_ref[c, i, 8 * o : 8 * o + 8] + 0.5 * (total - diag * mid)
                r_out[c, i, 8 * o : 8 * o + 8] = value
                u_out[c, i, 8 * o : 8 * o + 8] = mid
                acc = acc + jnp.where(count, value * value, 0.0)
        return acc

    acc = lax.fori_loop(0, 6, last, square[...], unroll=6)
    total = jnp.sum(jnp.sum(acc, axis=1, keepdims=True), axis=0, keepdims=True)
    total_out[...] = jnp.broadcast_to(total, (1, 128))


def band(rows, row_z, col_m):
    row = row_z(lax.broadcasted_iota(jnp.int32, (rows, 128), 0))
    col = col_m(lax.broadcasted_iota(jnp.int32, (rows, 128), 1))
    at = row - 2 * col + 1
    return jnp.where((at == 0) | (at == 3), 0.125, jnp.where((at == 1) | (at == 2), 0.375, 0.0)).astype(F32)


def merge(own, edge, g):
    lane = lanes()
    value = jnp.where(lane < 4, roll(edge, -32 * g - 4, 1), own)
    return jnp.where(lane >= 124, roll(edge, 100 - 32 * g, 1), value)


def results(v_own, u_own, residual_in, ve, ue, re, one, two, smoothed, visc_out, one_out, two_out, residual):
    one_out[...] = one[...]
    two_out[...] = two[...]
    for x in range(NX):
        g, i = (x + 4) // 6, (x + 4) % 6
        for c in range(3):
            for o in range(4):
                rows = slice(8 * o, 8 * o + 8)
                smoothed[c, x, rows] = merge(u_own[c, x, rows], ue[c, i, rows], g)
                residual[c, x, rows] = merge(residual_in[c, x, rows], re[c, i, rows], g)
        for o in range(4):
            rows = slice(8 * o, 8 * o + 8)
            visc_out[x, rows] = merge(v_own[x + 3, rows], ve[i, rows], g)


def coarsen(
    v_own, ve, total,
    one_out, two_out, send,
    v_m, v_s, w_m, w_s, y1, c1, t2, t3, parts,
):
    lo_x, hi_x = flags("gx")
    lo_y, hi_y = flags("gy")
    lo_z, hi_z = flags("gz")
    lane = lanes()
    for vx in range(22):
        g, i = (vx + 1) // 6, (vx + 1) % 6
        for o in range(5):
            edge = ve[i, 8 * o : 8 * o + 8]
            value = merge(v_own[vx, 8 * o : 8 * o + 8], edge, g)
            put_rows(v_m, (vx,), o, value)
            side = jnp.where(lane < 4, roll(edge, -28 - 32 * g, 1), 0.0)
            put_rows(v_s, (vx,), o, jnp.where(lane >= 124, roll(edge, 124 - 32 * g, 1), side))

    def coarse_x(k, _):
        w_m[k] = four(v_m[2 * k], v_m[2 * k + 1], v_m[2 * k + 2], v_m[2 * k + 3])
        w_s[k] = four(v_s[2 * k], v_s[2 * k + 1], v_s[2 * k + 2], v_s[2 * k + 3])
        return 0

    lax.fori_loop(0, 10, coarse_x, 0)
    y1[...] = jnp.zeros(y1.shape, F32)
    for k in range(10):
        for ref, at in ((w_m, 0), (w_s, 128)):
            y1[k, 0:18, at : at + 128] = four(*(ref[k, pl.ds(5 + i, 18, stride=2)] for i in range(4)))
    band1 = band(256, lambda r: jnp.where(r < 192, r, r - 256), lambda m: jnp.where(m < 65, m, jnp.where(m == 65, -1, 1000)))
    coarse = exact_dot(y1[...].reshape(240, 256), band1).reshape(10, 24, 128)
    row24, lane24 = subs(24), lanes(24)
    mask_yz = jnp.where(row24 == 0, lo_y, jnp.where(row24 == 17, hi_y, 1.0)) * jnp.where(
        lane24 == 64, hi_z, jnp.where(lane24 == 65, lo_z, 1.0)
    )
    for k in range(10):
        mask = mask_yz * (lo_x if k == 0 else hi_x if k == 9 else 1.0)
        c1[k] = coarse[k] * mask
    for k in range(8):
        one_out[k] = c1[k + 1, 1:17, 0:64]
    rows = []
    for k in range(4):
        t2[...] = four(c1[2 * k], c1[2 * k + 1], c1[2 * k + 2], c1[2 * k + 3])
        rows.append(four(*(t2[pl.ds(i, 8, stride=2)] for i in range(4))))
    band2 = band(128, lambda r: jnp.where(r < 65, r, jnp.where(r == 65, -1, 100000)), lambda m: jnp.where(m < 32, m, 1000))
    coarse = exact_dot(jnp.concatenate(rows, axis=0), band2)
    planes = [coarse[8 * k : 8 * k + 8] for k in range(4)]
    for k in range(4):
        two_out[k] = planes[k][:, 0:32]
    thirds = (
        0.125 * planes[0],
        0.125 * (3.0 * planes[0] + 3.0 * planes[1] + planes[2]),
        0.125 * (planes[1] + 3.0 * planes[2] + 3.0 * planes[3]),
        0.125 * planes[3],
    )
    rows = []
    t3[...] = jnp.zeros(t3.shape, F32)
    for k in range(4):
        t3[4:12] = thirds[k]
        rows.append(four(*(t3[pl.ds(1 + i, 8, stride=2)] for i in range(4))))
    band3 = band(128, lambda r: jnp.where(r < 32, r, 100000), lambda m: jnp.where(m < 18, m - 1, 1000))
    coarse = exact_dot(jnp.concatenate(rows, axis=0), band3)
    sub = subs()
    part = []
    for k in range(4):
        tile = coarse[8 * k : 8 * k + 8]
        ends = {
            -1: jnp.where(lane == 15, roll(tile, 15, 1), 0.0),
            0: jnp.where(lane < 16, roll(tile, -1, 1), 0.0),
            1: jnp.where(lane == 0, roll(tile, -17, 1), 0.0),
        }
        part.append({})
        for dz, value in ends.items():
            apart = pltpu.roll(value, 0, 1, stride=16, stride_axis=0)
            for dy, row, shift in ((-1, sub == 0, 48), (0, (sub >= 1) & (sub < 5), 112), (1, sub == 5, 48)):
                part[k][dy, dz] = roll(jnp.sum(jnp.where(row, apart, 0.0), axis=0, keepdims=True), shift, 1)
    offsets = [(dx, dy, dz) for dx in (-1, 0, 1) for dy in (-1, 0, 1) for dz in (-1, 0, 1)]
    for k, (dx, dy, dz) in enumerate(offsets):
        if dx == 0:
            value = part[1][dy, dz] + roll(part[2][dy, dz], 64, 1)
        else:
            value = part[3][dy, dz] if dx == 1 else roll(part[0][dy, dz], 64, 1)
        parts[k] = value
    mine = [lax.axis_index(axis) for axis in AX]
    size = [lax.axis_size(axis) for axis in AX]
    square = total[...]
    nothing = jnp.concatenate([square, jnp.zeros((1, 128), F32)], axis=1)

    def fill(r, _):
        send[r] = nothing
        return 0

    lax.fori_loop(0, send.shape[0], fill, 0, unroll=8)
    for k, offset in enumerate(offsets):
        at = [here + step for here, step in zip(mine, offset)]
        inside = functools.reduce(lambda a, b: a & b, [(p >= 0) & (p < n) for p, n in zip(at, size)])

        @pl.when(inside)
        def _():
            send[(at[0] * size[1] + at[1]) * size[2] + at[2], :, 128:256] = parts[k]


def per_device(velocity, forcing, phase_block, prefactor, yield_stress):
    send_a, send_b, own_a, own_b, phase = pl.pallas_call(
        pack_xy, out_shape=[sds(19, 32, 128)] * 2 + [sds(37, 8, 128)] * 2 + [sds(4, 8, 128)],
        in_specs=[HBM] * 3, out_specs=[VMEM] * 5,
        scratch_shapes=[
            pltpu.VMEM((4, 8, 32), jnp.int32), pltpu.VMEM((2, 3, 16, 8, 128), F32),
            pltpu.VMEM((2, 3, 16, 8, 128), F32), pltpu.SemaphoreType.DMA((17,)),
        ],
        compiler_params=params(LIM), name="pack_xy",
    )(*(pltpu.with_memory_space_constraint(value, pltpu.HBM) for value in (velocity, forcing, phase_block)))
    own = (velocity, forcing, phase)
    rx = (pair_a(send_a, "gx"), pair_b(send_b, "gx"))
    ry = (pair_a(own_a, "gy"), pair_b(own_b, "gy"))
    corner_a, corner_b = pl.pallas_call(
        pack_y, out_shape=[sds(16, 8, 128)] * 2, in_specs=[VMEM] * 2, out_specs=[VMEM] * 2,
        compiler_params=params(LIM), name="pack_y",
    )(*rx)
    ry = ry + (pair_a(corner_a, "gy"), pair_b(corner_b, "gy"))
    eu, ef = pl.pallas_call(
        edge_own, out_shape=[sds(3, 6, 32, 128)] * 2, in_specs=[VMEM] * 4, out_specs=[VMEM] * 2,
        compiler_params=params(LIM), cost_estimate=cost(3 << 23), name="edge_own",
    )(velocity, forcing, *rx)
    send_a, send_b, eu4, ef4, tiles = pl.pallas_call(
        pack_z, out_shape=[sds(25, 8, 128)] * 2 + [sds(3, 6, 8, 128)] * 2 + [sds(12, 8, 128)],
        in_specs=[VMEM] * 9, out_specs=[VMEM] * 5, compiler_params=params(LIM), name="pack_z",
    )(phase, *rx, *ry, eu, ef)
    rz = (pair_a(send_a, "gz"), pair_b(send_b, "gz"))
    v, u2, res, square = pl.pallas_call(
        main_work,
        out_shape=[pltpu.HBM((22, 40, 128), F32), pltpu.HBM((3, NX, NY, NZ), F32), sds(3, NX, NY, NZ), sds(8, 128)],
        in_specs=[VMEM] * 9 + [SMEM] * 2, out_specs=[HBM] * 2 + [VMEM] * 2,
        scratch_shapes=[
            pltpu.VMEM((3, 24, 56, 128), F32), pltpu.VMEM((3, 20, 40, 128), F32),
            pltpu.VMEM((6, 40, 128), F32), pltpu.VMEM((6, 40, 128), F32), pltpu.VMEM((22, 56, 128), F32),
            pltpu.VMEM((3, 20, 56, 128), F32), pltpu.VMEM((3, 18, 56, 128), F32), pltpu.SemaphoreType.DMA((2,)),
        ],
        compiler_params=params(LIM), cost_estimate=cost(1 << 25), name="main_work",
    )(*own, *rx, *ry, prefactor, yield_stress)
    ve, ue, re, total = pl.pallas_call(
        edge_work,
        out_shape=[sds(6, 40, 128), sds(3, 6, 32, 128), sds(3, 6, 32, 128), sds(1, 128)],
        in_specs=[VMEM] * 8 + [SMEM] * 2, out_specs=[VMEM] * 4,
        scratch_shapes=[
            pltpu.VMEM((3, 8, 56, 128), F32), pltpu.VMEM((3, 6, 40, 128), F32),
            *[pltpu.VMEM((6, 40, 128), F32)] * 4,
            pltpu.VMEM((8, 56, 128), F32), pltpu.VMEM((3, 8, 56, 128), F32), pltpu.VMEM((3, 8, 56, 128), F32),
        ],
        compiler_params=params(LIM), cost_estimate=cost(1 << 23), name="edge_work",
    )(*rz, eu, ef, eu4, ef4, tiles, square, prefactor, yield_stress)
    devices = 1
    for axis in AX:
        devices = devices * lax.axis_size(axis)
    one, two, send = pl.pallas_call(
        coarsen,
        out_shape=[sds(8, 16, 64), sds(4, 8, 32), sds(devices, 1, 256)],
        in_specs=[VMEM] * 3, out_specs=[VMEM] * 3,
        scratch_shapes=[
            pltpu.VMEM((22, 56, 128), F32), pltpu.VMEM((22, 56, 128), F32),
            pltpu.VMEM((10, 56, 128), F32), pltpu.VMEM((10, 56, 128), F32), pltpu.VMEM((10, 24, 256), F32),
            pltpu.VMEM((10, 24, 128), F32), pltpu.VMEM((24, 128), F32), pltpu.VMEM((24, 128), F32),
            pltpu.VMEM((27, 1, 128), F32),
        ],
        compiler_params=params(LIM), cost_estimate=cost(1 << 22), name="coarsen",
    )(v, ve, total)
    sums = jnp.sum(lax.all_to_all(send, AX, 0, 0, tiled=True), axis=0)[0]
    smoothed, visc, one, two, residual = pl.pallas_call(
        results,
        out_shape=[sds(3, NX, NY, NZ), sds(NX, NY, NZ), sds(8, 16, 64), sds(4, 8, 32), sds(3, NX, NY, NZ)],
        in_specs=[VMEM] * 8, out_specs=[VMEM] * 5,
        compiler_params=params(LIM), cost_estimate=cost(1 << 22), name="results",
    )(v, u2, res, ve, ue, re, one, two)
    three = sums[128:].reshape(2, 4, 16)
    cells = 3.0 * NX * NY * NZ
    for axis in AX:
        cells = cells * lax.axis_size(axis)
    return smoothed, visc, one, two, three, residual, jnp.sqrt(sums[0] / cells)


def solution(mesh):
    field, cell = P(None, *AX), P(*AX)
    return jax.shard_map(
        per_device,
        mesh=mesh,
        in_specs=(field, field, cell, P(), P()),
        out_specs=(field, cell, cell, cell, cell, field, P()),
        check_vma=False,
    )
```

```python
import functools

import jax
import jax.numpy as jnp
from jax import lax
from jax.experimental import pallas as pl
from jax.experimental.pallas import tpu as pltpu
from jax.sharding import PartitionSpec as P

F32 = jnp.float32
BLOCK = 4
AX = ("gx", "gy", "gz")
NX, NY, NZ = 16, 32, 128
VMEM = pl.BlockSpec(memory_space=pltpu.VMEM)
HBM = pl.BlockSpec(memory_space=pltpu.HBM)
LIM = 9
SMEM = pl.BlockSpec(memory_space=pltpu.SMEM)


def sds(*shape):
    return jax.ShapeDtypeStruct(shape, F32)


def position(axis):
    index = lax.axis_index(axis)
    return lax.rem(index, 2) == 0, index > 0, index < lax.axis_size(axis) - 1


def lanes(rows=8, width=128):
    return lax.broadcasted_iota(jnp.int32, (rows, width), 1)


def subs(rows=8, width=128):
    return lax.broadcasted_iota(jnp.int32, (rows, width), 0)


def roll(value, shift, axis):
    size = value.shape[axis]
    shift = shift % size
    return pltpu.roll(value, shift, axis) if shift else value


def pair_a(value, axis):
    count = lax.axis_size(axis)
    return lax.ppermute(value, axis, [(i, i ^ 1) for i in range(count)])


def pair_b(value, axis):
    count = lax.axis_size(axis)
    return lax.ppermute(
        value, axis, [(i, (i + 1) % count if i % 2 else (i - 1) % count) for i in range(count)]
    )


def params(mib):
    return pltpu.CompilerParams(vmem_limit_bytes=mib << 20)


def cost(flops):
    return pl.CostEstimate(flops=flops, bytes_accessed=1 << 20, transcendentals=0)


def put_pair(pair, axis, index, lo, hi):
    even = position(axis)[0]
    pair[0][index] = jnp.where(even, hi, lo)
    pair[1][index] = jnp.where(even, lo, hi)


def pack_rows4(pair, index, tile, p, q):
    sub = subs()
    lo = jnp.where(sub < 4, tile(p, 0), roll(tile(q, 0), 4, 0))
    hi = jnp.where(sub < 4, roll(tile(p, 3), 4, 0), tile(q, 3))
    put_pair(pair, "gy", index, lo, hi)


def pack_rows2(pair, index, tile, planes):
    sub = subs()
    lo = tile(planes[0], 0)
    hi = roll(tile(planes[0], 3), 2, 0)
    for k in range(1, 4):
        here = (sub >> 1) == k
        lo = jnp.where(here, roll(tile(planes[k], 0), 2 * k, 0), lo)
        hi = jnp.where(here, roll(tile(planes[k], 3), 2 * k + 2, 0), hi)
    put_pair(pair, "gy", index, lo, hi)


def pack_phase(pair, index, tiles):
    sub = subs()
    lo = jnp.zeros((8, 128), F32)
    hi = lo
    for b, tile in enumerate(tiles):
        lo = jnp.where(sub == b, tile[0:1], lo)
        hi = jnp.where(sub == b, tile[7:8], hi)
    put_pair(pair, "gy", index, lo, hi)


def pack_xy(vel, forc, blocks_in, send_a, send_b, own_a, own_b, phase, blocks, vel_y, forc_y, sems):
    even, _, _ = position("gx")
    pairs = [(blocks_in, blocks)]
    for k in range(2):
        pairs.append((vel.at[:, :, 24 * k : 24 * k + 8], vel_y.at[k]))
        pairs.append((forc.at[:, :, 24 * k : 24 * k + 8], forc_y.at[k]))
    for out, first in ((send_a, jnp.where(even, 1, 0)), (send_b, jnp.where(even, 0, 1))):
        for c in range(3):
            pairs.append((vel.at[c, pl.ds(12 * first, 4)], out.at[4 * c : 4 * c + 4]))
            pairs.append((forc.at[c, pl.ds(14 * first, 2)], out.at[12 + 2 * c : 14 + 2 * c]))
    copies = [pltpu.make_async_copy(source, target, sems.at[k]) for k, (source, target) in enumerate(pairs)]
    for copy in copies:
        copy.start()
    phase[...] = jnp.zeros(phase.shape, F32)
    copies[0].wait()
    for b in range(4):
        phase[b, :, 0:32] = blocks[b].astype(F32)
    send_a[18, 0:8] = jnp.where(even, phase[3], phase[0])
    send_b[18, 0:8] = jnp.where(even, phase[0], phase[3])
    for copy in copies[1:5]:
        copy.wait()
    pair = (own_a, own_b)
    for c in range(3):
        for g in range(8):
            pack_rows4(pair, 8 * c + g, lambda p, o: vel_y[o // 3, c, p], g, g + 8)
        for g in range(4):
            pack_rows2(pair, 24 + 4 * c + g, lambda p, o: forc_y[o // 3, c, p], [g + 4 * k for k in range(4)])
    pack_phase(pair, 36, [phase[b] for b in range(4)])
    for copy in copies[5:]:
        copy.wait()


def pack_y(rx_a, rx_b, corner_a, corner_b):
    rx, pair = (rx_a, rx_b), (corner_a, corner_b)
    for c in range(3):
        for i in range(4):
            pack_rows4(pair, 4 * c + i, lambda p, o: tile_of(None, c, p, o, 4, rx, 0, None), i, 20 + i)
        pack_rows2(pair, 12 + c, lambda p, o: tile_of(None, c, p, o, 2, rx, 12, None), [0, 1, 18, 19])
    pack_phase(pair, 15, [phase_rows(None, rx, 0), phase_rows(None, rx, 5)])


def halo(pair, axis, index):
    even, has_lo, has_hi = position(axis)
    a, b = pair[0][index], pair[1][index]
    lo = jnp.where(has_lo, jnp.where(even, b, a), 0.0)
    hi = jnp.where(has_hi, jnp.where(even, a, b), 0.0)
    return lo, hi


def tile_of(own, c, plane, o, width, rx, base, ry):
    rows = slice(8 * o, 8 * o + 8)
    if o == 4:
        sub = subs()
        inside = width <= plane < NX + width
        pair = ry[0] if inside else ry[1]
        at = plane - width if inside else plane if plane < width else plane - NX
        if width == 4:
            half = 8 if inside else 4
            lo, hi = halo(pair, "gy", half * c + at % half)
            if at < half:
                return jnp.where(sub < 4, hi, roll(lo, 4, 0))
            return jnp.where(sub < 4, roll(hi, 4, 0), lo)
        lo, hi = halo(pair, "gy", 24 + 4 * c + at % 4 if inside else 12 + c)
        k = at // 4 if inside else at
        return jnp.where(sub < 4, roll(hi, -2 * k, 0), roll(lo, 6 - 2 * k, 0))
    if plane < width:
        return halo(rx, "gx", (base + width * c + plane, rows))[0]
    if plane >= NX + width:
        return halo(rx, "gx", (base + width * c + plane - NX - width, rows))[1]
    return own[c, plane - width, rows]


def phase_rows(phase, rx, b):
    if b == 0:
        return halo(rx, "gx", (18, slice(0, 8)))[0]
    if b == 5:
        return halo(rx, "gx", (18, slice(0, 8)))[1]
    return phase[b - 1]


def phase_tiles(phase, rx, ry):
    own, corner = halo(ry[0], "gy", 36), halo(ry[1], "gy", 15)
    sub = subs()
    tiles = []
    for b in range(6):
        tiles.append(phase_rows(phase, rx, b))
        lo, hi = own if 0 < b < 5 else corner
        row = b - 1 if 0 < b < 5 else b // 5
        outer = jnp.where(sub == 0, hi[row : row + 1], jnp.where(sub == 1, lo[row : row + 1], 0.0))
        tiles.append(outer)
    return tiles


def slots():
    lane = lanes()
    return lane >> 5, lane & 31


def edge_tile(tile, i, low_plane, planes):
    slot, pos = slots()
    value = jnp.zeros((8, 128), F32)
    for g in range(4):
        plane = 6 * g + i - low_plane
        if not 0 <= plane < planes:
            continue
        own = tile(plane)
        here = slot == g
        value = jnp.where(here & (pos < 16), roll(own, 32 * g + 4, 1), value)
        value = jnp.where(here & (pos >= 16), roll(own, 32 * g + 28, 1), value)
    return jnp.where(((pos >= 4) & (pos < 12)) | ((pos >= 20) & (pos < 28)), value, 0.0)


def edge_own(vel, forc, rx_a, rx_b, eu, ef):
    rx = (rx_a, rx_b)
    for c in range(3):
        for i in range(6):
            for o in range(4):
                rows = slice(8 * o, 8 * o + 8)
                eu[c, i, rows] = edge_tile(lambda p: tile_of(vel, c, p, o, 4, rx, 0, None), i, 0, 24)
                ef[c, i, rows] = edge_tile(lambda p: tile_of(forc, c, p, o, 2, rx, 12, None), i, 2, 20)


def pack_z(phase, rx_a, rx_b, ryo_a, ryo_b, ryc_a, ryc_b, eu, ef, send_a, send_b, eu4, ef4, tiles):
    rx, ry = (rx_a, rx_b), ((ryo_a, ryo_b), (ryc_a, ryc_b))
    even, _, _ = position("gz")

    def put(index, lo, hi):
        send_a[index] = jnp.where(even, hi, lo)
        send_b[index] = jnp.where(even, lo, hi)

    lane = lanes()
    place = (lane & 31) >> 2
    for c in range(3):
        for i in range(6):
            eu4[c, i] = edge_tile(lambda p: tile_of(None, c, p, 4, 4, rx, 0, ry), i, 0, 24)
            ef4[c, i] = edge_tile(lambda p: tile_of(None, c, p, 4, 2, rx, 12, ry), i, 2, 20)
    for base, own, own4 in ((0, eu, eu4), (12, ef, ef4)):
        for w in range(12):
            lo = jnp.zeros((8, 128), F32)
            hi = lo
            for k in range(min(8, 90 - 8 * w)):
                n = 8 * w + k
                c, i, o = n // 30, n // 5 % 6, n % 5
                tile = own4[c, i] if o == 4 else own[c, i, 8 * o : 8 * o + 8]
                lo = jnp.where(place == k, roll(tile, 4 * k - 4, 1), lo)
                hi = jnp.where(place == k, roll(tile, 4 * k - 24, 1), hi)
            put(base + w, lo, hi)
    lo = jnp.zeros((8, 128), F32)
    hi = lo
    for j, tile in enumerate(phase_tiles(phase, rx, ry)):
        tiles[j] = tile
        lo = jnp.where(lane == j, roll(tile, j, 1), lo)
        hi = jnp.where(lane == j, roll(tile, j - 31, 1), hi)
    put(24, lo, hi)


def exact_dot(a, b):
    return jnp.dot(a, b, preferred_element_type=F32, precision=lax.Precision.HIGHEST)


def four(a, b, c, d):
    return (a + 3.0 * b + 3.0 * c + d) * 0.125


def put_rows(ref, index, o, value):
    ref[index + (slice(8 + 8 * o, 16 + 8 * o),)] = value
    if o == 0:
        ref[index + (slice(48, 56),)] = value
    if o == 4:
        ref[index + (slice(0, 8),)] = value


def tables(tiles, wide, pre, yld, creep, limit):
    block = lax.broadcasted_iota(jnp.int32, (128, 128), 0)
    spread = jnp.dot(
        jnp.concatenate(tiles, axis=0), (wide == block).astype(F32), preferred_element_type=F32
    )
    row = lax.broadcasted_iota(jnp.int32, (40, 16), 0)
    by = lax.broadcasted_iota(jnp.int32, (40, 16), 1)
    tall = (jnp.where(row < 32, row >> 2, jnp.where(row < 36, 8, 9)) == by).astype(F32)
    for b in range(6):
        phase = jnp.dot(tall, spread[16 * b : 16 * b + 16], preferred_element_type=F32)
        first = jnp.full(phase.shape, pre[0], F32)
        second = jnp.full(phase.shape, yld[0], F32)
        for k in range(1, 8):
            here = phase == float(k)
            first = jnp.where(here, pre[k], first)
            second = jnp.where(here, yld[k], second)
        creep[b] = first
        limit[b] = 0.5 * second


def viscosity_tile(u, creep, limit):
    d = []
    for c in range(3):
        mid = u(c, 0, 0)
        d.append((u(c, 1, 0) - u(c, -1, 0), u(c, 0, 1) - u(c, 0, -1), roll(mid, 127, 1) - roll(mid, 1, 1)))
    a01, a02, a12 = d[0][1] + d[1][0], d[0][2] + d[2][0], d[1][2] + d[2][1]
    own = d[0][0] * d[0][0] + d[1][1] * d[1][1] + d[2][2] * d[2][2]
    off = a01 * a01 + a02 * a02 + a12 * a12
    invariant = 1.0 + (own * 0.125 + off * 0.0625)
    return jnp.minimum(creep * jnp.exp(jnp.log(invariant) * (-1.0 / 3.0)), limit * lax.rsqrt(invariant))


def around(ref, index, o):
    head, p = index[:-1], index[-1]
    mid = ref[head + (p, slice(8 + 8 * o, 16 + 8 * o))]
    return mid, (
        ref[head + (p + 1, slice(8 + 8 * o, 16 + 8 * o))],
        ref[head + (p - 1, slice(8 + 8 * o, 16 + 8 * o))],
        ref[head + (p, slice(9 + 8 * o, 17 + 8 * o))],
        ref[head + (p, slice(7 + 8 * o, 15 + 8 * o))],
        roll(mid, 127, 1),
        roll(mid, 1, 1),
    )


def faces(v_ref, vx, o):
    mid, near = around(v_ref, (vx,), o)
    f = [mid + value for value in near]
    return mid, f, (f[0] + f[1]) + (f[2] + f[3]) + (f[4] + f[5])


def weighted(ref, index, o, f):
    mid, near = around(ref, index, o)
    total = f[0] * near[0]
    for k in range(1, 6):
        total = total + f[k] * near[k]
    return mid, total


def relax(mid_v, diag):
    return jnp.where(mid_v > 0.0, 0.8 / diag, 0.0)


def flags(axis):
    return tuple(flag.astype(F32) for flag in position(axis)[1:])


def main_work(
    vel, forc, phase_ref, rx_a, rx_b, ryo_a, ryo_b, ryc_a, ryc_b, pre, yld,
    v_own, u_own, residual, square,
    u_ref, f_ref, creep, limit, v_ref, u1, u2, sems,
):
    rx, ry = (rx_a, rx_b), ((ryo_a, ryo_b), (ryc_a, ryc_b))
    lo_x, hi_x = flags("gx")
    lo_y, hi_y = flags("gy")
    for c in range(3):
        for p in range(24):
            for o in range(5):
                put_rows(u_ref, (c, p), o, tile_of(vel, c, p, o, 4, rx, 0, ry))
        for p in range(20):
            for o in range(5):
                f_ref[c, p, 8 * o : 8 * o + 8] = tile_of(forc, c, p, o, 2, rx, 12, ry)
    wide = lax.broadcasted_iota(jnp.int32, (128, 128), 1) >> 2
    tables(phase_tiles(phase_ref, rx, ry), wide, pre, yld, creep, limit)
    mask_y = jnp.where(subs() < 4, hi_y, lo_y)

    def viscosity(vx, _):
        mask_x = jnp.where(vx < 3, lo_x, jnp.where(vx >= 19, hi_x, 1.0))
        bx = (vx + 1) >> 2
        for o in range(5):
            value = viscosity_tile(
                lambda c, dx, dy: u_ref[c, vx + 1 + dx, 8 + 8 * o + dy : 16 + 8 * o + dy],
                creep[bx, 8 * o : 8 * o + 8], limit[bx, 8 * o : 8 * o + 8],
            )
            value = value * (mask_y * mask_x if o == 4 else mask_x)
            put_rows(v_ref, (vx,), o, value)
        return 0

    lax.fori_loop(0, 22, viscosity, 0, unroll=22)
    copy_v = pltpu.make_async_copy(v_ref.at[:, 8:48], v_own, sems.at[0])
    copy_v.start()

    def sweep(source, target, first, first_u):
        def body(x, _):
            for o in range(5):
                mid_v, f, diag = faces(v_ref, x + first, o)
                rate = relax(mid_v, diag)
                for c in range(3):
                    mid, total = weighted(source, (c, x + first_u), o, f)
                    force = f_ref[c, x + first - 1, 8 * o : 8 * o + 8]
                    put_rows(target, (c, x), o, 0.2 * mid + rate * (2.0 * force + total))
            return 0

        return body

    lax.fori_loop(0, 20, sweep(u_ref, u1, 1, 2), 0, unroll=20)
    lax.fori_loop(0, 18, sweep(u1, u2, 2, 1), 0, unroll=18)
    copy_u = pltpu.make_async_copy(u2.at[:, 1:17, 8:40], u_own, sems.at[1])
    copy_u.start()

    def last(x, acc):
        for o in range(4):
            _, f, diag = faces(v_ref, x + 3, o)
            for c in range(3):
                mid, total = weighted(u2, (c, x + 1), o, f)
                value = f_ref[c, x + 2, 8 * o : 8 * o + 8] + 0.5 * (total - diag * mid)
                residual[c, x, 8 * o : 8 * o + 8] = value
                acc = acc + value * value
        return acc

    acc = lax.fori_loop(0, NX, last, jnp.zeros((8, 128), F32), unroll=16)
    lane = lanes()
    square[...] = jnp.where((lane >= 4) & (lane < 124), acc, 0.0)
    copy_v.wait()
    copy_u.wait()


def put_edge(ref, index, i, o, value):
    put_rows(ref, index + (i + 1,), o, value)


def wrap_planes(ref, lead):
    for index in lead:
        for r in range(7):
            rows = slice(8 * r, 8 * r + 8)
            ref[index + (0, rows)] = roll(ref[index + (6, rows)], 32, 1)
            ref[index + (7, rows)] = roll(ref[index + (1, rows)], -32, 1)


def edge_work(
    rz_a, rz_b, eu, ef, eu4, ef4, phases, square, pre, yld,
    v_out, u_out, r_out, total_out,
    u_ref, f_ref, creep, limit, creep_e, limit_e, v_ref, u1, u2,
):
    rz = (rz_a, rz_b)
    lo_x, hi_x = flags("gx")
    lo_y, hi_y = flags("gy")
    lo_z, hi_z = flags("gz")
    lane = lanes()
    slot, pos = slots()
    lead = ((0,), (1,), (2,))
    for base, own, own4 in ((0, eu, eu4), (12, ef, ef4)):
        for w in range(12):
            lo, hi = halo(rz, "gz", base + w)
            for k in range(min(8, 90 - 8 * w)):
                n = 8 * w + k
                c, i, o = n // 30, n // 5 % 6, n % 5
                tile = own4[c, i] if o == 4 else own[c, i, 8 * o : 8 * o + 8]
                tile = jnp.where(pos < 4, roll(lo, -4 * k, 1), tile)
                tile = jnp.where(pos >= 28, roll(hi, 28 - 4 * k, 1), tile)
                if base == 0:
                    put_edge(u_ref, (c,), i, o, tile)
                else:
                    f_ref[c, i, 8 * o : 8 * o + 8] = tile
    wrap_planes(u_ref, lead)

    lo, hi = halo(rz, "gz", 24)
    tiles = []
    for j in range(12):
        tile = jnp.where(lane == 32, roll(hi, 32 - j, 1), phases[j])
        tiles.append(jnp.where(lane == 33, roll(lo, 33 - j, 1), tile))
    at = lax.broadcasted_iota(jnp.int32, (128, 128), 1) & 31
    wide = jnp.where(at < 4, 33, jnp.where(at < 12, (at - 4) >> 2, jnp.where(at < 20, 127, 25 + (at >> 2))))
    tables(tiles, wide, pre, yld, creep, limit)
    for i in range(6):
        first, second = creep[i // 4], limit[i // 4]
        slot40 = lanes(40) >> 5
        for g in range(1, 4):
            b = (6 * g + i) // 4
            first = jnp.where(slot40 == g, creep[b], first)
            second = jnp.where(slot40 == g, limit[b], second)
        creep_e[i] = first
        limit_e[i] = second

    mask_z = jnp.where(pos < 4, lo_z, jnp.where(pos >= 28, hi_z, jnp.where((pos < 12) | (pos >= 20), 1.0, 0.0)))
    mask_y = jnp.where(subs() < 4, hi_y, lo_y)

    def viscosity(i, _):
        px = 6 * slot + i
        mask = mask_z * jnp.where(px < 4, lo_x, jnp.where(px >= 20, hi_x, 1.0))
        for o in range(5):
            value = viscosity_tile(
                lambda c, dx, dy: u_ref[c, i + 1 + dx, 8 + 8 * o + dy : 16 + 8 * o + dy],
                creep_e[i, 8 * o : 8 * o + 8], limit_e[i, 8 * o : 8 * o + 8],
            )
            value = value * (mask * mask_y if o == 4 else mask)
            put_edge(v_ref, (), i, o, value)
            v_out[i, 8 * o : 8 * o + 8] = value
        return 0

    lax.fori_loop(0, 6, viscosity, 0, unroll=6)
    wrap_planes(v_ref, ((),))

    def sweep(source, target):
        def body(i, _):
            for o in range(5):
                mid_v, f, diag = faces(v_ref, i + 1, o)
                rate = relax(mid_v, diag)
                for c in range(3):
                    mid, total = weighted(source, (c, i + 1), o, f)
                    force = f_ref[c, i, 8 * o : 8 * o + 8]
                    put_edge(target, (c,), i, o, 0.2 * mid + rate * (2.0 * force + total))
            return 0

        lax.fori_loop(0, 6, body, 0, unroll=6)
        wrap_planes(target, lead)

    sweep(u_ref, u1)
    sweep(u1, u2)

    def last(i, acc):
        px = 6 * slot + i
        count = (px >= 4) & (px < 20) & (((pos >= 4) & (pos < 8)) | ((pos >= 24) & (pos < 28)))
        for o in range(4):
            _, f, diag = faces(v_ref, i + 1, o)
            for c in range(3):
                mid, total = weighted(u2, (c, i + 1), o, f)
                value = f_ref[c, i, 8 * o : 8 * o + 8] + 0.5 * (total - diag * mid)
                r_out[c, i, 8 * o : 8 * o + 8] = value
                u_out[c, i, 8 * o : 8 * o + 8] = mid
                acc = acc + jnp.where(count, value * value, 0.0)
        return acc

    acc = lax.fori_loop(0, 6, last, square[...], unroll=6)
    total = jnp.sum(jnp.sum(acc, axis=1, keepdims=True), axis=0, keepdims=True)
    total_out[...] = jnp.broadcast_to(total, (1, 128))


def band(rows, row_z, col_m):
    row = row_z(lax.broadcasted_iota(jnp.int32, (rows, 128), 0))
    col = col_m(lax.broadcasted_iota(jnp.int32, (rows, 128), 1))
    at = row - 2 * col + 1
    return jnp.where((at == 0) | (at == 3), 0.125, jnp.where((at == 1) | (at == 2), 0.375, 0.0)).astype(F32)


def merge(own, edge, g):
    lane = lanes()
    value = jnp.where(lane < 4, roll(edge, -32 * g - 4, 1), own)
    return jnp.where(lane >= 124, roll(edge, 100 - 32 * g, 1), value)


def results(v_own, u_own, residual_in, ve, ue, re, one, two, smoothed, visc_out, one_out, two_out, residual):
    one_out[...] = one[...]
    two_out[...] = two[...]
    for x in range(NX):
        g, i = (x + 4) // 6, (x + 4) % 6
        for c in range(3):
            for o in range(4):
                rows = slice(8 * o, 8 * o + 8)
                smoothed[c, x, rows] = merge(u_own[c, x, rows], ue[c, i, rows], g)
                residual[c, x, rows] = merge(residual_in[c, x, rows], re[c, i, rows], g)
        for o in range(4):
            rows = slice(8 * o, 8 * o + 8)
            visc_out[x, rows] = merge(v_own[x + 3, rows], ve[i, rows], g)


def coarsen(
    v_own, ve, total,
    one_out, two_out, send,
    v_m, v_s, w_m, w_s, y1, c1, t2, t3, parts,
):
    lo_x, hi_x = flags("gx")
    lo_y, hi_y = flags("gy")
    lo_z, hi_z = flags("gz")
    lane = lanes()
    for vx in range(22):
        g, i = (vx + 1) // 6, (vx + 1) % 6
        for o in range(5):
            edge = ve[i, 8 * o : 8 * o + 8]
            value = merge(v_own[vx, 8 * o : 8 * o + 8], edge, g)
            put_rows(v_m, (vx,), o, value)
            side = jnp.where(lane < 4, roll(edge, -28 - 32 * g, 1), 0.0)
            put_rows(v_s, (vx,), o, jnp.where(lane >= 124, roll(edge, 124 - 32 * g, 1), side))

    def coarse_x(k, _):
        w_m[k] = four(v_m[2 * k], v_m[2 * k + 1], v_m[2 * k + 2], v_m[2 * k + 3])
        w_s[k] = four(v_s[2 * k], v_s[2 * k + 1], v_s[2 * k + 2], v_s[2 * k + 3])
        return 0

    lax.fori_loop(0, 10, coarse_x, 0, unroll=10)
    y1[...] = jnp.zeros(y1.shape, F32)
    for k in range(10):
        for ref, at in ((w_m, 0), (w_s, 128)):
            y1[k, 0:18, at : at + 128] = four(*(ref[k, pl.ds(5 + i, 18, stride=2)] for i in range(4)))
    band1 = band(256, lambda r: jnp.where(r < 192, r, r - 256), lambda m: jnp.where(m < 65, m, jnp.where(m == 65, -1, 1000)))
    coarse = exact_dot(y1[...].reshape(240, 256), band1).reshape(10, 24, 128)
    row24, lane24 = subs(24), lanes(24)
    mask_yz = jnp.where(row24 == 0, lo_y, jnp.where(row24 == 17, hi_y, 1.0)) * jnp.where(
        lane24 == 64, hi_z, jnp.where(lane24 == 65, lo_z, 1.0)
    )
    for k in range(10):
        mask = mask_yz * (lo_x if k == 0 else hi_x if k == 9 else 1.0)
        c1[k] = coarse[k] * mask
    for k in range(8):
        one_out[k] = c1[k + 1, 1:17, 0:64]
    rows = []
    for k in range(4):
        t2[...] = four(c1[2 * k], c1[2 * k + 1], c1[2 * k + 2], c1[2 * k + 3])
        rows.append(four(*(t2[pl.ds(i, 8, stride=2)] for i in range(4))))
    band2 = band(128, lambda r: jnp.where(r < 65, r, jnp.where(r == 65, -1, 100000)), lambda m: jnp.where(m < 32, m, 1000))
    coarse = exact_dot(jnp.concatenate(rows, axis=0), band2)
    planes = [coarse[8 * k : 8 * k + 8] for k in range(4)]
    for k in range(4):
        two_out[k] = planes[k][:, 0:32]
    thirds = (
        0.125 * planes[0],
        0.125 * (3.0 * planes[0] + 3.0 * planes[1] + planes[2]),
        0.125 * (planes[1] + 3.0 * planes[2] + 3.0 * planes[3]),
        0.125 * planes[3],
    )
    rows = []
    t3[...] = jnp.zeros(t3.shape, F32)
    for k in range(4):
        t3[4:12] = thirds[k]
        rows.append(four(*(t3[pl.ds(1 + i, 8, stride=2)] for i in range(4))))
    band3 = band(128, lambda r: jnp.where(r < 32, r, 100000), lambda m: jnp.where(m < 18, m - 1, 1000))
    coarse = exact_dot(jnp.concatenate(rows, axis=0), band3)
    sub = subs()
    part = []
    for k in range(4):
        tile = coarse[8 * k : 8 * k + 8]
        ends = {
            -1: jnp.where(lane == 15, roll(tile, 15, 1), 0.0),
            0: jnp.where(lane < 16, roll(tile, -1, 1), 0.0),
            1: jnp.where(lane == 0, roll(tile, -17, 1), 0.0),
        }
        part.append({})
        for dz, value in ends.items():
            apart = pltpu.roll(value, 0, 1, stride=16, stride_axis=0)
            for dy, row, shift in ((-1, sub == 0, 48), (0, (sub >= 1) & (sub < 5), 112), (1, sub == 5, 48)):
                part[k][dy, dz] = roll(jnp.sum(jnp.where(row, apart, 0.0), axis=0, keepdims=True), shift, 1)
    offsets = [(dx, dy, dz) for dx in (-1, 0, 1) for dy in (-1, 0, 1) for dz in (-1, 0, 1)]
    for k, (dx, dy, dz) in enumerate(offsets):
        if dx == 0:
            value = part[1][dy, dz] + roll(part[2][dy, dz], 64, 1)
        else:
            value = part[3][dy, dz] if dx == 1 else roll(part[0][dy, dz], 64, 1)
        parts[k] = value
    mine = [lax.axis_index(axis) for axis in AX]
    size = [lax.axis_size(axis) for axis in AX]
    square = total[...]
    nothing = jnp.concatenate([square, jnp.zeros((1, 128), F32)], axis=1)

    def fill(r, _):
        send[r] = nothing
        return 0

    lax.fori_loop(0, send.shape[0], fill, 0, unroll=32)
    for k, offset in enumerate(offsets):
        at = [here + step for here, step in zip(mine, offset)]
        inside = functools.reduce(lambda a, b: a & b, [(p >= 0) & (p < n) for p, n in zip(at, size)])

        @pl.when(inside)
        def _():
            send[(at[0] * size[1] + at[1]) * size[2] + at[2], :, 128:256] = parts[k]


def finish(cells, got, three, rms):
    sums = jnp.sum(got[...], axis=0)
    row = sums[:, 128:256]
    for k in range(2):
        for j in range(4):
            three[k, j : j + 1] = roll(row, -16 * (4 * k + j), 1)[:, 0:16]
    rms[...] = jnp.sqrt(sums[:, 0:128] * (1.0 / cells))


def per_device(velocity, forcing, phase_block, prefactor, yield_stress):
    send_a, send_b, own_a, own_b, phase = pl.pallas_call(
        pack_xy, out_shape=[sds(19, 32, 128)] * 2 + [sds(37, 8, 128)] * 2 + [sds(4, 8, 128)],
        in_specs=[HBM] * 3, out_specs=[VMEM] * 5,
        scratch_shapes=[
            pltpu.VMEM((4, 8, 32), jnp.int32), pltpu.VMEM((2, 3, 16, 8, 128), F32),
            pltpu.VMEM((2, 3, 16, 8, 128), F32), pltpu.SemaphoreType.DMA((17,)),
        ],
        compiler_params=params(LIM), name="pack_xy",
    )(*(pltpu.with_memory_space_constraint(value, pltpu.HBM) for value in (velocity, forcing, phase_block)))
    own = (velocity, forcing, phase)
    rx = (pair_a(send_a, "gx"), pair_b(send_b, "gx"))
    ry = (pair_a(own_a, "gy"), pair_b(own_b, "gy"))
    corner_a, corner_b = pl.pallas_call(
        pack_y, out_shape=[sds(16, 8, 128)] * 2, in_specs=[VMEM] * 2, out_specs=[VMEM] * 2,
        compiler_params=params(LIM), name="pack_y",
    )(*rx)
    ry = ry + (pair_a(corner_a, "gy"), pair_b(corner_b, "gy"))
    eu, ef = pl.pallas_call(
        edge_own, out_shape=[sds(3, 6, 32, 128)] * 2, in_specs=[VMEM] * 4, out_specs=[VMEM] * 2,
        compiler_params=params(LIM), cost_estimate=cost(3 << 23), name="edge_own",
    )(velocity, forcing, *rx)
    send_a, send_b, eu4, ef4, tiles = pl.pallas_call(
        pack_z, out_shape=[sds(25, 8, 128)] * 2 + [sds(3, 6, 8, 128)] * 2 + [sds(12, 8, 128)],
        in_specs=[VMEM] * 9, out_specs=[VMEM] * 5, compiler_params=params(LIM), name="pack_z",
    )(phase, *rx, *ry, eu, ef)
    rz = (pair_a(send_a, "gz"), pair_b(send_b, "gz"))
    v, u2, res, square = pl.pallas_call(
        main_work,
        out_shape=[pltpu.HBM((22, 40, 128), F32), pltpu.HBM((3, NX, NY, NZ), F32), sds(3, NX, NY, NZ), sds(8, 128)],
        in_specs=[VMEM] * 9 + [SMEM] * 2, out_specs=[HBM] * 2 + [VMEM] * 2,
        scratch_shapes=[
            pltpu.VMEM((3, 24, 56, 128), F32), pltpu.VMEM((3, 20, 40, 128), F32),
            pltpu.VMEM((6, 40, 128), F32), pltpu.VMEM((6, 40, 128), F32), pltpu.VMEM((22, 56, 128), F32),
            pltpu.VMEM((3, 20, 56, 128), F32), pltpu.VMEM((3, 18, 56, 128), F32), pltpu.SemaphoreType.DMA((2,)),
        ],
        compiler_params=params(LIM), cost_estimate=cost(1 << 25), name="main_work",
    )(*own, *rx, *ry, prefactor, yield_stress)
    ve, ue, re, total = pl.pallas_call(
        edge_work,
        out_shape=[sds(6, 40, 128), sds(3, 6, 32, 128), sds(3, 6, 32, 128), sds(1, 128)],
        in_specs=[VMEM] * 8 + [SMEM] * 2, out_specs=[VMEM] * 4,
        scratch_shapes=[
            pltpu.VMEM((3, 8, 56, 128), F32), pltpu.VMEM((3, 6, 40, 128), F32),
            *[pltpu.VMEM((6, 40, 128), F32)] * 4,
            pltpu.VMEM((8, 56, 128), F32), pltpu.VMEM((3, 8, 56, 128), F32), pltpu.VMEM((3, 8, 56, 128), F32),
        ],
        compiler_params=params(LIM), cost_estimate=cost(1 << 23), name="edge_work",
    )(*rz, eu, ef, eu4, ef4, tiles, square, prefactor, yield_stress)
    devices = 1
    for axis in AX:
        devices = devices * lax.axis_size(axis)
    one, two, send = pl.pallas_call(
        coarsen,
        out_shape=[sds(8, 16, 64), sds(4, 8, 32), sds(devices, 1, 256)],
        in_specs=[VMEM] * 3, out_specs=[VMEM] * 3,
        scratch_shapes=[
            pltpu.VMEM((22, 56, 128), F32), pltpu.VMEM((22, 56, 128), F32),
            pltpu.VMEM((10, 56, 128), F32), pltpu.VMEM((10, 56, 128), F32), pltpu.VMEM((10, 24, 256), F32),
            pltpu.VMEM((10, 24, 128), F32), pltpu.VMEM((24, 128), F32), pltpu.VMEM((24, 128), F32),
            pltpu.VMEM((27, 1, 128), F32),
        ],
        compiler_params=params(LIM), cost_estimate=cost(1 << 22), name="coarsen",
    )(v, ve, total)
    got = lax.all_to_all(send, AX, 0, 0, tiled=True)
    smoothed, visc, one, two, residual = pl.pallas_call(
        results,
        out_shape=[sds(3, NX, NY, NZ), sds(NX, NY, NZ), sds(8, 16, 64), sds(4, 8, 32), sds(3, NX, NY, NZ)],
        in_specs=[VMEM] * 8, out_specs=[VMEM] * 5,
        compiler_params=params(LIM), cost_estimate=cost(1 << 22), name="results",
    )(v, u2, res, ve, ue, re, one, two)
    cells = 3.0 * NX * NY * NZ * devices
    three, rms = pl.pallas_call(
        functools.partial(finish, cells), out_shape=[sds(2, 4, 16), sds(1, 128)],
        in_specs=[VMEM], out_specs=[VMEM] * 2, compiler_params=params(LIM), name="finish",
    )(got)
    return smoothed, visc, one, two, three, residual, rms[0, 0]


def solution(mesh):
    field, cell = P(None, *AX), P(*AX)
    return jax.shard_map(
        per_device,
        mesh=mesh,
        in_specs=(field, field, cell, P(), P()),
        out_specs=(field, cell, cell, cell, cell, field, P()),
        check_vma=False,
    )
```
